32 devices in a mesh: dp: 2 (over x), tpa: 4 (over z), tpb: 4 (over y, core).
Axes of the slice: x: 2, y: 2, z: 4, core: 2. Of those that a mesh axis runs over, the one named last changes fastest.
Arguments:
- hidden: bfloat16 [32, 25, 3072], P('dp'), parts along dimension 0
- w_head: bfloat16 [3072, 128256], P(None, ('tpa', 'tpb'))
- q_draft: float32 [32, 24, 128256], P(('dp', 'tpa', 'tpb')), parts along dimension 0
- x_draft: int32 [32, 24], P('dp'), parts along dimension 0
Outputs:
- output 1: float32 [32, 24], P('dp'), parts along dimension 0
- output 2: float32 [32], P('dp'), parts along dimension 0
- output 3: float32 [32, 24, 128256], P('dp', None, ('tpa', 'tpb')), parts along dimension 0
- output 4: float32 [32, 128256], P('dp', ('tpa', 'tpb')), parts along dimension 0
There are 2 independent parts. The reference program is written for one: setup_inputs(seed, part) draws one part's arguments, and reference() takes and returns one part's arrays. A program takes and returns all parts, laid end to end along the dimension named above; an argument that names none is the same for every part.
All inputs are finite; a program needn't handle non-finite values.
Results may differ from the reference program's by a relative error of at most 0.001.
Values are sent between devices in bfloat16 or wider.
A program may use at most 1 GiB of HBM per device.

```python
import jax
import jax.numpy as jnp
from jax import lax

NUM_SEQS = 16
NUM_DRAFT = 24
D_MODEL = 3072
VOCAB_SIZE = 128256
ROW_BLOCK = 8
INV_TEMP = 1.25
DRAFT_LOGIT_SCALE = 0.5


def draw_tokens(tok_key):
    key_vals, key_low, key_high = jax.random.split(tok_key, 3)
    n_total = NUM_SEQS * NUM_DRAFT
    tokens = jax.random.randint(key_vals, (n_total,), 0, VOCAB_SIZE, jnp.int32)
    low_slot = jax.random.randint(key_low, (), 0, n_total, jnp.int32)
    high_slot = (low_slot + 1 + jax.random.randint(key_high, (), 0, n_total - 1, jnp.int32)) % n_total
    slots = jnp.arange(n_total, dtype=jnp.int32)
    tokens = jnp.where(slots == low_slot, 0, tokens)
    tokens = jnp.where(slots == high_slot, VOCAB_SIZE - 1, tokens)
    return tokens.reshape(NUM_SEQS, NUM_DRAFT)


def setup_inputs(seed: int = 0, part: int = 0) -> dict:
    base_key = jax.random.key(seed)
    part_key = jax.random.fold_in(base_key, part)
    key_hidden, key_draft, key_tok = jax.random.split(part_key, 3)
    hidden = jax.random.normal(key_hidden, (NUM_SEQS, NUM_DRAFT + 1, D_MODEL), jnp.float32)
    w_head = jax.random.normal(jax.random.key(seed + 1), (D_MODEL, VOCAB_SIZE), jnp.float32) * D_MODEL ** -0.5
    draft_logits = jax.random.normal(key_draft, (NUM_SEQS, NUM_DRAFT, VOCAB_SIZE), jnp.float32) * DRAFT_LOGIT_SCALE
    q_draft = jax.nn.softmax(draft_logits, axis=-1)
    x_draft = draw_tokens(key_tok)
    return {"hidden": hidden.astype(jnp.bfloat16), "w_head": w_head.astype(jnp.bfloat16), "q_draft": q_draft, "x_draft": x_draft}


def reference(hidden, w_head, q_draft, x_draft):
    num_blocks = NUM_SEQS // ROW_BLOCK

    def one_block(block):
        hid_blk, q_blk, tok_blk = block
        flat_hid = hid_blk.reshape(ROW_BLOCK * (NUM_DRAFT + 1), D_MODEL)
        logits = jnp.dot(flat_hid, w_head, preferred_element_type=jnp.float32) * INV_TEMP
        prob_all = jax.nn.softmax(logits, axis=-1).reshape(ROW_BLOCK, NUM_DRAFT + 1, VOCAB_SIZE)
        p_draft = prob_all[:, :NUM_DRAFT, :]
        tok_idx = tok_blk[:, :, None]
        p_pick = jnp.take_along_axis(p_draft, tok_idx, axis=2)[:, :, 0]
        q_pick = jnp.take_along_axis(q_blk, tok_idx, axis=2)[:, :, 0]
        accept = jnp.minimum(1.0, p_pick / q_pick)
        excess = jnp.maximum(p_draft - q_blk, 0.0)
        residual = excess / jnp.sum(excess, axis=-1, keepdims=True)
        return accept, residual, prob_all[:, NUM_DRAFT, :]

    block_outs = lax.map(one_block, (
        hidden.reshape(num_blocks, ROW_BLOCK, NUM_DRAFT + 1, D_MODEL),
        q_draft.reshape(num_blocks, ROW_BLOCK, NUM_DRAFT, VOCAB_SIZE),
        x_draft.reshape(num_blocks, ROW_BLOCK, NUM_DRAFT)))
    accept = block_outs[0].reshape(NUM_SEQS, NUM_DRAFT)
    residual = block_outs[1].reshape(NUM_SEQS, NUM_DRAFT, VOCAB_SIZE)
    bonus_prob = block_outs[2].reshape(NUM_SEQS, VOCAB_SIZE)
    expected = jnp.sum(jnp.cumprod(accept, axis=1), axis=1)
    return accept, expected, residual, bonus_prob
```

```python
import functools

import jax
import jax.numpy as jnp
from jax import lax
from jax.experimental import pallas as pl
from jax.experimental.pallas import tpu as pltpu
from jax.sharding import PartitionSpec as P

INV_TEMP = 1.25
VOCAB_AXES = ("tpa", "tpb")
MESH = pl.DeviceIdType.MESH
LANES = 128
ROWS = 8
W_ROWS = 256
W_BUFS = 4


def xor4(a, r):
    low = lax.rem(lax.rem(a, 2) + lax.rem(r, 2), 2)
    high = lax.rem(lax.div(a, 2) + lax.div(r, 2), 2)
    return low + 2 * high


def exchange_kernel(n, phases, vl, hid_ref, w_ref, q_ref, x_ref, z_ref, tot_ref,
                    hid_v, hs, wbuf, qbuf, x_v, colmax, colsum, scale, part, stat, zmsg,
                    in_sem, w_sem, qs_sem, qr_sem, ss_sem, sr_sem, zs_sem, zr_sem):
    vp = z_ref.shape[1]
    tiles = vp // LANES
    last = vl - (tiles - 1) * LANES
    rows_all = z_ref.shape[0]
    draft_rows = phases * n * ROWS
    my_a, my_b = lax.axis_index("tpa"), lax.axis_index("tpb")
    me = my_a * 4 + my_b
    lane = lax.broadcasted_iota(jnp.int32, (ROWS, LANES), 1)

    def peer(r):
        return xor4(my_a, lax.div(r, 4)), xor4(my_b, lax.rem(r, 4))

    def window(k):
        col = lax.div(k * vl, LANES) * LANES
        return pl.multiple_of(col, LANES), k * vl - col

    def sized(k, body):
        _, o = window(k)
        wide = o + vl > vp
        pl.when(wide)(lambda: body(vp + LANES))
        pl.when(jnp.logical_not(wide))(lambda: body(vp))

    def q_copy(g, r, width):
        a, b = peer(r)
        col, _ = window(a * 4 + b)
        return pltpu.make_async_remote_copy(
            src_ref=q_ref.at[pl.ds(pl.multiple_of(g * ROWS, ROWS), ROWS), pl.ds(col, width)],
            dst_ref=qbuf.at[g, me, :, pl.ds(0, width)],
            send_sem=qs_sem.at[g, r], recv_sem=qr_sem.at[g, me],
            device_id={"tpa": a, "tpb": b}, device_id_type=MESH)

    def own_copy(g, width):
        col, _ = window(me)
        return pltpu.make_async_copy(
            q_ref.at[pl.ds(pl.multiple_of(g * ROWS, ROWS), ROWS), pl.ds(col, width)],
            qbuf.at[g, me, :, pl.ds(0, width)], qr_sem.at[g, me])

    def q_arrival(g, s, width):
        return pltpu.make_async_remote_copy(
            src_ref=qbuf.at[g, s, :, pl.ds(0, width)], dst_ref=qbuf.at[g, s, :, pl.ds(0, width)],
            send_sem=qs_sem.at[g, 0], recv_sem=qr_sem.at[g, s],
            device_id={"tpa": my_a, "tpb": my_b}, device_id_type=MESH)

    def send_phase(g):
        def one(r, c):
            a, b = peer(r)
            sized(a * 4 + b, lambda width: q_copy(g, r, width).start())
            return c
        lax.fori_loop(1, n, one, 0)

    def w_copy(c, slot):
        return pltpu.make_async_copy(w_ref.at[pl.ds(pl.multiple_of(c * W_ROWS, W_ROWS), W_ROWS), :], wbuf.at[slot], w_sem.at[slot])

    full_chunks = vl // W_ROWS
    w_tail = vl - full_chunks * W_ROWS
    tail_slot = full_chunks % W_BUFS
    tail_copy = pltpu.make_async_copy(
        w_ref.at[pl.ds(full_chunks * W_ROWS, w_tail), :], wbuf.at[tail_slot, pl.ds(0, w_tail), :], w_sem.at[tail_slot])

    hid_copy = pltpu.make_async_copy(hid_ref, hid_v, in_sem.at[0])
    x_copy = pltpu.make_async_copy(x_ref, x_v, in_sem.at[1])
    hid_copy.start()
    x_copy.start()
    for c in range(W_BUFS):
        w_copy(c, c).start()

    barrier = pltpu.get_barrier_semaphore()

    def greet(r, c):
        a, b = peer(r)
        pl.semaphore_signal(barrier, inc=1, device_id={"tpa": a, "tpb": b}, device_id_type=MESH)
        return c
    lax.fori_loop(1, n, greet, 0)
    pl.semaphore_wait(barrier, n - 1)

    send_phase(0)
    send_phase(1)
    for g in range(phases):
        sized(me, lambda width, g=g: own_copy(g, width).start())

    hid_copy.wait()
    row = lax.broadcasted_iota(jnp.int32, (rows_all, rows_all), 0)
    col = lax.broadcasted_iota(jnp.int32, (rows_all, rows_all), 1)
    source = jnp.where(row < draft_rows, ((row // (n * ROWS)) * ROWS + row % ROWS) * n + (row // ROWS) % n, row)
    permute = jnp.where(col == source, 1.0, 0.0).astype(jnp.bfloat16)
    depth = hid_v.shape[1]

    def permute_columns(c, carry):
        at = pl.ds(pl.multiple_of(c * 256, 256), 256)
        hs[:, at] = jnp.dot(permute, hid_v[:, at], preferred_element_type=jnp.float32).astype(jnp.bfloat16)
        return carry
    lax.fori_loop(0, depth // 256, permute_columns, 0)

    nt = (((1,), (1,)), ((), ()))

    def logits(c, carry):
        slot = lax.rem(c, W_BUFS)
        w_copy(c, slot).wait()
        z_ref[:, pl.ds(pl.multiple_of(c * W_ROWS, W_ROWS), W_ROWS)] = lax.dot_general(
            hs[...], wbuf[slot], nt, preferred_element_type=jnp.float32) * INV_TEMP

        @pl.when(c + W_BUFS < full_chunks)
        def _():
            w_copy(c + W_BUFS, slot).start()

        @pl.when(c + W_BUFS == full_chunks)
        def _():
            tail_copy.start()
        return carry
    lax.fori_loop(0, full_chunks, logits, 0)
    tail_copy.wait()
    z_ref[:, full_chunks * W_ROWS:vl] = lax.dot_general(
        hs[...], wbuf[tail_slot, 0:w_tail, :], nt, preferred_element_type=jnp.float32) * INV_TEMP

    def tile_of(j):
        return slice(j * LANES, (j + 1) * LANES)

    def row_stats(t, carry):
        rows = pl.ds(pl.multiple_of(t * ROWS, ROWS), ROWS)
        m = jnp.where(lane < last, z_ref[rows, tile_of(tiles - 1)], -jnp.inf)
        for j in range(tiles - 1):
            m = jnp.maximum(m, z_ref[rows, tile_of(j)])
        m = jnp.broadcast_to(jnp.max(m, axis=1, keepdims=True), (ROWS, LANES))
        s = jnp.zeros((ROWS, LANES), jnp.float32)
        for j in range(tiles):
            e = jnp.exp(z_ref[rows, tile_of(j)] - m)
            if j == tiles - 1:
                e = jnp.where(lane < last, e, 0.0)
            z_ref[rows, tile_of(j)] = e
            s = s + e
        colmax[rows, :] = m
        colsum[rows, :] = jnp.broadcast_to(jnp.sum(s, axis=1, keepdims=True), (ROWS, LANES))
        return carry
    lax.fori_loop(0, rows_all // ROWS, row_stats, 0)
    spare = colmax.shape[0] - rows_all
    colmax[rows_all:, :] = jnp.zeros((spare, LANES), jnp.float32)
    colsum[rows_all:, :] = jnp.ones((spare, LANES), jnp.float32)

    blocks = colmax.shape[0] // LANES

    def as_rows(ref):
        return jnp.concatenate([ref[i * LANES:(i + 1) * LANES, :].T[0:1, :] for i in range(blocks)], axis=0)
    stat[me, 0] = as_rows(colmax)
    stat[me, 1] = as_rows(colsum)

    def stat_copy(r, s):
        a, b = peer(r)
        return pltpu.make_async_remote_copy(
            src_ref=stat.at[me], dst_ref=stat.at[s], send_sem=ss_sem.at[r], recv_sem=sr_sem.at[s],
            device_id={"tpa": a, "tpb": b}, device_id_type=MESH)

    def send_stat(r, c):
        stat_copy(r, me).start()
        return c
    lax.fori_loop(1, n, send_stat, 0)
    send_phase(2)

    def wait_stat(r, c):
        a, b = peer(r)
        stat_copy(r, a * 4 + b).wait_recv()
        return c
    lax.fori_loop(1, n, wait_stat, 0)
    glob_max = stat[0, 0]
    for s in range(1, n):
        glob_max = jnp.maximum(glob_max, stat[s, 0])
    glob_sum = jnp.zeros_like(glob_max)
    for s in range(n):
        glob_sum = glob_sum + stat[s, 1] * jnp.exp(stat[s, 0] - glob_max)
    factor = jnp.exp(stat[me, 0] - glob_max) / glob_sum
    for i in range(blocks):
        scale[i * LANES:(i + 1) * LANES, :] = jnp.broadcast_to(factor[i:i + 1, :], (LANES, LANES)).T

    for t in range(draft_rows // ROWS, rows_all // ROWS):
        rows = slice(t * ROWS, (t + 1) * ROWS)
        for j in range(tiles):
            z_ref[rows, tile_of(j)] = z_ref[rows, tile_of(j)] * scale[rows, :]

    x_copy.wait()
    _, offset = window(me)
    shift = lax.rem(LANES - offset, LANES)
    lane_f = lane.astype(jnp.float32)
    num_draft = x_v.shape[1]

    def excess(g, s):
        rows = pl.ds(pl.multiple_of(g * (n * ROWS) + s * ROWS, ROWS), ROWS)
        tokens = jnp.broadcast_to(x_v[pl.ds(s, 1), :].astype(jnp.float32), (ROWS, num_draft))
        position = lax.broadcasted_iota(jnp.int32, (ROWS, num_draft), 0) + g * ROWS
        here = lax.broadcasted_iota(jnp.int32, (ROWS, num_draft), 1) == position
        token = jnp.sum(jnp.where(here, tokens, 0.0), axis=1, keepdims=True) - (me * vl).astype(jnp.float32)
        token = jnp.broadcast_to(jnp.where(token < vl, token, -1.0), (ROWS, LANES))
        sc = scale[rows, :]
        z_sum = p_pick = q_pick = jnp.zeros((ROWS, LANES), jnp.float32)
        this = pltpu.roll(qbuf[g, s, :, 0:LANES], shift, 1)
        for j in range(tiles):
            following = pltpu.roll(qbuf[g, s, :, (j + 1) * LANES:(j + 2) * LANES], shift, 1)
            q = jnp.where(lane < LANES - offset, this, following)
            this = following
            p = z_ref[rows, tile_of(j)] * sc
            d = jnp.maximum(p - q, 0.0)
            if j == tiles - 1:
                d = jnp.where(lane < last, d, 0.0)
            z_ref[rows, tile_of(j)] = d
            z_sum = z_sum + d
            hit = lane_f == token - float(j * LANES)
            p_pick = jnp.where(hit, p, p_pick)
            q_pick = jnp.where(hit, q, q_pick)
        part[0, rows, :] = z_sum
        part[1, rows, :] = p_pick
        part[2, rows, :] = q_pick

    def z_copy(g, r, s):
        a, b = peer(r)
        return pltpu.make_async_remote_copy(
            src_ref=zmsg.at[g, me], dst_ref=zmsg.at[g, s], send_sem=zs_sem.at[g, r], recv_sem=zr_sem.at[g, s],
            device_id={"tpa": a, "tpb": b}, device_id_type=MESH)

    def phase(g, carry):
        sized(me, lambda width: own_copy(g, width).wait())
        excess(g, me)

        def one(r, c):
            a, b = peer(r)
            s = a * 4 + b
            sized(me, lambda width: q_arrival(g, s, width).wait_recv())
            excess(g, s)
            return c
        lax.fori_loop(1, n, one, 0)
        block = pl.ds(pl.multiple_of(g * (n * ROWS), n * ROWS), n * ROWS)
        sums = [jnp.sum(part[i, block, :].T, axis=0, keepdims=True) for i in range(3)]
        zmsg[g, me] = jnp.concatenate(sums + [jnp.zeros((1, LANES), jnp.float32)], axis=0)

        def send(r, c):
            z_copy(g, r, me).start()
            return c
        lax.fori_loop(1, n, send, 0)
        return carry
    lax.fori_loop(0, phases, phase, 0)

    def collect(i, c):
        g, r = lax.div(i, n), lax.rem(i, n)

        @pl.when(r > 0)
        def _():
            a, b = peer(r)
            z_copy(g, r, a * 4 + b).wait_recv()
        return c
    lax.fori_loop(0, phases * n, collect, 0)
    for g in range(phases):
        total = zmsg[g, 0]
        for s in range(1, n):
            total = total + zmsg[g, s]
        tot_ref[g] = total

    def drain(i, c):
        g, r = lax.div(i, n), lax.rem(i, n)

        @pl.when(r > 0)
        def _():
            a, b = peer(r)
            sized(a * 4 + b, lambda width: q_copy(g, r, width).wait_send())
            z_copy(g, r, me).wait_send()

        @pl.when(jnp.logical_and(r > 0, g == 0))
        def _():
            stat_copy(r, me).wait_send()
        return c
    lax.fori_loop(0, phases * n, drain, 0)


def finish_kernel(n, phases, vl, tot_ref, z_ref, res_ref, bonus_ref, accept_ref, expected_ref, zcol):
    b = pl.program_id(0)
    width = n * ROWS
    num_draft = phases * ROWS

    @pl.when(b == 0)
    def _():
        for g in range(phases):
            zcol[g] = jnp.broadcast_to(tot_ref[g, 0:1, :], (width, LANES)).T
        bonus_ref[...] = z_ref[phases * width:phases * width + n, 0:vl]
        seq_of = lax.broadcasted_iota(jnp.int32, (n, width), 1) // ROWS == lax.broadcasted_iota(jnp.int32, (n, width), 0)
        pos_of = lax.broadcasted_iota(jnp.int32, (ROWS, width), 1) % ROWS == lax.broadcasted_iota(jnp.int32, (ROWS, width), 0)
        to_seq = (lax.broadcasted_iota(jnp.int32, (width, n), 0) // ROWS
                  == lax.broadcasted_iota(jnp.int32, (width, n), 1)).astype(jnp.float32)
        by_seq = jnp.zeros((n, num_draft), jnp.float32)
        by_pos = []
        for g in range(phases):
            a = jnp.minimum(1.0, tot_ref[g, 1:2, :] / tot_ref[g, 2:3, :])
            to_pos = (lax.broadcasted_iota(jnp.int32, (width, num_draft), 0) % ROWS + g * ROWS
                      == lax.broadcasted_iota(jnp.int32, (width, num_draft), 1)).astype(jnp.float32)
            by_seq = by_seq + jnp.dot(jnp.where(seq_of, jnp.broadcast_to(a, (n, width)), 0.0), to_pos,
                                      precision=lax.Precision.HIGHEST, preferred_element_type=jnp.float32)
            by_pos.append(jnp.dot(jnp.where(pos_of, jnp.broadcast_to(a, (ROWS, width)), 0.0), to_seq,
                                  precision=lax.Precision.HIGHEST, preferred_element_type=jnp.float32))
        accept_ref[...] = by_seq
        product = by_pos[0][0:1, :]
        total = product
        for k in range(1, num_draft):
            product = product * by_pos[k // ROWS][k % ROWS:k % ROWS + 1, :]
            total = total + product
        expected_ref[...] = total

    for g in range(phases):
        norm = zcol[g, pl.ds(pl.multiple_of(b * ROWS, ROWS), ROWS), :]
        rows = pl.ds(pl.multiple_of(g * width + b * ROWS, ROWS), ROWS)
        for j in range(pl.cdiv(vl, LANES)):
            w = min(LANES, vl - j * LANES)
            res_ref[0, g * ROWS:(g + 1) * ROWS, j * LANES:j * LANES + w] = (z_ref[rows, j * LANES:(j + 1) * LANES] / norm)[:, 0:w]


def solution(mesh):
    n = mesh.shape["tpa"] * mesh.shape["tpb"]

    def local_step(hidden, w_head, q_draft, x_draft):
        seqs, positions, depth = hidden.shape
        vl = w_head.shape[1]
        num_draft = x_draft.shape[1]
        phases = num_draft // ROWS
        vp = pl.cdiv(vl, LANES) * LANES
        rows = seqs * positions
        stat_rows = pl.cdiv(rows, LANES) * LANES
        f32 = jnp.float32
        any_spec = pl.BlockSpec(memory_space=pl.ANY)
        vmem_spec = pl.BlockSpec(memory_space=pltpu.VMEM)
        z, tot = pl.pallas_call(
            functools.partial(exchange_kernel, n, phases, vl),
            name="exchange",
            out_shape=(pltpu.VMEM((rows, vp), f32), pltpu.VMEM((phases, 4, LANES), f32)),
            in_specs=[any_spec] * 4,
            out_specs=(vmem_spec, vmem_spec),
            scratch_shapes=[
                pltpu.VMEM((rows, depth), jnp.bfloat16),
                pltpu.VMEM((rows, depth), jnp.bfloat16),
                pltpu.VMEM((W_BUFS, W_ROWS, depth), jnp.bfloat16),
                pltpu.VMEM((phases, n, ROWS, vp + LANES), f32),
                pltpu.VMEM((seqs, num_draft), jnp.int32),
                pltpu.VMEM((stat_rows, LANES), f32),
                pltpu.VMEM((stat_rows, LANES), f32),
                pltpu.VMEM((stat_rows, LANES), f32),
                pltpu.VMEM((3, phases * n * ROWS, LANES), f32),
                pltpu.VMEM((n, 2, stat_rows // LANES, LANES), f32),
                pltpu.VMEM((phases, n, 4, LANES), f32),
                pltpu.SemaphoreType.DMA((2,)),
                pltpu.SemaphoreType.DMA((W_BUFS,)),
                pltpu.SemaphoreType.DMA((phases, n)),
                pltpu.SemaphoreType.DMA((phases, n)),
                pltpu.SemaphoreType.DMA((n,)),
                pltpu.SemaphoreType.DMA((n,)),
                pltpu.SemaphoreType.DMA((phases, n)),
                pltpu.SemaphoreType.DMA((phases, n)),
            ],
            compiler_params=pltpu.CompilerParams(collective_id=0, has_side_effects=True, vmem_limit_bytes=48 * 2**20),
        )(hidden.transpose(1, 0, 2).reshape(rows, depth), w_head.T, q_draft.reshape(num_draft, q_draft.shape[2]), x_draft)
        residual, bonus, accept, expected = pl.pallas_call(
            functools.partial(finish_kernel, n, phases, vl),
            name="finish",
            grid=(seqs,),
            out_shape=(jax.ShapeDtypeStruct((seqs, num_draft, vl), f32), jax.ShapeDtypeStruct((seqs, vl), f32),
                       jax.ShapeDtypeStruct((seqs, num_draft), f32), jax.ShapeDtypeStruct((1, seqs), f32)),
            in_specs=[vmem_spec, vmem_spec],
            out_specs=(pl.BlockSpec((1, num_draft, vl), lambda b: (b, 0, 0)), pl.BlockSpec((seqs, vl), lambda b: (0, 0)),
                       pl.BlockSpec((seqs, num_draft), lambda b: (0, 0)), pl.BlockSpec((1, seqs), lambda b: (0, 0))),
            scratch_shapes=[pltpu.VMEM((phases, n * ROWS, LANES), f32)],
            compiler_params=pltpu.CompilerParams(vmem_limit_bytes=16 * 2**20),
        )(tot, z)
        return accept, expected.reshape(seqs), residual, bonus

    return jax.shard_map(
        local_step, mesh=mesh,
        in_specs=(P("dp", None, None), P(None, VOCAB_AXES), P(("dp",) + VOCAB_AXES, None, None), P("dp", None)),
        out_specs=(P("dp", None), P("dp"), P("dp", None, VOCAB_AXES), P("dp", VOCAB_AXES)),
        check_vma=False)
```

```python
import functools

import jax
import jax.numpy as jnp
from jax import lax
from jax.experimental import pallas as pl
from jax.experimental.pallas import tpu as pltpu
from jax.sharding import PartitionSpec as P

INV_TEMP = 1.25
VOCAB_AXES = ("tpa", "tpb")
MESH = pl.DeviceIdType.MESH
LANES = 128
ROWS = 8
W_ROWS = 256
W_BUFS = 4
ORDER_0 = (8, 12, 4, 9, 13, 1, 10, 14, 5, 11, 15, 2, 6, 7, 3)
ORDER_1 = (12, 4, 8, 13, 1, 9, 14, 5, 10, 15, 2, 11, 6, 7, 3)
SCALE = 2.0 ** 64


def xor4(a, r):
    low = lax.rem(lax.rem(a, 2) + lax.rem(r, 2), 2)
    high = lax.rem(lax.div(a, 2) + lax.div(r, 2), 2)
    return low + 2 * high


def exchange_kernel(n, phases, vl, hid_ref, w_ref, q_ref, x_ref, z_ref, tot_ref,
                    hid_v, hs, wbuf, qbuf, x_v, colmax, colsum, scale, part, stat, zmsg,
                    in_sem, w_sem, qs_sem, qr_sem, ss_sem, sr_sem, zs_sem, zr_sem):
    vp = z_ref.shape[1]
    tiles = vp // LANES
    last = vl - (tiles - 1) * LANES
    rows_all = z_ref.shape[0]
    draft_rows = phases * n * ROWS
    my_a, my_b = lax.axis_index("tpa"), lax.axis_index("tpb")
    me = my_a * 4 + my_b
    lane = lax.broadcasted_iota(jnp.int32, (ROWS, LANES), 1)

    def peer(r):
        return xor4(my_a, lax.div(r, 4)), xor4(my_b, lax.rem(r, 4))

    def window(k):
        col = lax.div(k * vl, LANES) * LANES
        return pl.multiple_of(col, LANES), k * vl - col

    def sized(k, body):
        _, o = window(k)
        wide = o + vl > vp
        pl.when(wide)(lambda: body(vp + LANES))
        pl.when(jnp.logical_not(wide))(lambda: body(vp))

    def q_copy(g, r, width):
        a, b = peer(r)
        col, _ = window(a * 4 + b)
        return pltpu.make_async_remote_copy(
            src_ref=q_ref.at[pl.ds(pl.multiple_of(g * ROWS, ROWS), ROWS), pl.ds(col, width)],
            dst_ref=qbuf.at[g, me, :, pl.ds(0, width)],
            send_sem=qs_sem.at[g, r], recv_sem=qr_sem.at[g, me],
            device_id={"tpa": a, "tpb": b}, device_id_type=MESH)

    def own_copy(g, width):
        col, _ = window(me)
        return pltpu.make_async_copy(
            q_ref.at[pl.ds(pl.multiple_of(g * ROWS, ROWS), ROWS), pl.ds(col, width)],
            qbuf.at[g, me, :, pl.ds(0, width)], qr_sem.at[g, me])

    def q_arrival(g, s, width):
        return pltpu.make_async_remote_copy(
            src_ref=qbuf.at[g, s, :, pl.ds(0, width)], dst_ref=qbuf.at[g, s, :, pl.ds(0, width)],
            send_sem=qs_sem.at[g, 0], recv_sem=qr_sem.at[g, s],
            device_id={"tpa": my_a, "tpb": my_b}, device_id_type=MESH)

    core = lax.rem(my_b, 2)

    def nth(g, i):
        i = i if g < phases - 1 else len(ORDER_0) - 1 - i
        return ORDER_0[i] + core * (ORDER_1[i] - ORDER_0[i])

    def send_phase(g):
        for i in range(n - 1):
            r = nth(g, i)
            a, b = peer(r)
            sized(a * 4 + b, lambda width, r=r: q_copy(g, r, width).start())

    def w_copy(c, slot):
        return pltpu.make_async_copy(w_ref.at[pl.ds(pl.multiple_of(c * W_ROWS, W_ROWS), W_ROWS), :], wbuf.at[slot], w_sem.at[slot])

    full_chunks = vl // W_ROWS
    w_tail = vl - full_chunks * W_ROWS
    tail_slot = full_chunks % W_BUFS
    tail_copy = pltpu.make_async_copy(
        w_ref.at[pl.ds(full_chunks * W_ROWS, w_tail), :], wbuf.at[tail_slot, pl.ds(0, w_tail), :], w_sem.at[tail_slot])

    hid_copy = pltpu.make_async_copy(hid_ref, hid_v, in_sem.at[0])
    x_copy = pltpu.make_async_copy(x_ref, x_v, in_sem.at[1])
    hid_copy.start()
    x_copy.start()
    for c in range(W_BUFS):
        w_copy(c, c).start()

    barrier = pltpu.get_barrier_semaphore()

    def greet(r, c):
        a, b = peer(r)
        pl.semaphore_signal(barrier, inc=1, device_id={"tpa": a, "tpb": b}, device_id_type=MESH)
        return c
    lax.fori_loop(1, n, greet, 0)
    pl.semaphore_wait(barrier, n - 1)

    send_phase(0)
    send_phase(1)
    for g in range(phases):
        sized(me, lambda width, g=g: own_copy(g, width).start())

    hid_copy.wait()
    row = lax.broadcasted_iota(jnp.int32, (rows_all, rows_all), 0)
    col = lax.broadcasted_iota(jnp.int32, (rows_all, rows_all), 1)
    source = jnp.where(row < draft_rows, ((row // (n * ROWS)) * ROWS + row % ROWS) * n + (row // ROWS) % n, row)
    permute = jnp.where(col == source, 1.0, 0.0).astype(jnp.bfloat16)
    depth = hid_v.shape[1]

    def permute_columns(c, carry):
        at = pl.ds(pl.multiple_of(c * 256, 256), 256)
        hs[:, at] = jnp.dot(permute, hid_v[:, at], preferred_element_type=jnp.float32).astype(jnp.bfloat16)
        return carry
    lax.fori_loop(0, depth // 256, permute_columns, 0)

    nt = (((1,), (1,)), ((), ()))

    def logits(c, carry):
        slot = lax.rem(c, W_BUFS)
        w_copy(c, slot).wait()
        z_ref[:, pl.ds(pl.multiple_of(c * W_ROWS, W_ROWS), W_ROWS)] = lax.dot_general(
            hs[...], wbuf[slot], nt, preferred_element_type=jnp.float32) * INV_TEMP

        @pl.when(c + W_BUFS < full_chunks)
        def _():
            w_copy(c + W_BUFS, slot).start()

        @pl.when(c + W_BUFS == full_chunks)
        def _():
            tail_copy.start()
        return carry
    lax.fori_loop(0, full_chunks, logits, 0)
    tail_copy.wait()
    z_ref[:, full_chunks * W_ROWS:vl] = lax.dot_general(
        hs[...], wbuf[tail_slot, 0:w_tail, :], nt, preferred_element_type=jnp.float32) * INV_TEMP

    def tile_of(j):
        return slice(j * LANES, (j + 1) * LANES)

    def row_stats(t, carry):
        rows = pl.ds(pl.multiple_of(t * ROWS, ROWS), ROWS)
        m = jnp.where(lane < last, z_ref[rows, tile_of(tiles - 1)], -jnp.inf)
        for j in range(tiles - 1):
            m = jnp.maximum(m, z_ref[rows, tile_of(j)])
        m = jnp.broadcast_to(jnp.max(m, axis=1, keepdims=True), (ROWS, LANES))
        s = jnp.zeros((ROWS, LANES), jnp.float32)
        for j in range(tiles):
            e = jnp.exp(z_ref[rows, tile_of(j)] - m)
            if j == tiles - 1:
                e = jnp.where(lane < last, e, 0.0)
            z_ref[rows, tile_of(j)] = e
            s = s + e
        colmax[rows, :] = m
        colsum[rows, :] = jnp.broadcast_to(jnp.sum(s, axis=1, keepdims=True), (ROWS, LANES))
        return carry
    lax.fori_loop(0, rows_all // ROWS, row_stats, 0)
    spare = colmax.shape[0] - rows_all
    colmax[rows_all:, :] = jnp.zeros((spare, LANES), jnp.float32)
    colsum[rows_all:, :] = jnp.ones((spare, LANES), jnp.float32)

    blocks = colmax.shape[0] // LANES

    def as_rows(ref):
        return jnp.concatenate([ref[i * LANES:(i + 1) * LANES, :].T[0:1, :] for i in range(blocks)], axis=0)
    stat[me, 0] = as_rows(colmax)
    stat[me, 1] = as_rows(colsum)

    def stat_copy(r, s):
        a, b = peer(r)
        return pltpu.make_async_remote_copy(
            src_ref=stat.at[me], dst_ref=stat.at[s], send_sem=ss_sem.at[r], recv_sem=sr_sem.at[s],
            device_id={"tpa": a, "tpb": b}, device_id_type=MESH)

    def send_stat(r, c):
        stat_copy(r, me).start()
        return c
    lax.fori_loop(1, n, send_stat, 0)
    send_phase(2)

    def wait_stat(r, c):
        a, b = peer(r)
        stat_copy(r, a * 4 + b).wait_recv()
        return c
    lax.fori_loop(1, n, wait_stat, 0)
    glob_max = stat[0, 0]
    for s in range(1, n):
        glob_max = jnp.maximum(glob_max, stat[s, 0])
    glob_sum = jnp.zeros_like(glob_max)
    for s in range(n):
        glob_sum = glob_sum + stat[s, 1] * jnp.exp(stat[s, 0] - glob_max)
    factor = jnp.exp(stat[me, 0] - glob_max) / glob_sum
    for i in range(blocks):
        scale[i * LANES:(i + 1) * LANES, :] = jnp.broadcast_to(factor[i:i + 1, :], (LANES, LANES)).T

    for t in range(draft_rows // ROWS, rows_all // ROWS):
        rows = slice(t * ROWS, (t + 1) * ROWS)
        for j in range(tiles):
            z_ref[rows, tile_of(j)] = z_ref[rows, tile_of(j)] * scale[rows, :]

    x_copy.wait()
    _, offset = window(me)
    shift = lax.rem(LANES - offset, LANES)
    lane_f = lane.astype(jnp.float32)
    num_draft = x_v.shape[1]

    def excess(g, s):
        rows = pl.ds(pl.multiple_of(g * (n * ROWS) + s * ROWS, ROWS), ROWS)
        tokens = jnp.broadcast_to(x_v[pl.ds(s, 1), :].astype(jnp.float32), (ROWS, num_draft))
        position = lax.broadcasted_iota(jnp.int32, (ROWS, num_draft), 0) + g * ROWS
        here = lax.broadcasted_iota(jnp.int32, (ROWS, num_draft), 1) == position
        token = jnp.sum(jnp.where(here, tokens, 0.0), axis=1, keepdims=True) - (me * vl).astype(jnp.float32)
        token = jnp.broadcast_to(jnp.where(token < vl, token, -1.0), (ROWS, LANES))
        sc = scale[rows, :]
        z_sum = p_pick = q_pick = jnp.zeros((ROWS, LANES), jnp.float32)
        this = pltpu.roll(qbuf[g, s, :, 0:LANES], shift, 1)
        for j in range(tiles):
            following = pltpu.roll(qbuf[g, s, :, (j + 1) * LANES:(j + 2) * LANES], shift, 1)
            q = jnp.where(lane < LANES - offset, this, following)
            this = following
            p = z_ref[rows, tile_of(j)] * sc
            d = jnp.maximum(p - q, 0.0)
            if j == tiles - 1:
                d = jnp.where(lane < last, d, 0.0)
            z_ref[rows, tile_of(j)] = d
            z_sum = z_sum + d
            hit = lane_f == token - float(j * LANES)
            p_pick = jnp.where(hit, p, p_pick)
            q_pick = jnp.where(hit, q, q_pick)
        part[0, rows, :] = z_sum
        part[1, rows, :] = p_pick
        part[2, rows, :] = q_pick

    def z_copy(g, r, s):
        a, b = peer(r)
        return pltpu.make_async_remote_copy(
            src_ref=zmsg.at[g, me], dst_ref=zmsg.at[g, s], send_sem=zs_sem.at[g, r], recv_sem=zr_sem.at[g, s],
            device_id={"tpa": a, "tpb": b}, device_id_type=MESH)

    def phase(g, carry):
        sized(me, lambda width: own_copy(g, width).wait())
        excess(g, me)

        def one(i, c):
            r = jnp.where(g == phases - 1, i, n - i)
            a, b = peer(r)
            s = a * 4 + b
            sized(me, lambda width: q_arrival(g, s, width).wait_recv())
            excess(g, s)
            return c
        lax.fori_loop(1, n, one, 0)
        block = pl.ds(pl.multiple_of(g * (n * ROWS), n * ROWS), n * ROWS)
        sums = [jnp.sum(part[i, block, :].T, axis=0, keepdims=True) for i in range(3)]
        zmsg[g, me] = jnp.concatenate(sums + [jnp.zeros((1, LANES), jnp.float32)], axis=0)

        def send(r, c):
            z_copy(g, r, me).start()
            return c
        lax.fori_loop(1, n, send, 0)
        return carry
    lax.fori_loop(0, phases, phase, 0)

    def drain(i, c):
        g, r = lax.div(i, n), lax.rem(i, n)

        @pl.when(r > 0)
        def _():
            a, b = peer(r)
            sized(a * 4 + b, lambda width: q_copy(g, r, width).wait_send())

        @pl.when(jnp.logical_and(r > 0, g == 0))
        def _():
            stat_copy(r, me).wait_send()
        return c
    lax.fori_loop(0, phases * n, drain, 0)

    def collect(i, c):
        g, r = lax.div(i, n), lax.rem(i, n)

        @pl.when(r > 0)
        def _():
            a, b = peer(r)
            z_copy(g, r, me).wait_send()
            z_copy(g, r, a * 4 + b).wait_recv()
        return c
    lax.fori_loop(0, phases * n, collect, 0)
    for g in range(phases):
        total = zmsg[g, 0]
        for s in range(1, n):
            total = total + zmsg[g, s]
        tot_ref[g] = total


def finish_kernel(n, phases, vl, tot_ref, z_ref, res_ref, bonus_ref, accept_ref, expected_ref, inverse, staged, staged_bonus, sem, bonus_sem):
    width = n * ROWS
    num_draft = phases * ROWS
    for g in range(phases):
        inverse[g] = jnp.broadcast_to(1.0 / (tot_ref[g, 0:1, :] * SCALE), (width, LANES)).T

    def block_copy(b):
        return pltpu.make_async_copy(staged.at[b], res_ref.at[b], sem.at[b])

    def one(b, c):
        for g in range(phases):
            inv = inverse[g, pl.ds(pl.multiple_of(b * ROWS, ROWS), ROWS), :]
            rows = pl.ds(pl.multiple_of(g * width + b * ROWS, ROWS), ROWS)
            for j in range(pl.cdiv(vl, LANES)):
                w = min(LANES, vl - j * LANES)
                value = (z_ref[rows, j * LANES:(j + 1) * LANES] * SCALE) * inv
                staged[b, g * ROWS:(g + 1) * ROWS, j * LANES:j * LANES + w] = value[:, 0:w]
        block_copy(b).start()
        return c
    lax.fori_loop(0, n, one, 0)
    staged_bonus[...] = z_ref[phases * width:phases * width + n, 0:vl]
    bonus_copy = pltpu.make_async_copy(staged_bonus, bonus_ref, bonus_sem)
    bonus_copy.start()

    seq_of = lax.broadcasted_iota(jnp.int32, (n, width), 1) // ROWS == lax.broadcasted_iota(jnp.int32, (n, width), 0)
    pos_of = lax.broadcasted_iota(jnp.int32, (ROWS, width), 1) % ROWS == lax.broadcasted_iota(jnp.int32, (ROWS, width), 0)
    to_seq = (lax.broadcasted_iota(jnp.int32, (width, n), 0) // ROWS
              == lax.broadcasted_iota(jnp.int32, (width, n), 1)).astype(jnp.float32)
    by_seq = jnp.zeros((n, num_draft), jnp.float32)
    by_pos = []
    for g in range(phases):
        a = jnp.minimum(1.0, tot_ref[g, 1:2, :] / tot_ref[g, 2:3, :])
        to_pos = (lax.broadcasted_iota(jnp.int32, (width, num_draft), 0) % ROWS + g * ROWS
                  == lax.broadcasted_iota(jnp.int32, (width, num_draft), 1)).astype(jnp.float32)
        by_seq = by_seq + jnp.dot(jnp.where(seq_of, jnp.broadcast_to(a, (n, width)), 0.0), to_pos,
                                  precision=lax.Precision.HIGHEST, preferred_element_type=jnp.float32)
        by_pos.append(jnp.dot(jnp.where(pos_of, jnp.broadcast_to(a, (ROWS, width)), 0.0), to_seq,
                              precision=lax.Precision.HIGHEST, preferred_element_type=jnp.float32))
    accept_ref[...] = by_seq
    product = by_pos[0][0:1, :]
    total = product
    for k in range(1, num_draft):
        product = product * by_pos[k // ROWS][k % ROWS:k % ROWS + 1, :]
        total = total + product
    expected_ref[...] = total

    def finished(b, c):
        block_copy(b).wait()
        return c
    lax.fori_loop(0, n, finished, 0)
    bonus_copy.wait()


def solution(mesh):
    n = mesh.shape["tpa"] * mesh.shape["tpb"]

    def local_step(hidden, w_head, q_draft, x_draft):
        seqs, positions, depth = hidden.shape
        vl = w_head.shape[1]
        num_draft = x_draft.shape[1]
        phases = num_draft // ROWS
        vp = pl.cdiv(vl, LANES) * LANES
        rows = seqs * positions
        stat_rows = pl.cdiv(rows, LANES) * LANES
        f32 = jnp.float32
        any_spec = pl.BlockSpec(memory_space=pl.ANY)
        vmem_spec = pl.BlockSpec(memory_space=pltpu.VMEM)
        z, tot = pl.pallas_call(
            functools.partial(exchange_kernel, n, phases, vl),
            name="exchange",
            out_shape=(pltpu.VMEM((rows, vp), f32), pltpu.VMEM((phases, 4, LANES), f32)),
            in_specs=[any_spec] * 4,
            out_specs=(vmem_spec, vmem_spec),
            scratch_shapes=[
                pltpu.VMEM((rows, depth), jnp.bfloat16),
                pltpu.VMEM((rows, depth), jnp.bfloat16),
                pltpu.VMEM((W_BUFS, W_ROWS, depth), jnp.bfloat16),
                pltpu.VMEM((phases, n, ROWS, vp + LANES), f32),
                pltpu.VMEM((seqs, num_draft), jnp.int32),
                pltpu.VMEM((stat_rows, LANES), f32),
                pltpu.VMEM((stat_rows, LANES), f32),
                pltpu.VMEM((stat_rows, LANES), f32),
                pltpu.VMEM((3, phases * n * ROWS, LANES), f32),
                pltpu.VMEM((n, 2, stat_rows // LANES, LANES), f32),
                pltpu.VMEM((phases, n, 4, LANES), f32),
                pltpu.SemaphoreType.DMA((2,)),
                pltpu.SemaphoreType.DMA((W_BUFS,)),
                pltpu.SemaphoreType.DMA((phases, n)),
                pltpu.SemaphoreType.DMA((phases, n)),
                pltpu.SemaphoreType.DMA((n,)),
                pltpu.SemaphoreType.DMA((n,)),
                pltpu.SemaphoreType.DMA((phases, n)),
                pltpu.SemaphoreType.DMA((phases, n)),
            ],
            compiler_params=pltpu.CompilerParams(collective_id=0, has_side_effects=True, vmem_limit_bytes=48 * 2**20),
        )(hidden.transpose(1, 0, 2).reshape(rows, depth), w_head.T, q_draft.reshape(num_draft, q_draft.shape[2]), x_draft)
        residual, bonus, accept, expected = pl.pallas_call(
            functools.partial(finish_kernel, n, phases, vl),
            name="finish",
            out_shape=(jax.ShapeDtypeStruct((seqs, num_draft, vl), f32), jax.ShapeDtypeStruct((seqs, vl), f32),
                       jax.ShapeDtypeStruct((seqs, num_draft), f32), jax.ShapeDtypeStruct((1, seqs), f32)),
            in_specs=[vmem_spec, vmem_spec],
            out_specs=(any_spec, any_spec, vmem_spec, vmem_spec),
            scratch_shapes=[pltpu.VMEM((phases, n * ROWS, LANES), f32), pltpu.VMEM((seqs, num_draft, vl), f32),
                            pltpu.VMEM((seqs, vl), f32), pltpu.SemaphoreType.DMA((seqs,)), pltpu.SemaphoreType.DMA],
            compiler_params=pltpu.CompilerParams(vmem_limit_bytes=32 * 2**20),
        )(tot, z)
        return accept, expected.reshape(seqs), residual, bonus

    return jax.shard_map(
        local_step, mesh=mesh,
        in_specs=(P("dp", None, None), P(None, VOCAB_AXES), P(("dp",) + VOCAB_AXES, None, None), P("dp", None)),
        out_specs=(P("dp", None), P("dp"), P("dp", None, VOCAB_AXES), P("dp", VOCAB_AXES)),
        check_vma=False)
```

```python
import functools

import jax
import jax.numpy as jnp
from jax import lax
from jax.experimental import pallas as pl
from jax.experimental.pallas import tpu as pltpu
from jax.sharding import PartitionSpec as P

INV_TEMP = 1.25
VOCAB_AXES = ("tpa", "tpb")
MESH = pl.DeviceIdType.MESH
LANES = 128
ROWS = 8
W_ROWS = 256
W_BUFS = 4
SCALE = 2.0 ** 64


def xor4(a, r):
    low = lax.rem(lax.rem(a, 2) + lax.rem(r, 2), 2)
    high = lax.rem(lax.div(a, 2) + lax.div(r, 2), 2)
    return low + 2 * high


def exchange_kernel(n, phases, vl, hid_ref, w_ref, q_ref, x_ref, z_ref, tot_ref,
                    hid_v, hs, wbuf, sbuf, qbuf, x_v, colmax, colsum, scale, part, stat, zmsg,
                    in_sem, w_sem, ld_sem, qs_sem, qr_sem, ss_sem, sr_sem, zs_sem, zr_sem):
    vp = z_ref.shape[1]
    tiles = vp // LANES
    last = vl - (tiles - 1) * LANES
    rows_all = z_ref.shape[0]
    draft_rows = phases * n * ROWS
    my_a, my_b = lax.axis_index("tpa"), lax.axis_index("tpb")
    me = my_a * 4 + my_b
    lane = lax.broadcasted_iota(jnp.int32, (ROWS, LANES), 1)

    def peer(r):
        return xor4(my_a, lax.div(r, 4)), xor4(my_b, lax.rem(r, 4))

    def window(k):
        col = lax.div(k * vl, LANES) * LANES
        return pl.multiple_of(col, LANES), k * vl - col

    def sized(k, body):
        _, o = window(k)
        wide = o + vl > vp
        pl.when(wide)(lambda: body(vp + LANES))
        pl.when(jnp.logical_not(wide))(lambda: body(vp))

    core = lax.rem(my_b, 2)

    def nth(i):
        r = lax.rem((n // 2 + 1) * i + n // 2, n)
        far = lax.div(r, n // 2)
        return far * (n // 2 + lax.rem(r + core * (n // 4), n // 2)) + (1 - far) * r

    def width_of(g):
        return vp if g < phases - 1 else vp - LANES

    def load(g, k, width):
        col, _ = window(k)
        return pltpu.make_async_copy(q_ref.at[g * ROWS:(g + 1) * ROWS, pl.ds(col, width)], sbuf.at[g, k, :, pl.ds(0, width)], ld_sem.at[g, k])

    def q_copy(g, r, s):
        a, b = peer(r)
        return pltpu.make_async_remote_copy(
            src_ref=sbuf.at[g, a * 4 + b, :, pl.ds(0, width_of(g))], dst_ref=qbuf.at[g, s, :, pl.ds(0, width_of(g))],
            send_sem=qs_sem.at[g, r], recv_sem=qr_sem.at[g, s],
            device_id={"tpa": a, "tpb": b}, device_id_type=MESH)

    def tile_of(j):
        return slice(j * LANES, (j + 1) * LANES)

    free = LANES - last

    def prepare(g, k):
        _, o = window(k)
        shift = lax.rem(LANES - o, LANES)

        def last_tile(h):
            return jnp.where(lane < LANES - o, pltpu.roll(sbuf[h, k, :, tile_of(tiles - 1)], shift, 1),
                             pltpu.roll(sbuf[h, k, :, tile_of(tiles)], shift, 1))
        ending = last_tile(g)
        if g < phases - 1:
            guest = pltpu.roll(last_tile(phases - 1), last if g == 0 else LANES - (free - last) % LANES, 1)
            ending = jnp.where(lane < last, ending, guest)
        this = pltpu.roll(sbuf[g, k, :, tile_of(0)], shift, 1)
        for j in range(tiles - 1):
            following = pltpu.roll(sbuf[g, k, :, tile_of(j + 1)], shift, 1)
            sbuf[g, k, :, tile_of(j)] = jnp.where(lane < LANES - o, this, following)
            this = following
        sbuf[g, k, :, tile_of(tiles - 1)] = ending

    def send_phase(g):
        def one(i, c):
            @pl.when(i < n)
            def _():
                r = nth(i)
                a, b = peer(r)
                k = a * 4 + b
                if g == 0:
                    sized(k, lambda width: load(0, k, width).wait())
                    sized(k, lambda width: load(phases - 1, k, width).wait())
                elif g < phases - 1:
                    sized(k, lambda width: load(g, k, width).wait())
                prepare(g, k)

                @pl.when(r == 0)
                def _():
                    for j in range(tiles):
                        qbuf[g, me, :, tile_of(j)] = sbuf[g, me, :, tile_of(j)]

            @pl.when(i > 0)
            def _():
                before = nth(i - 1)

                @pl.when(before > 0)
                def _():
                    q_copy(g, before, me).start()
            return c
        lax.fori_loop(0, n + 1, one, 0)

    def w_copy(c, slot):
        return pltpu.make_async_copy(w_ref.at[pl.ds(pl.multiple_of(c * W_ROWS, W_ROWS), W_ROWS), :], wbuf.at[slot], w_sem.at[slot])

    full_chunks = vl // W_ROWS
    w_tail = vl - full_chunks * W_ROWS
    tail_slot = full_chunks % W_BUFS
    tail_copy = pltpu.make_async_copy(
        w_ref.at[pl.ds(full_chunks * W_ROWS, w_tail), :], wbuf.at[tail_slot, pl.ds(0, w_tail), :], w_sem.at[tail_slot])

    hid_copy = pltpu.make_async_copy(hid_ref, hid_v, in_sem.at[0])
    x_copy = pltpu.make_async_copy(x_ref, x_v, in_sem.at[1])
    def start_load(g):
        def one(i, c):
            a, b = peer(nth(i))
            k = a * 4 + b
            sized(k, lambda width: load(g, k, width).start())
            if g == 0:
                sized(k, lambda width: load(phases - 1, k, width).start())
            return c
        lax.fori_loop(0, n, one, 0)
    for g in range(phases - 1):
        start_load(g)
    hid_copy.start()
    x_copy.start()
    for c in range(W_BUFS):
        w_copy(c, c).start()

    barrier = pltpu.get_barrier_semaphore()

    def greet(r, c):
        a, b = peer(r)
        pl.semaphore_signal(barrier, inc=1, device_id={"tpa": a, "tpb": b}, device_id_type=MESH)
        return c
    lax.fori_loop(1, n, greet, 0)
    pl.semaphore_wait(barrier, n - 1)

    send_phase(0)
    send_phase(1)

    hid_copy.wait()
    row = lax.broadcasted_iota(jnp.int32, (rows_all, rows_all), 0)
    col = lax.broadcasted_iota(jnp.int32, (rows_all, rows_all), 1)
    source = jnp.where(row < draft_rows, ((row // (n * ROWS)) * ROWS + row % ROWS) * n + (row // ROWS) % n, row)
    permute = jnp.where(col == source, 1.0, 0.0).astype(jnp.bfloat16)
    depth = hid_v.shape[1]

    def permute_columns(c, carry):
        at = pl.ds(pl.multiple_of(c * 256, 256), 256)
        hs[:, at] = jnp.dot(permute, hid_v[:, at], preferred_element_type=jnp.float32).astype(jnp.bfloat16)
        return carry
    lax.fori_loop(0, depth // 256, permute_columns, 0)

    nt = (((1,), (1,)), ((), ()))

    def logits(c, carry):
        slot = lax.rem(c, W_BUFS)
        w_copy(c, slot).wait()
        z_ref[:, pl.ds(pl.multiple_of(c * W_ROWS, W_ROWS), W_ROWS)] = lax.dot_general(
            hs[...], wbuf[slot], nt, preferred_element_type=jnp.float32) * INV_TEMP

        @pl.when(c + W_BUFS < full_chunks)
        def _():
            w_copy(c + W_BUFS, slot).start()

        @pl.when(c + W_BUFS == full_chunks)
        def _():
            tail_copy.start()
        return carry
    lax.fori_loop(0, full_chunks, logits, 0)
    tail_copy.wait()
    z_ref[:, full_chunks * W_ROWS:vl] = lax.dot_general(
        hs[...], wbuf[tail_slot, 0:w_tail, :], nt, preferred_element_type=jnp.float32) * INV_TEMP

    def row_stats(t, carry):
        rows = pl.ds(pl.multiple_of(t * ROWS, ROWS), ROWS)
        m = jnp.where(lane < last, z_ref[rows, tile_of(tiles - 1)], -jnp.inf)
        for j in range(tiles - 1):
            m = jnp.maximum(m, z_ref[rows, tile_of(j)])
        m = jnp.broadcast_to(jnp.max(m, axis=1, keepdims=True), (ROWS, LANES))
        s = jnp.zeros((ROWS, LANES), jnp.float32)
        for j in range(tiles):
            e = jnp.exp(z_ref[rows, tile_of(j)] - m)
            if j == tiles - 1:
                e = jnp.where(lane < last, e, 0.0)
            z_ref[rows, tile_of(j)] = e
            s = s + e
        colmax[rows, :] = m
        colsum[rows, :] = jnp.broadcast_to(jnp.sum(s, axis=1, keepdims=True), (ROWS, LANES))
        return carry
    lax.fori_loop(0, rows_all // ROWS, row_stats, 0)
    spare = colmax.shape[0] - rows_all
    colmax[rows_all:, :] = jnp.zeros((spare, LANES), jnp.float32)
    colsum[rows_all:, :] = jnp.ones((spare, LANES), jnp.float32)

    blocks = colmax.shape[0] // LANES

    def as_rows(ref):
        return jnp.concatenate([ref[i * LANES:(i + 1) * LANES, :].T[0:1, :] for i in range(blocks)], axis=0)
    stat[me, 0] = as_rows(colmax)
    stat[me, 1] = as_rows(colsum)

    def stat_copy(r, s):
        a, b = peer(r)
        return pltpu.make_async_remote_copy(
            src_ref=stat.at[me], dst_ref=stat.at[s], send_sem=ss_sem.at[r], recv_sem=sr_sem.at[s],
            device_id={"tpa": a, "tpb": b}, device_id_type=MESH)

    def send_stat(r, c):
        stat_copy(r, me).start()
        return c
    lax.fori_loop(1, n, send_stat, 0)
    send_phase(2)

    def wait_stat(r, c):
        a, b = peer(r)
        stat_copy(r, a * 4 + b).wait_recv()
        return c
    lax.fori_loop(1, n, wait_stat, 0)
    glob_max = stat[0, 0]
    for s in range(1, n):
        glob_max = jnp.maximum(glob_max, stat[s, 0])
    glob_sum = jnp.zeros_like(glob_max)
    for s in range(n):
        glob_sum = glob_sum + stat[s, 1] * jnp.exp(stat[s, 0] - glob_max)
    factor = jnp.exp(stat[me, 0] - glob_max) / glob_sum
    for i in range(blocks):
        scale[i * LANES:(i + 1) * LANES, :] = jnp.broadcast_to(factor[i:i + 1, :], (LANES, LANES)).T

    for t in range(draft_rows // ROWS, rows_all // ROWS):
        rows = slice(t * ROWS, (t + 1) * ROWS)
        for j in range(tiles):
            z_ref[rows, tile_of(j)] = z_ref[rows, tile_of(j)] * scale[rows, :]

    x_copy.wait()
    lane_f = lane.astype(jnp.float32)
    num_draft = x_v.shape[1]

    def excess(g, s):
        rows = pl.ds(pl.multiple_of(g * (n * ROWS) + s * ROWS, ROWS), ROWS)
        tokens = jnp.broadcast_to(x_v[pl.ds(s, 1), :].astype(jnp.float32), (ROWS, num_draft))
        position = lax.broadcasted_iota(jnp.int32, (ROWS, num_draft), 0) + g * ROWS
        here = lax.broadcasted_iota(jnp.int32, (ROWS, num_draft), 1) == position
        token = jnp.sum(jnp.where(here, tokens, 0.0), axis=1, keepdims=True) - (me * vl).astype(jnp.float32)
        token = jnp.broadcast_to(jnp.where(token < vl, token, -1.0), (ROWS, LANES))
        sc = scale[rows, :]
        z_sum = p_pick = q_pick = jnp.zeros((ROWS, LANES), jnp.float32)
        for j in range(tiles):
            if g == phases - 1 and j == tiles - 1:
                q = jnp.where(lane < free, pltpu.roll(qbuf[0, s, :, tile_of(j)], free, 1),
                              pltpu.roll(qbuf[1, s, :, tile_of(j)], (free - last) % LANES, 1))
            else:
                q = qbuf[g, s, :, tile_of(j)]
            p = z_ref[rows, tile_of(j)] * sc
            d = jnp.maximum(p - q, 0.0)
            if j == tiles - 1:
                d = jnp.where(lane < last, d, 0.0)
            z_ref[rows, tile_of(j)] = d
            z_sum = z_sum + d
            hit = lane_f == token - float(j * LANES)
            p_pick = jnp.where(hit, p, p_pick)
            q_pick = jnp.where(hit, q, q_pick)
        part[0, rows, :] = z_sum
        part[1, rows, :] = p_pick
        part[2, rows, :] = q_pick

    def z_copy(g, r, s):
        a, b = peer(r)
        return pltpu.make_async_remote_copy(
            src_ref=zmsg.at[g, me], dst_ref=zmsg.at[g, s], send_sem=zs_sem.at[g, r], recv_sem=zr_sem.at[g, s],
            device_id={"tpa": a, "tpb": b}, device_id_type=MESH)

    def add_up(g):
        def arrived(r, c):
            a, b = peer(r)
            z_copy(g, r, a * 4 + b).wait_recv()
            return c
        lax.fori_loop(1, n, arrived, 0)
        total = zmsg[g, 0]
        for s in range(1, n):
            total = total + zmsg[g, s]
        tot_ref[g] = total

    for g in range(phases):
        def one(i, c, g=g):
            r = nth(i)
            a, b = peer(r)
            s = a * 4 + b

            @pl.when(r > 0)
            def _():
                q_copy(g, r, s).wait_recv()
            excess(g, s)
            return c
        lax.fori_loop(0, n, one, 0)
        block = slice(g * n * ROWS, (g + 1) * n * ROWS)
        zmsg[g, me] = jnp.concatenate([jnp.sum(part[i, block, :].T, axis=0, keepdims=True) for i in range(3)], axis=0)

        def send(r, c, g=g):
            z_copy(g, r, me).start()
            return c
        lax.fori_loop(1, n, send, 0)

    def drain(r, c):
        for g in range(phases):
            q_copy(g, r, me).wait_send()
            z_copy(g, r, me).wait_send()
        stat_copy(r, me).wait_send()
        return c
    lax.fori_loop(1, n, drain, 0)
    for g in range(phases):
        add_up(g)


def finish_kernel(n, phases, vl, tot_ref, z_ref, res_ref, bonus_ref, accept_ref, expected_ref, inverse, staged, staged_bonus, sem, bonus_sem):
    width = n * ROWS
    num_draft = phases * ROWS
    for g in range(phases):
        inverse[g] = jnp.broadcast_to(1.0 / (tot_ref[g, 0:1, :] * SCALE), (width, LANES)).T

    def block_copy(b):
        return pltpu.make_async_copy(staged.at[b], res_ref.at[b], sem.at[b])

    def one(b, c):
        for g in range(phases):
            inv = inverse[g, pl.ds(pl.multiple_of(b * ROWS, ROWS), ROWS), :]
            rows = pl.ds(pl.multiple_of(g * width + b * ROWS, ROWS), ROWS)
            for j in range(pl.cdiv(vl, LANES)):
                w = min(LANES, vl - j * LANES)
                value = (z_ref[rows, j * LANES:(j + 1) * LANES] * SCALE) * inv
                staged[b, g * ROWS:(g + 1) * ROWS, j * LANES:j * LANES + w] = value[:, 0:w]
        block_copy(b).start()
        return c
    lax.fori_loop(0, n, one, 0)
    staged_bonus[...] = z_ref[phases * width:phases * width + n, 0:vl]
    bonus_copy = pltpu.make_async_copy(staged_bonus, bonus_ref, bonus_sem)
    bonus_copy.start()

    seq_of = lax.broadcasted_iota(jnp.int32, (n, width), 1) // ROWS == lax.broadcasted_iota(jnp.int32, (n, width), 0)
    pos_of = lax.broadcasted_iota(jnp.int32, (ROWS, width), 1) % ROWS == lax.broadcasted_iota(jnp.int32, (ROWS, width), 0)
    to_seq = (lax.broadcasted_iota(jnp.int32, (width, n), 0) // ROWS
              == lax.broadcasted_iota(jnp.int32, (width, n), 1)).astype(jnp.float32)
    by_seq = jnp.zeros((n, num_draft), jnp.float32)
    by_pos = []
    for g in range(phases):
        a = jnp.minimum(1.0, tot_ref[g, 1:2, :] / tot_ref[g, 2:3, :])
        to_pos = (lax.broadcasted_iota(jnp.int32, (width, num_draft), 0) % ROWS + g * ROWS
                  == lax.broadcasted_iota(jnp.int32, (width, num_draft), 1)).astype(jnp.float32)
        by_seq = by_seq + jnp.dot(jnp.where(seq_of, jnp.broadcast_to(a, (n, width)), 0.0), to_pos,
                                  precision=lax.Precision.HIGHEST, preferred_element_type=jnp.float32)
        by_pos.append(jnp.dot(jnp.where(pos_of, jnp.broadcast_to(a, (ROWS, width)), 0.0), to_seq,
                              precision=lax.Precision.HIGHEST, preferred_element_type=jnp.float32))
    accept_ref[...] = by_seq
    product = by_pos[0][0:1, :]
    total = product
    for k in range(1, num_draft):
        product = product * by_pos[k // ROWS][k % ROWS:k % ROWS + 1, :]
        total = total + product
    expected_ref[...] = total

    def finished(b, c):
        block_copy(b).wait()
        return c
    lax.fori_loop(0, n, finished, 0)
    bonus_copy.wait()


def solution(mesh):
    n = mesh.shape["tpa"] * mesh.shape["tpb"]

    def local_step(hidden, w_head, q_draft, x_draft):
        seqs, positions, depth = hidden.shape
        vl = w_head.shape[1]
        num_draft = x_draft.shape[1]
        phases = num_draft // ROWS
        vp = pl.cdiv(vl, LANES) * LANES
        rows = seqs * positions
        stat_rows = pl.cdiv(rows, LANES) * LANES
        f32 = jnp.float32
        any_spec = pl.BlockSpec(memory_space=pl.ANY)
        vmem_spec = pl.BlockSpec(memory_space=pltpu.VMEM)
        z, tot = pl.pallas_call(
            functools.partial(exchange_kernel, n, phases, vl),
            name="exchange",
            out_shape=(pltpu.VMEM((rows, vp), f32), pltpu.VMEM((phases, 3, LANES), f32)),
            in_specs=[any_spec] * 4,
            out_specs=(vmem_spec, vmem_spec),
            scratch_shapes=[
                pltpu.VMEM((rows, depth), jnp.bfloat16),
                pltpu.VMEM((rows, depth), jnp.bfloat16),
                pltpu.VMEM((W_BUFS, W_ROWS, depth), jnp.bfloat16),
                pltpu.VMEM((phases, n, ROWS, vp + LANES), f32),
                pltpu.VMEM((phases, n, ROWS, vp), f32),
                pltpu.VMEM((seqs, num_draft), jnp.int32),
                pltpu.VMEM((stat_rows, LANES), f32),
                pltpu.VMEM((stat_rows, LANES), f32),
                pltpu.VMEM((stat_rows, LANES), f32),
                pltpu.VMEM((3, phases * n * ROWS, LANES), f32),
                pltpu.VMEM((n, 2, stat_rows // LANES, LANES), f32),
                pltpu.VMEM((phases, n, 3, LANES), f32),
                pltpu.SemaphoreType.DMA((2,)),
                pltpu.SemaphoreType.DMA((W_BUFS,)),
                pltpu.SemaphoreType.DMA((phases, n)),
                pltpu.SemaphoreType.DMA((phases, n)),
                pltpu.SemaphoreType.DMA((phases, n)),
                pltpu.SemaphoreType.DMA((n,)),
                pltpu.SemaphoreType.DMA((n,)),
                pltpu.SemaphoreType.DMA((phases, n)),
                pltpu.SemaphoreType.DMA((phases, n)),
            ],
            compiler_params=pltpu.CompilerParams(collective_id=0, has_side_effects=True, vmem_limit_bytes=48 * 2**20),
        )(hidden.transpose(1, 0, 2).reshape(rows, depth), w_head.T, q_draft.reshape(num_draft, q_draft.shape[2]), x_draft)
        residual, bonus, accept, expected = pl.pallas_call(
            functools.partial(finish_kernel, n, phases, vl),
            name="finish",
            out_shape=(jax.ShapeDtypeStruct((seqs, num_draft, vl), f32), jax.ShapeDtypeStruct((seqs, vl), f32),
                       jax.ShapeDtypeStruct((seqs, num_draft), f32), jax.ShapeDtypeStruct((1, seqs), f32)),
            in_specs=[vmem_spec, vmem_spec],
            out_specs=(any_spec, any_spec, vmem_spec, vmem_spec),
            scratch_shapes=[pltpu.VMEM((phases, n * ROWS, LANES), f32), pltpu.VMEM((seqs, num_draft, vl), f32),
                            pltpu.VMEM((seqs, vl), f32), pltpu.SemaphoreType.DMA((seqs,)), pltpu.SemaphoreType.DMA],
            compiler_params=pltpu.CompilerParams(vmem_limit_bytes=32 * 2**20),
        )(tot, z)
        return accept, expected.reshape(seqs), residual, bonus

    return jax.shard_map(
        local_step, mesh=mesh,
        in_specs=(P("dp", None, None), P(None, VOCAB_AXES), P(("dp",) + VOCAB_AXES, None, None), P("dp", None)),
        out_specs=(P("dp", None), P("dp"), P("dp", None, VOCAB_AXES), P("dp", VOCAB_AXES)),
        check_vma=False)
```

```python
import functools

import jax
import jax.numpy as jnp
from jax import lax
from jax.experimental import pallas as pl
from jax.experimental.pallas import tpu as pltpu
from jax.sharding import PartitionSpec as P

INV_TEMP = 1.25
VOCAB_AXES = ("tpa", "tpb")
MESH = pl.DeviceIdType.MESH
LANES = 128
ROWS = 8
W_ROWS = 256
W_BUFS = 4
SCALE = 2.0 ** 64


def xor4(a, r):
    low = lax.rem(lax.rem(a, 2) + lax.rem(r, 2), 2)
    high = lax.rem(lax.div(a, 2) + lax.div(r, 2), 2)
    return low + 2 * high


def exchange_kernel(n, phases, vl, hid_ref, w_ref, q_ref, x_ref, z_ref, tot_ref,
                    hid_v, hs, wbuf, sbuf, qbuf, x_v, colmax, colsum, scale, part, stat, zmsg,
                    in_sem, w_sem, ld_sem, qs_sem, qr_sem, ss_sem, sr_sem, zs_sem, zr_sem):
    vp = z_ref.shape[1]
    tiles = vp // LANES
    last = vl - (tiles - 1) * LANES
    rows_all = z_ref.shape[0]
    draft_rows = phases * n * ROWS
    my_a, my_b = lax.axis_index("tpa"), lax.axis_index("tpb")
    me = my_a * 4 + my_b
    lane = lax.broadcasted_iota(jnp.int32, (ROWS, LANES), 1)

    def peer(r):
        return xor4(my_a, lax.div(r, 4)), xor4(my_b, lax.rem(r, 4))

    def window(k):
        col = lax.div(k * vl, LANES) * LANES
        return pl.multiple_of(col, LANES), k * vl - col

    def sized(k, body):
        _, o = window(k)
        wide = o + vl > vp
        pl.when(wide)(lambda: body(vp + LANES))
        pl.when(jnp.logical_not(wide))(lambda: body(vp))

    core = lax.rem(my_b, 2)
    inner = lax.rem(lax.div(my_a + 1, 2), 2)

    def nth(i):
        return inner * lax.rem((n // 2 + 1) * (i + core) + n // 2, n) + (1 - inner) * i

    def width_of(g):
        return vp if g < phases - 1 else vp - LANES

    def load(g, k, width):
        col, _ = window(k)
        return pltpu.make_async_copy(q_ref.at[g * ROWS:(g + 1) * ROWS, pl.ds(col, width)], sbuf.at[g, k, :, pl.ds(0, width)], ld_sem.at[g, k])

    def q_copy(g, r, s):
        a, b = peer(r)
        return pltpu.make_async_remote_copy(
            src_ref=sbuf.at[g, a * 4 + b, :, pl.ds(0, width_of(g))], dst_ref=qbuf.at[g, s, :, pl.ds(0, width_of(g))],
            send_sem=qs_sem.at[g, r], recv_sem=qr_sem.at[g, s],
            device_id={"tpa": a, "tpb": b}, device_id_type=MESH)

    def tile_of(j):
        return slice(j * LANES, (j + 1) * LANES)

    free = LANES - last

    def prepare(g, k):
        _, o = window(k)
        shift = lax.rem(LANES - o, LANES)

        def last_tile(h):
            return jnp.where(lane < LANES - o, pltpu.roll(sbuf[h, k, :, tile_of(tiles - 1)], shift, 1),
                             pltpu.roll(sbuf[h, k, :, tile_of(tiles)], shift, 1))
        ending = last_tile(g)
        if g < phases - 1:
            guest = pltpu.roll(last_tile(phases - 1), last if g == 0 else LANES - (free - last) % LANES, 1)
            ending = jnp.where(lane < last, ending, guest)
        this = pltpu.roll(sbuf[g, k, :, tile_of(0)], shift, 1)
        for j in range(tiles - 1):
            following = pltpu.roll(sbuf[g, k, :, tile_of(j + 1)], shift, 1)
            sbuf[g, k, :, tile_of(j)] = jnp.where(lane < LANES - o, this, following)
            this = following
        sbuf[g, k, :, tile_of(tiles - 1)] = ending

    def send_phase(g):
        def one(i, c):
            @pl.when(i < n)
            def _():
                r = nth(i)
                a, b = peer(r)
                k = a * 4 + b
                if g == 0:
                    sized(k, lambda width: load(0, k, width).wait())
                    sized(k, lambda width: load(phases - 1, k, width).wait())
                elif g < phases - 1:
                    sized(k, lambda width: load(g, k, width).wait())
                prepare(g, k)

                @pl.when(r == 0)
                def _():
                    for j in range(tiles):
                        qbuf[g, me, :, tile_of(j)] = sbuf[g, me, :, tile_of(j)]

            @pl.when(i > 0)
            def _():
                before = nth(i - 1)

                @pl.when(before > 0)
                def _():
                    q_copy(g, before, me).start()
            return c
        lax.fori_loop(0, n + 1, one, 0)

    def w_copy(c, slot):
        return pltpu.make_async_copy(w_ref.at[pl.ds(pl.multiple_of(c * W_ROWS, W_ROWS), W_ROWS), :], wbuf.at[slot], w_sem.at[slot])

    full_chunks = vl // W_ROWS
    w_tail = vl - full_chunks * W_ROWS
    tail_slot = full_chunks % W_BUFS
    tail_copy = pltpu.make_async_copy(
        w_ref.at[pl.ds(full_chunks * W_ROWS, w_tail), :], wbuf.at[tail_slot, pl.ds(0, w_tail), :], w_sem.at[tail_slot])

    hid_copy = pltpu.make_async_copy(hid_ref, hid_v, in_sem.at[0])
    x_copy = pltpu.make_async_copy(x_ref, x_v, in_sem.at[1])
    def start_load(g):
        def one(i, c):
            a, b = peer(nth(i))
            k = a * 4 + b
            sized(k, lambda width: load(g, k, width).start())
            if g == 0:
                sized(k, lambda width: load(phases - 1, k, width).start())
            return c
        lax.fori_loop(0, n, one, 0)
    for g in range(phases - 1):
        start_load(g)
    hid_copy.start()
    x_copy.start()
    for c in range(W_BUFS):
        w_copy(c, c).start()

    barrier = pltpu.get_barrier_semaphore()

    def greet(r, c):
        a, b = peer(r)
        pl.semaphore_signal(barrier, inc=1, device_id={"tpa": a, "tpb": b}, device_id_type=MESH)
        return c
    lax.fori_loop(1, n, greet, 0)
    pl.semaphore_wait(barrier, n - 1)

    send_phase(0)
    send_phase(1)

    hid_copy.wait()
    row = lax.broadcasted_iota(jnp.int32, (rows_all, rows_all), 0)
    col = lax.broadcasted_iota(jnp.int32, (rows_all, rows_all), 1)
    source = jnp.where(row < draft_rows, ((row // (n * ROWS)) * ROWS + row % ROWS) * n + (row // ROWS) % n, row)
    permute = jnp.where(col == source, 1.0, 0.0).astype(jnp.bfloat16)
    depth = hid_v.shape[1]

    def permute_columns(c, carry):
        at = pl.ds(pl.multiple_of(c * 256, 256), 256)
        hs[:, at] = jnp.dot(permute, hid_v[:, at], preferred_element_type=jnp.float32).astype(jnp.bfloat16)
        return carry
    lax.fori_loop(0, depth // 256, permute_columns, 0)

    nt = (((1,), (1,)), ((), ()))

    def logits(c, carry):
        slot = lax.rem(c, W_BUFS)
        w_copy(c, slot).wait()
        z_ref[:, pl.ds(pl.multiple_of(c * W_ROWS, W_ROWS), W_ROWS)] = lax.dot_general(
            hs[...], wbuf[slot], nt, preferred_element_type=jnp.float32) * INV_TEMP

        @pl.when(c + W_BUFS < full_chunks)
        def _():
            w_copy(c + W_BUFS, slot).start()

        @pl.when(c + W_BUFS == full_chunks)
        def _():
            tail_copy.start()
        return carry
    lax.fori_loop(0, full_chunks, logits, 0)
    tail_copy.wait()
    z_ref[:, full_chunks * W_ROWS:vl] = lax.dot_general(
        hs[...], wbuf[tail_slot, 0:w_tail, :], nt, preferred_element_type=jnp.float32) * INV_TEMP

    def row_stats(t, carry):
        rows = pl.ds(pl.multiple_of(t * ROWS, ROWS), ROWS)
        m = jnp.where(lane < last, z_ref[rows, tile_of(tiles - 1)], -jnp.inf)
        for j in range(tiles - 1):
            m = jnp.maximum(m, z_ref[rows, tile_of(j)])
        m = jnp.broadcast_to(jnp.max(m, axis=1, keepdims=True), (ROWS, LANES))
        s = jnp.zeros((ROWS, LANES), jnp.float32)
        for j in range(tiles):
            e = jnp.exp(z_ref[rows, tile_of(j)] - m)
            if j == tiles - 1:
                e = jnp.where(lane < last, e, 0.0)
            z_ref[rows, tile_of(j)] = e
            s = s + e
        colmax[rows, :] = m
        colsum[rows, :] = jnp.broadcast_to(jnp.sum(s, axis=1, keepdims=True), (ROWS, LANES))
        return carry
    lax.fori_loop(0, rows_all // ROWS, row_stats, 0)
    spare = colmax.shape[0] - rows_all
    colmax[rows_all:, :] = jnp.zeros((spare, LANES), jnp.float32)
    colsum[rows_all:, :] = jnp.ones((spare, LANES), jnp.float32)

    blocks = colmax.shape[0] // LANES

    def as_rows(ref):
        return jnp.concatenate([ref[i * LANES:(i + 1) * LANES, :].T[0:1, :] for i in range(blocks)], axis=0)
    stat[me, 0] = as_rows(colmax)
    stat[me, 1] = as_rows(colsum)

    def stat_copy(r, s):
        a, b = peer(r)
        return pltpu.make_async_remote_copy(
            src_ref=stat.at[me], dst_ref=stat.at[s], send_sem=ss_sem.at[r], recv_sem=sr_sem.at[s],
            device_id={"tpa": a, "tpb": b}, device_id_type=MESH)

    def send_stat(r, c):
        stat_copy(r, me).start()
        return c
    lax.fori_loop(1, n, send_stat, 0)
    send_phase(2)

    def wait_stat(r, c):
        a, b = peer(r)
        stat_copy(r, a * 4 + b).wait_recv()
        return c
    lax.fori_loop(1, n, wait_stat, 0)
    glob_max = stat[0, 0]
    for s in range(1, n):
        glob_max = jnp.maximum(glob_max, stat[s, 0])
    glob_sum = jnp.zeros_like(glob_max)
    for s in range(n):
        glob_sum = glob_sum + stat[s, 1] * jnp.exp(stat[s, 0] - glob_max)
    factor = jnp.exp(stat[me, 0] - glob_max) / glob_sum
    for i in range(blocks):
        scale[i * LANES:(i + 1) * LANES, :] = jnp.broadcast_to(factor[i:i + 1, :], (LANES, LANES)).T

    for t in range(draft_rows // ROWS, rows_all // ROWS):
        rows = slice(t * ROWS, (t + 1) * ROWS)
        for j in range(tiles):
            z_ref[rows, tile_of(j)] = z_ref[rows, tile_of(j)] * scale[rows, :]

    x_copy.wait()
    lane_f = lane.astype(jnp.float32)
    num_draft = x_v.shape[1]

    def excess(g, s):
        rows = pl.ds(pl.multiple_of(g * (n * ROWS) + s * ROWS, ROWS), ROWS)
        tokens = jnp.broadcast_to(x_v[pl.ds(s, 1), :].astype(jnp.float32), (ROWS, num_draft))
        position = lax.broadcasted_iota(jnp.int32, (ROWS, num_draft), 0) + g * ROWS
        here = lax.broadcasted_iota(jnp.int32, (ROWS, num_draft), 1) == position
        token = jnp.sum(jnp.where(here, tokens, 0.0), axis=1, keepdims=True) - (me * vl).astype(jnp.float32)
        token = jnp.broadcast_to(jnp.where(token < vl, token, -1.0), (ROWS, LANES))
        sc = scale[rows, :]
        z_sum = p_pick = q_pick = jnp.zeros((ROWS, LANES), jnp.float32)
        for j in range(tiles):
            if g == phases - 1 and j == tiles - 1:
                q = jnp.where(lane < free, pltpu.roll(qbuf[0, s, :, tile_of(j)], free, 1),
                              pltpu.roll(qbuf[1, s, :, tile_of(j)], (free - last) % LANES, 1))
            else:
                q = qbuf[g, s, :, tile_of(j)]
            p = z_ref[rows, tile_of(j)] * sc
            d = jnp.maximum(p - q, 0.0)
            if j == tiles - 1:
                d = jnp.where(lane < last, d, 0.0)
            z_ref[rows, tile_of(j)] = d
            z_sum = z_sum + d
            hit = lane_f == token - float(j * LANES)
            p_pick = jnp.where(hit, p, p_pick)
            q_pick = jnp.where(hit, q, q_pick)
        part[0, rows, :] = z_sum
        part[1, rows, :] = p_pick
        part[2, rows, :] = q_pick

    def z_copy(g, r, s):
        a, b = peer(r)
        return pltpu.make_async_remote_copy(
            src_ref=zmsg.at[g, me], dst_ref=zmsg.at[g, s], send_sem=zs_sem.at[g, r], recv_sem=zr_sem.at[g, s],
            device_id={"tpa": a, "tpb": b}, device_id_type=MESH)

    def add_up(g):
        def arrived(r, c):
            a, b = peer(r)
            z_copy(g, r, a * 4 + b).wait_recv()
            return c
        lax.fori_loop(1, n, arrived, 0)
        total = zmsg[g, 0]
        for s in range(1, n):
            total = total + zmsg[g, s]
        tot_ref[g] = total

    for g in range(phases):
        def one(i, c, g=g):
            a, b = peer(i)
            s = a * 4 + b

            @pl.when(i > 0)
            def _():
                q_copy(g, i, s).wait_recv()
            excess(g, s)
            return c
        lax.fori_loop(0, n, one, 0)
        block = slice(g * n * ROWS, (g + 1) * n * ROWS)
        zmsg[g, me] = jnp.concatenate([jnp.sum(part[i, block, :].T, axis=0, keepdims=True) for i in range(3)], axis=0)

        def send(r, c, g=g):
            z_copy(g, r, me).start()
            return c
        lax.fori_loop(1, n, send, 0)

    def drain(r, c):
        for g in range(phases):
            q_copy(g, r, me).wait_send()
            z_copy(g, r, me).wait_send()
        stat_copy(r, me).wait_send()
        return c
    lax.fori_loop(1, n, drain, 0)
    for g in range(phases):
        add_up(g)


def finish_kernel(n, phases, vl, tot_ref, z_ref, res_ref, bonus_ref, accept_ref, expected_ref, inverse, staged, staged_bonus, sem, bonus_sem):
    width = n * ROWS
    num_draft = phases * ROWS
    for g in range(phases):
        inverse[g] = jnp.broadcast_to(1.0 / (tot_ref[g, 0:1, :] * SCALE), (width, LANES)).T

    def block_copy(b):
        return pltpu.make_async_copy(staged.at[b], res_ref.at[b], sem.at[b])

    def one(b, c):
        for g in range(phases):
            inv = inverse[g, pl.ds(pl.multiple_of(b * ROWS, ROWS), ROWS), :]
            rows = pl.ds(pl.multiple_of(g * width + b * ROWS, ROWS), ROWS)
            for j in range(pl.cdiv(vl, LANES)):
                w = min(LANES, vl - j * LANES)
                value = (z_ref[rows, j * LANES:(j + 1) * LANES] * SCALE) * inv
                staged[b, g * ROWS:(g + 1) * ROWS, j * LANES:j * LANES + w] = value[:, 0:w]
        block_copy(b).start()
        return c
    lax.fori_loop(0, n, one, 0)
    staged_bonus[...] = z_ref[phases * width:phases * width + n, 0:vl]
    bonus_copy = pltpu.make_async_copy(staged_bonus, bonus_ref, bonus_sem)
    bonus_copy.start()

    seq_of = lax.broadcasted_iota(jnp.int32, (n, width), 1) // ROWS == lax.broadcasted_iota(jnp.int32, (n, width), 0)
    pos_of = lax.broadcasted_iota(jnp.int32, (ROWS, width), 1) % ROWS == lax.broadcasted_iota(jnp.int32, (ROWS, width), 0)
    to_seq = (lax.broadcasted_iota(jnp.int32, (width, n), 0) // ROWS
              == lax.broadcasted_iota(jnp.int32, (width, n), 1)).astype(jnp.float32)
    by_seq = jnp.zeros((n, num_draft), jnp.float32)
    by_pos = []
    for g in range(phases):
        a = jnp.minimum(1.0, tot_ref[g, 1:2, :] / tot_ref[g, 2:3, :])
        to_pos = (lax.broadcasted_iota(jnp.int32, (width, num_draft), 0) % ROWS + g * ROWS
                  == lax.broadcasted_iota(jnp.int32, (width, num_draft), 1)).astype(jnp.float32)
        by_seq = by_seq + jnp.dot(jnp.where(seq_of, jnp.broadcast_to(a, (n, width)), 0.0), to_pos,
                                  precision=lax.Precision.HIGHEST, preferred_element_type=jnp.float32)
        by_pos.append(jnp.dot(jnp.where(pos_of, jnp.broadcast_to(a, (ROWS, width)), 0.0), to_seq,
                              precision=lax.Precision.HIGHEST, preferred_element_type=jnp.float32))
    accept_ref[...] = by_seq
    product = by_pos[0][0:1, :]
    total = product
    for k in range(1, num_draft):
        product = product * by_pos[k // ROWS][k % ROWS:k % ROWS + 1, :]
        total = total + product
    expected_ref[...] = total

    def finished(b, c):
        block_copy(b).wait()
        return c
    lax.fori_loop(0, n, finished, 0)
    bonus_copy.wait()


def solution(mesh):
    n = mesh.shape["tpa"] * mesh.shape["tpb"]

    def local_step(hidden, w_head, q_draft, x_draft):
        seqs, positions, depth = hidden.shape
        vl = w_head.shape[1]
        num_draft = x_draft.shape[1]
        phases = num_draft // ROWS
        vp = pl.cdiv(vl, LANES) * LANES
        rows = seqs * positions
        stat_rows = pl.cdiv(rows, LANES) * LANES
        f32 = jnp.float32
        any_spec = pl.BlockSpec(memory_space=pl.ANY)
        vmem_spec = pl.BlockSpec(memory_space=pltpu.VMEM)
        z, tot = pl.pallas_call(
            functools.partial(exchange_kernel, n, phases, vl),
            name="exchange",
            out_shape=(pltpu.VMEM((rows, vp), f32), pltpu.VMEM((phases, 3, LANES), f32)),
            in_specs=[any_spec] * 4,
            out_specs=(vmem_spec, vmem_spec),
            scratch_shapes=[
                pltpu.VMEM((rows, depth), jnp.bfloat16),
                pltpu.VMEM((rows, depth), jnp.bfloat16),
                pltpu.VMEM((W_BUFS, W_ROWS, depth), jnp.bfloat16),
                pltpu.VMEM((phases, n, ROWS, vp + LANES), f32),
                pltpu.VMEM((phases, n, ROWS, vp), f32),
                pltpu.VMEM((seqs, num_draft), jnp.int32),
                pltpu.VMEM((stat_rows, LANES), f32),
                pltpu.VMEM((stat_rows, LANES), f32),
                pltpu.VMEM((stat_rows, LANES), f32),
                pltpu.VMEM((3, phases * n * ROWS, LANES), f32),
                pltpu.VMEM((n, 2, stat_rows // LANES, LANES), f32),
                pltpu.VMEM((phases, n, 3, LANES), f32),
                pltpu.SemaphoreType.DMA((2,)),
                pltpu.SemaphoreType.DMA((W_BUFS,)),
                pltpu.SemaphoreType.DMA((phases, n)),
                pltpu.SemaphoreType.DMA((phases, n)),
                pltpu.SemaphoreType.DMA((phases, n)),
                pltpu.SemaphoreType.DMA((n,)),
                pltpu.SemaphoreType.DMA((n,)),
                pltpu.SemaphoreType.DMA((phases, n)),
                pltpu.SemaphoreType.DMA((phases, n)),
            ],
            compiler_params=pltpu.CompilerParams(collective_id=0, has_side_effects=True, vmem_limit_bytes=48 * 2**20),
        )(hidden.transpose(1, 0, 2).reshape(rows, depth), w_head.T, q_draft.reshape(num_draft, q_draft.shape[2]), x_draft)
        residual, bonus, accept, expected = pl.pallas_call(
            functools.partial(finish_kernel, n, phases, vl),
            name="finish",
            out_shape=(jax.ShapeDtypeStruct((seqs, num_draft, vl), f32), jax.ShapeDtypeStruct((seqs, vl), f32),
                       jax.ShapeDtypeStruct((seqs, num_draft), f32), jax.ShapeDtypeStruct((1, seqs), f32)),
            in_specs=[vmem_spec, vmem_spec],
            out_specs=(any_spec, any_spec, vmem_spec, vmem_spec),
            scratch_shapes=[pltpu.VMEM((phases, n * ROWS, LANES), f32), pltpu.VMEM((seqs, num_draft, vl), f32),
                            pltpu.VMEM((seqs, vl), f32), pltpu.SemaphoreType.DMA((seqs,)), pltpu.SemaphoreType.DMA],
            compiler_params=pltpu.CompilerParams(vmem_limit_bytes=32 * 2**20),
        )(tot, z)
        return accept, expected.reshape(seqs), residual, bonus

    return jax.shard_map(
        local_step, mesh=mesh,
        in_specs=(P("dp", None, None), P(None, VOCAB_AXES), P(("dp",) + VOCAB_AXES, None, None), P("dp", None)),
        out_specs=(P("dp", None), P("dp"), P("dp", None, VOCAB_AXES), P("dp", VOCAB_AXES)),
        check_vma=False)
```

```python
import functools

import jax
import jax.numpy as jnp
from jax import lax
from jax.experimental import pallas as pl
from jax.experimental.pallas import tpu as pltpu
from jax.sharding import PartitionSpec as P

INV_TEMP = 1.25
VOCAB_AXES = ("tpa", "tpb")
MESH = pl.DeviceIdType.MESH
LANES = 128
ROWS = 8
W_ROWS = 256
W_BUFS = 4
AHEAD = 4
SCALE = 2.0 ** 64


def xor4(a, r):
    low = lax.rem(lax.rem(a, 2) + lax.rem(r, 2), 2)
    high = lax.rem(lax.div(a, 2) + lax.div(r, 2), 2)
    return low + 2 * high


def exchange_kernel(n, phases, vl, hid_ref, w_ref, q_ref, x_ref, z_ref, tot_ref,
                    hid_v, hs, wbuf, sbuf, qbuf, x_v, colmax, colsum, scale, part, stat, zmsg,
                    in_sem, w_sem, ld_sem, qs_sem, qr_sem, ss_sem, sr_sem, zs_sem, zr_sem):
    vp = qbuf.shape[3]
    tiles = vp // LANES
    last = vl - (tiles - 1) * LANES
    rows_all = z_ref.shape[0]
    draft_rows = phases * n * ROWS
    my_a, my_b = lax.axis_index("tpa"), lax.axis_index("tpb")
    me = my_a * 4 + my_b
    lane = lax.broadcasted_iota(jnp.int32, (ROWS, LANES), 1)

    def peer(r):
        return xor4(my_a, lax.div(r, 4)), xor4(my_b, lax.rem(r, 4))

    def window(k):
        col = lax.div(k * vl, LANES) * LANES
        return pl.multiple_of(col, LANES), k * vl - col

    def sized(k, body):
        _, o = window(k)
        wide = o + vl > vp
        pl.when(wide)(lambda: body(vp + LANES))
        pl.when(jnp.logical_not(wide))(lambda: body(vp))

    core = lax.rem(my_b, 2)
    inner = lax.rem(lax.div(my_a + 1, 2), 2)

    def nth(i):
        return inner * lax.rem((n // 2 + 1) * (i + core) + n // 2, n) + (1 - inner) * i

    def width_of(g):
        return vp if g < phases - 1 else vp - LANES

    def load(g, k, width):
        col, _ = window(k)
        return pltpu.make_async_copy(q_ref.at[g * ROWS:(g + 1) * ROWS, pl.ds(col, width)], sbuf.at[g, k, :, pl.ds(0, width)], ld_sem.at[g, k])

    def q_copy(g, r, s):
        a, b = peer(r)
        return pltpu.make_async_remote_copy(
            src_ref=sbuf.at[g, a * 4 + b, :, pl.ds(0, width_of(g))], dst_ref=qbuf.at[g, s, :, pl.ds(0, width_of(g))],
            send_sem=qs_sem.at[g, r], recv_sem=qr_sem.at[g, s],
            device_id={"tpa": a, "tpb": b}, device_id_type=MESH)

    def tile_of(j):
        return slice(j * LANES, (j + 1) * LANES)

    def part_of(j):
        return slice(j * LANES, min((j + 1) * LANES, vl))

    free = LANES - last

    def prepare(g, k):
        _, o = window(k)
        shift = lax.rem(LANES - o, LANES)

        def last_tile(h):
            return jnp.where(lane < LANES - o, pltpu.roll(sbuf[h, k, :, tile_of(tiles - 1)], shift, 1),
                             pltpu.roll(sbuf[h, k, :, tile_of(tiles)], shift, 1))
        ending = last_tile(g)
        if g < phases - 1:
            guest = pltpu.roll(last_tile(phases - 1), last if g == 0 else LANES - (free - last) % LANES, 1)
            ending = jnp.where(lane < last, ending, guest)
        this = pltpu.roll(sbuf[g, k, :, tile_of(0)], shift, 1)
        for j in range(tiles - 1):
            following = pltpu.roll(sbuf[g, k, :, tile_of(j + 1)], shift, 1)
            sbuf[g, k, :, tile_of(j)] = jnp.where(lane < LANES - o, this, following)
            this = following
        sbuf[g, k, :, tile_of(tiles - 1)] = ending

    def send_phase(g):
        def one(i, c):
            if g < phases - 1:
                @pl.when(i + AHEAD < n)
                def _():
                    start_load(g, i + AHEAD)

            @pl.when(i < n)
            def _():
                r = nth(i)
                a, b = peer(r)
                k = a * 4 + b
                if g == 0:
                    sized(k, lambda width: load(0, k, width).wait())
                    sized(k, lambda width: load(phases - 1, k, width).wait())
                elif g < phases - 1:
                    sized(k, lambda width: load(g, k, width).wait())
                prepare(g, k)

                @pl.when(r == 0)
                def _():
                    for j in range(tiles):
                        qbuf[g, me, :, tile_of(j)] = sbuf[g, me, :, tile_of(j)]

            @pl.when(i > 0)
            def _():
                before = nth(i - 1)

                @pl.when(before > 0)
                def _():
                    q_copy(g, before, me).start()
            return c
        lax.fori_loop(0, n + 1, one, 0)

    def w_copy(c, slot):
        return pltpu.make_async_copy(w_ref.at[pl.ds(pl.multiple_of(c * W_ROWS, W_ROWS), W_ROWS), :], wbuf.at[slot], w_sem.at[slot])

    full_chunks = vl // W_ROWS
    w_tail = vl - full_chunks * W_ROWS
    tail_slot = full_chunks % W_BUFS
    tail_copy = pltpu.make_async_copy(
        w_ref.at[pl.ds(full_chunks * W_ROWS, w_tail), :], wbuf.at[tail_slot, pl.ds(0, w_tail), :], w_sem.at[tail_slot])

    hid_copy = pltpu.make_async_copy(hid_ref, hid_v, in_sem.at[0])
    x_copy = pltpu.make_async_copy(x_ref, x_v, in_sem.at[1])
    barrier = pltpu.get_barrier_semaphore()

    def greet(i, c):
        a, b = peer(n - i)
        pl.semaphore_signal(barrier, inc=1, device_id={"tpa": a, "tpb": b}, device_id_type=MESH)
        return c
    lax.fori_loop(1, n, greet, 0)

    def start_load(g, i):
        a, b = peer(nth(i))
        k = a * 4 + b
        for h in (0, phases - 1) if g == 0 else (g,):
            sized(k, lambda width, h=h: load(h, k, width).start())

    for i in range(AHEAD):
        start_load(0, i)
    x_copy.start()
    pl.semaphore_wait(barrier, n - 1)

    send_phase(0)
    for g in range(1, phases - 1):
        for i in range(AHEAD):
            start_load(g, i)
    hid_copy.start()
    for c in range(W_BUFS):
        w_copy(c, c).start()
    for g in range(1, phases - 1):
        send_phase(g)

    hid_copy.wait()
    row = lax.broadcasted_iota(jnp.int32, (rows_all, rows_all), 0)
    col = lax.broadcasted_iota(jnp.int32, (rows_all, rows_all), 1)
    source = jnp.where(row < draft_rows, ((row // (n * ROWS)) * ROWS + row % ROWS) * n + (row // ROWS) % n, row)
    permute = jnp.where(col == source, 1.0, 0.0).astype(jnp.bfloat16)
    depth = hid_v.shape[1]

    def permute_columns(c, carry):
        at = pl.ds(pl.multiple_of(c * 256, 256), 256)
        hs[:, at] = jnp.dot(permute, hid_v[:, at], preferred_element_type=jnp.float32).astype(jnp.bfloat16)
        return carry
    lax.fori_loop(0, depth // 256, permute_columns, 0)

    nt = (((1,), (1,)), ((), ()))

    def logits(c, carry):
        slot = lax.rem(c, W_BUFS)
        w_copy(c, slot).wait()
        z_ref[:, pl.ds(pl.multiple_of(c * W_ROWS, W_ROWS), W_ROWS)] = lax.dot_general(
            hs[...], wbuf[slot], nt, preferred_element_type=jnp.float32) * INV_TEMP

        @pl.when(c + W_BUFS < full_chunks)
        def _():
            w_copy(c + W_BUFS, slot).start()

        @pl.when(c + W_BUFS == full_chunks)
        def _():
            tail_copy.start()
        return carry
    lax.fori_loop(0, full_chunks, logits, 0)
    tail_copy.wait()
    z_ref[:, full_chunks * W_ROWS:vl] = lax.dot_general(
        hs[...], wbuf[tail_slot, 0:w_tail, :], nt, preferred_element_type=jnp.float32) * INV_TEMP

    def row_stats(t, carry):
        rows = pl.ds(pl.multiple_of(t * ROWS, ROWS), ROWS)
        ending = z_ref[rows, part_of(tiles - 1)]
        m = z_ref[rows, part_of(0)]
        for j in range(1, tiles - 1):
            m = jnp.maximum(m, z_ref[rows, part_of(j)])
        m = jnp.maximum(jnp.max(m, axis=1, keepdims=True), jnp.max(ending, axis=1, keepdims=True))
        m = jnp.broadcast_to(m, (ROWS, LANES))
        ending = jnp.exp(ending - m[:, 0:last])
        z_ref[rows, part_of(tiles - 1)] = ending
        s = jnp.zeros((ROWS, LANES), jnp.float32)
        for j in range(tiles - 1):
            e = jnp.exp(z_ref[rows, part_of(j)] - m)
            z_ref[rows, part_of(j)] = e
            s = s + e
        s = jnp.sum(s, axis=1, keepdims=True) + jnp.sum(ending, axis=1, keepdims=True)
        colmax[rows, :] = m
        colsum[rows, :] = jnp.broadcast_to(s, (ROWS, LANES))
        return carry
    lax.fori_loop(0, rows_all // ROWS, row_stats, 0)
    spare = colmax.shape[0] - rows_all
    colmax[rows_all:, :] = jnp.zeros((spare, LANES), jnp.float32)
    colsum[rows_all:, :] = jnp.ones((spare, LANES), jnp.float32)

    blocks = colmax.shape[0] // LANES

    def as_rows(ref):
        return jnp.concatenate([ref[i * LANES:(i + 1) * LANES, :].T[0:1, :] for i in range(blocks)], axis=0)
    stat[me, 0] = as_rows(colmax)
    stat[me, 1] = as_rows(colsum)

    def stat_copy(r, s):
        a, b = peer(r)
        return pltpu.make_async_remote_copy(
            src_ref=stat.at[me], dst_ref=stat.at[s], send_sem=ss_sem.at[r], recv_sem=sr_sem.at[s],
            device_id={"tpa": a, "tpb": b}, device_id_type=MESH)

    def send_stat(r, c):
        stat_copy(r, me).start()
        return c
    lax.fori_loop(1, n, send_stat, 0)
    send_phase(2)

    def wait_stat(r, c):
        a, b = peer(r)
        stat_copy(r, a * 4 + b).wait_recv()
        return c
    lax.fori_loop(1, n, wait_stat, 0)
    glob_max = stat[0, 0]
    for s in range(1, n):
        glob_max = jnp.maximum(glob_max, stat[s, 0])
    glob_sum = jnp.zeros_like(glob_max)
    for s in range(n):
        glob_sum = glob_sum + stat[s, 1] * jnp.exp(stat[s, 0] - glob_max)
    factor = jnp.exp(stat[me, 0] - glob_max) / glob_sum
    for i in range(blocks):
        scale[i * LANES:(i + 1) * LANES, :] = jnp.broadcast_to(factor[i:i + 1, :], (LANES, LANES)).T

    for t in range(draft_rows // ROWS, rows_all // ROWS):
        rows = slice(t * ROWS, (t + 1) * ROWS)
        for j in range(tiles):
            value = z_ref[rows, part_of(j)]
            z_ref[rows, part_of(j)] = value * scale[rows, 0:value.shape[1]]

    x_copy.wait()
    lane_f = lane.astype(jnp.float32)
    num_draft = x_v.shape[1]

    def excess(g, s):
        rows = pl.ds(pl.multiple_of(g * (n * ROWS) + s * ROWS, ROWS), ROWS)
        tokens = jnp.broadcast_to(x_v[pl.ds(s, 1), :].astype(jnp.float32), (ROWS, num_draft))
        position = lax.broadcasted_iota(jnp.int32, (ROWS, num_draft), 0) + g * ROWS
        here = lax.broadcasted_iota(jnp.int32, (ROWS, num_draft), 1) == position
        token = jnp.sum(jnp.where(here, tokens, 0.0), axis=1, keepdims=True) - (me * vl).astype(jnp.float32)
        token = jnp.broadcast_to(jnp.where(token < vl, token, -1.0), (ROWS, LANES))
        sc = scale[rows, :]
        z_sum = p_pick = q_pick = jnp.zeros((ROWS, LANES), jnp.float32)
        for j in range(tiles - 1):
            q = qbuf[g, s, :, tile_of(j)]
            p = z_ref[rows, part_of(j)] * sc
            d = jnp.maximum(p - q, 0.0)
            z_ref[rows, part_of(j)] = d
            z_sum = z_sum + d
            hit = lane_f == token - float(j * LANES)
            p_pick = jnp.where(hit, p, p_pick)
            q_pick = jnp.where(hit, q, q_pick)
        j = tiles - 1
        if g < phases - 1:
            q = qbuf[g, s, :, tile_of(j)]
        else:
            q = jnp.where(lane < free, pltpu.roll(qbuf[0, s, :, tile_of(j)], free, 1),
                          pltpu.roll(qbuf[1, s, :, tile_of(j)], (free - last) % LANES, 1))
        q = q[:, 0:last]
        p = z_ref[rows, part_of(j)] * sc[:, 0:last]
        d = jnp.maximum(p - q, 0.0)
        z_ref[rows, part_of(j)] = d
        hit = (lane_f == token - float(j * LANES))[:, 0:last]
        part[0, rows, :] = z_sum
        part[1, rows, :] = p_pick
        part[2, rows, :] = q_pick
        part[0, rows, 0:last] = z_sum[:, 0:last] + d
        part[1, rows, 0:last] = jnp.where(hit, p, p_pick[:, 0:last])
        part[2, rows, 0:last] = jnp.where(hit, q, q_pick[:, 0:last])

    def z_copy(g, r, s):
        a, b = peer(r)
        return pltpu.make_async_remote_copy(
            src_ref=zmsg.at[g, me], dst_ref=zmsg.at[g, s], send_sem=zs_sem.at[g, r], recv_sem=zr_sem.at[g, s],
            device_id={"tpa": a, "tpb": b}, device_id_type=MESH)

    def add_up(g):
        def arrived(r, c):
            a, b = peer(r)
            z_copy(g, r, a * 4 + b).wait_recv()
            return c
        lax.fori_loop(1, n, arrived, 0)
        total = zmsg[g, 0]
        for s in range(1, n):
            total = total + zmsg[g, s]
        tot_ref[g] = total

    for g in range(phases):
        def one(i, c, g=g):
            a, b = peer(i)
            s = a * 4 + b

            @pl.when(i > 0)
            def _():
                q_copy(g, i, s).wait_recv()
            excess(g, s)
            return c
        lax.fori_loop(0, n, one, 0)
        block = slice(g * n * ROWS, (g + 1) * n * ROWS)
        zmsg[g, me] = jnp.concatenate([jnp.sum(part[i, block, :].T, axis=0, keepdims=True) for i in range(3)], axis=0)

        def send(i, c, g=g):
            z_copy(g, n - i, me).start()
            return c
        lax.fori_loop(1, n, send, 0)

    def drain(r, c):
        for g in range(phases):
            q_copy(g, r, me).wait_send()
            z_copy(g, r, me).wait_send()
        stat_copy(r, me).wait_send()
        return c

    def divide(g):
        inverse = jnp.broadcast_to(1.0 / (tot_ref[g, 0:1, :] * SCALE), (n * ROWS, LANES)).T
        scale[0:n * ROWS, :] = inverse

        def one(s, c):
            rows = pl.ds(pl.multiple_of(g * (n * ROWS) + s * ROWS, ROWS), ROWS)
            inv = scale[pl.ds(pl.multiple_of(s * ROWS, ROWS), ROWS), :]
            for j in range(tiles):
                value = z_ref[rows, part_of(j)] * SCALE
                z_ref[rows, part_of(j)] = value * inv[:, 0:value.shape[1]]
            return c
        lax.fori_loop(0, n, one, 0)

    for g in range(phases - 1):
        add_up(g)
        divide(g)
    lax.fori_loop(1, n, drain, 0)
    add_up(phases - 1)


def finish_kernel(n, phases, vl, tot_ref, z_ref, res_ref, bonus_ref, accept_ref, expected_ref, inverse, staged, sem, bonus_sem):
    width = n * ROWS
    num_draft = phases * ROWS
    last = phases - 1

    def ready_copy(g, b):
        return pltpu.make_async_copy(z_ref.at[pl.ds(pl.multiple_of(g * width + b * ROWS, ROWS), ROWS), :],
                                     res_ref.at[b, g * ROWS:(g + 1) * ROWS, :], sem.at[g, b])

    def staged_copy(b):
        return pltpu.make_async_copy(staged.at[b], res_ref.at[b, last * ROWS:, :], sem.at[last, b])

    bonus_copy = pltpu.make_async_copy(z_ref.at[phases * width:phases * width + n, :], bonus_ref, bonus_sem)

    def start(b, c):
        for g in range(last):
            ready_copy(g, b).start()
        return c
    lax.fori_loop(0, n, start, 0)
    bonus_copy.start()
    inverse[...] = jnp.broadcast_to(1.0 / (tot_ref[last, 0:1, :] * SCALE), (width, LANES)).T

    def one(b, c):
        inv = inverse[pl.ds(pl.multiple_of(b * ROWS, ROWS), ROWS), :]
        rows = pl.ds(pl.multiple_of(last * width + b * ROWS, ROWS), ROWS)
        for j in range(pl.cdiv(vl, LANES)):
            w = min(LANES, vl - j * LANES)
            staged[b, :, j * LANES:j * LANES + w] = (z_ref[rows, j * LANES:j * LANES + w] * SCALE) * inv[:, 0:w]
        staged_copy(b).start()
        return c
    lax.fori_loop(0, n, one, 0)

    seq_of = lax.broadcasted_iota(jnp.int32, (n, width), 1) // ROWS == lax.broadcasted_iota(jnp.int32, (n, width), 0)
    pos_of = lax.broadcasted_iota(jnp.int32, (ROWS, width), 1) % ROWS == lax.broadcasted_iota(jnp.int32, (ROWS, width), 0)
    to_seq = (lax.broadcasted_iota(jnp.int32, (width, n), 0) // ROWS
              == lax.broadcasted_iota(jnp.int32, (width, n), 1)).astype(jnp.float32)
    by_seq = jnp.zeros((n, num_draft), jnp.float32)
    by_pos = []
    for g in range(phases):
        a = jnp.minimum(1.0, tot_ref[g, 1:2, :] / tot_ref[g, 2:3, :])
        to_pos = (lax.broadcasted_iota(jnp.int32, (width, num_draft), 0) % ROWS + g * ROWS
                  == lax.broadcasted_iota(jnp.int32, (width, num_draft), 1)).astype(jnp.float32)
        by_seq = by_seq + jnp.dot(jnp.where(seq_of, jnp.broadcast_to(a, (n, width)), 0.0), to_pos,
                                  precision=lax.Precision.HIGHEST, preferred_element_type=jnp.float32)
        by_pos.append(jnp.dot(jnp.where(pos_of, jnp.broadcast_to(a, (ROWS, width)), 0.0), to_seq,
                              precision=lax.Precision.HIGHEST, preferred_element_type=jnp.float32))
    accept_ref[...] = by_seq
    product = by_pos[0][0:1, :]
    total = product
    for k in range(1, num_draft):
        product = product * by_pos[k // ROWS][k % ROWS:k % ROWS + 1, :]
        total = total + product
    expected_ref[...] = total

    def finished(b, c):
        for g in range(last):
            ready_copy(g, b).wait()
        staged_copy(b).wait()
        return c
    lax.fori_loop(0, n, finished, 0)
    bonus_copy.wait()


def solution(mesh):
    n = mesh.shape["tpa"] * mesh.shape["tpb"]

    def local_step(hidden, w_head, q_draft, x_draft):
        seqs, positions, depth = hidden.shape
        vl = w_head.shape[1]
        num_draft = x_draft.shape[1]
        phases = num_draft // ROWS
        vp = pl.cdiv(vl, LANES) * LANES
        rows = seqs * positions
        stat_rows = pl.cdiv(rows, LANES) * LANES
        f32 = jnp.float32
        any_spec = pl.BlockSpec(memory_space=pl.ANY)
        vmem_spec = pl.BlockSpec(memory_space=pltpu.VMEM)
        z, tot = pl.pallas_call(
            functools.partial(exchange_kernel, n, phases, vl),
            name="exchange",
            out_shape=(pltpu.VMEM((rows, vl), f32), pltpu.VMEM((phases, 3, LANES), f32)),
            in_specs=[any_spec] * 4,
            out_specs=(vmem_spec, vmem_spec),
            scratch_shapes=[
                pltpu.VMEM((rows, depth), jnp.bfloat16),
                pltpu.VMEM((rows, depth), jnp.bfloat16),
                pltpu.VMEM((W_BUFS, W_ROWS, depth), jnp.bfloat16),
                pltpu.VMEM((phases, n, ROWS, vp + LANES), f32),
                pltpu.VMEM((phases, n, ROWS, vp), f32),
                pltpu.VMEM((seqs, num_draft), jnp.int32),
                pltpu.VMEM((stat_rows, LANES), f32),
                pltpu.VMEM((stat_rows, LANES), f32),
                pltpu.VMEM((stat_rows, LANES), f32),
                pltpu.VMEM((3, phases * n * ROWS, LANES), f32),
                pltpu.VMEM((n, 2, stat_rows // LANES, LANES), f32),
                pltpu.VMEM((phases, n, 3, LANES), f32),
                pltpu.SemaphoreType.DMA((2,)),
                pltpu.SemaphoreType.DMA((W_BUFS,)),
                pltpu.SemaphoreType.DMA((phases, n)),
                pltpu.SemaphoreType.DMA((phases, n)),
                pltpu.SemaphoreType.DMA((phases, n)),
                pltpu.SemaphoreType.DMA((n,)),
                pltpu.SemaphoreType.DMA((n,)),
                pltpu.SemaphoreType.DMA((phases, n)),
                pltpu.SemaphoreType.DMA((phases, n)),
            ],
            compiler_params=pltpu.CompilerParams(collective_id=0, has_side_effects=True, vmem_limit_bytes=48 * 2**20),
        )(hidden.transpose(1, 0, 2).reshape(rows, depth), w_head.T, q_draft.reshape(num_draft, q_draft.shape[2]), x_draft)
        residual, bonus, accept, expected = pl.pallas_call(
            functools.partial(finish_kernel, n, phases, vl),
            name="finish",
            out_shape=(jax.ShapeDtypeStruct((seqs, num_draft, vl), f32), jax.ShapeDtypeStruct((seqs, vl), f32),
                       jax.ShapeDtypeStruct((seqs, num_draft), f32), jax.ShapeDtypeStruct((1, seqs), f32)),
            in_specs=[vmem_spec, vmem_spec],
            out_specs=(any_spec, any_spec, vmem_spec, vmem_spec),
            scratch_shapes=[pltpu.VMEM((n * ROWS, LANES), f32), pltpu.VMEM((seqs, ROWS, vl), f32),
                            pltpu.SemaphoreType.DMA((phases, seqs)), pltpu.SemaphoreType.DMA],
            compiler_params=pltpu.CompilerParams(vmem_limit_bytes=32 * 2**20),
        )(tot, z)
        return accept, expected.reshape(seqs), residual, bonus

    return jax.shard_map(
        local_step, mesh=mesh,
        in_specs=(P("dp", None, None), P(None, VOCAB_AXES), P(("dp",) + VOCAB_AXES, None, None), P("dp", None)),
        out_specs=(P("dp", None), P("dp"), P("dp", None, VOCAB_AXES), P("dp", VOCAB_AXES)),
        check_vma=False)
```

```python
import functools

import jax
import jax.numpy as jnp
from jax import lax
from jax.experimental import pallas as pl
from jax.experimental.pallas import tpu as pltpu
from jax.sharding import PartitionSpec as P

INV_TEMP = 1.25
VOCAB_AXES = ("tpa", "tpb")
MESH = pl.DeviceIdType.MESH
LANES = 128
ROWS = 8
W_ROWS = 256
W_BUFS = 4
AHEAD = 4
SCALE = 2.0 ** 64


def xor4(a, r):
    low = lax.rem(lax.rem(a, 2) + lax.rem(r, 2), 2)
    high = lax.rem(lax.div(a, 2) + lax.div(r, 2), 2)
    return low + 2 * high


def exchange_kernel(n, phases, vl, hid_ref, w_ref, q_ref, x_ref, z_ref, tot_ref,
                    hid_v, hs, wbuf, sbuf, qbuf, x_v, colmax, colsum, scale, part, stat_core, stat_chip, stat_half, sum_core, sum_chip, sum_half, zmsg,
                    in_sem, w_sem, ld_sem, qs_sem, qr_sem, swap_s, swap_r, chip_s, chip_r, zs_sem, zr_sem):
    vp = qbuf.shape[3]
    tiles = vp // LANES
    last = vl - (tiles - 1) * LANES
    rows_all = z_ref.shape[0]
    draft_rows = phases * n * ROWS
    my_a, my_b = lax.axis_index("tpa"), lax.axis_index("tpb")
    me = my_a * 4 + my_b
    lane = lax.broadcasted_iota(jnp.int32, (ROWS, LANES), 1)

    def peer(r):
        return xor4(my_a, lax.div(r, 4)), xor4(my_b, lax.rem(r, 4))

    def window(k):
        col = lax.div(k * vl, LANES) * LANES
        return pl.multiple_of(col, LANES), k * vl - col

    def sized(k, body):
        _, o = window(k)
        wide = o + vl > vp
        pl.when(wide)(lambda: body(vp + LANES))
        pl.when(jnp.logical_not(wide))(lambda: body(vp))

    core = lax.rem(my_b, 2)
    inner = lax.rem(lax.div(my_a + 1, 2), 2)

    def nth(g, i):
        r = inner * lax.rem((n // 2 + 1) * (i + core) + n // 2, n) + (1 - inner) * i
        if g == phases - 1:
            far = lax.div(r, n // 2)
            r = (1 - far) * r + far * (n // 2 + lax.rem(r + (1 - inner) * (n // 4), n // 2))
        return r

    def arrival_order(g, i):
        return i

    def width_of(g):
        return vp if g < phases - 1 else vp - LANES

    def load(g, k, width):
        col, _ = window(k)
        return pltpu.make_async_copy(q_ref.at[g * ROWS:(g + 1) * ROWS, pl.ds(col, width)], sbuf.at[g, k, :, pl.ds(0, width)], ld_sem.at[g, k])

    def q_copy(g, r, s):
        a, b = peer(r)
        return pltpu.make_async_remote_copy(
            src_ref=sbuf.at[g, a * 4 + b, :, pl.ds(0, width_of(g))], dst_ref=qbuf.at[g, s, :, pl.ds(0, width_of(g))],
            send_sem=qs_sem.at[g, r], recv_sem=qr_sem.at[g, s],
            device_id={"tpa": a, "tpb": b}, device_id_type=MESH)

    def tile_of(j):
        return slice(j * LANES, (j + 1) * LANES)

    def part_of(j):
        return slice(j * LANES, min((j + 1) * LANES, vl))

    free = LANES - last

    def prepare(g, k):
        _, o = window(k)
        shift = lax.rem(LANES - o, LANES)

        def last_tile(h):
            return jnp.where(lane < LANES - o, pltpu.roll(sbuf[h, k, :, tile_of(tiles - 1)], shift, 1),
                             pltpu.roll(sbuf[h, k, :, tile_of(tiles)], shift, 1))
        ending = last_tile(g)
        if g < phases - 1:
            guest = pltpu.roll(last_tile(phases - 1), last if g == 0 else LANES - (free - last) % LANES, 1)
            ending = jnp.where(lane < last, ending, guest)
        this = pltpu.roll(sbuf[g, k, :, tile_of(0)], shift, 1)
        for j in range(tiles - 1):
            following = pltpu.roll(sbuf[g, k, :, tile_of(j + 1)], shift, 1)
            sbuf[g, k, :, tile_of(j)] = jnp.where(lane < LANES - o, this, following)
            this = following
        sbuf[g, k, :, tile_of(tiles - 1)] = ending

    def send_phase(g):
        def one(i, c):
            if g < phases - 1:
                @pl.when(i + AHEAD < n)
                def _():
                    start_load(g, i + AHEAD)

            @pl.when(i < n)
            def _():
                r = nth(g, i)
                a, b = peer(r)
                k = a * 4 + b
                if g == 0:
                    sized(k, lambda width: load(0, k, width).wait())
                    sized(k, lambda width: load(phases - 1, k, width).wait())
                elif g < phases - 1:
                    sized(k, lambda width: load(g, k, width).wait())
                prepare(g, k)

                @pl.when(r == 0)
                def _():
                    for j in range(tiles):
                        qbuf[g, me, :, tile_of(j)] = sbuf[g, me, :, tile_of(j)]

            @pl.when(i > 0)
            def _():
                before = nth(g, i - 1)

                @pl.when(before > 0)
                def _():
                    q_copy(g, before, me).start()
            return c
        lax.fori_loop(0, n + 1, one, 0)

    def w_copy(c, slot):
        return pltpu.make_async_copy(w_ref.at[pl.ds(pl.multiple_of(c * W_ROWS, W_ROWS), W_ROWS), :], wbuf.at[slot], w_sem.at[slot])

    full_chunks = vl // W_ROWS
    w_tail = vl - full_chunks * W_ROWS
    tail_slot = full_chunks % W_BUFS
    tail_copy = pltpu.make_async_copy(
        w_ref.at[pl.ds(full_chunks * W_ROWS, w_tail), :], wbuf.at[tail_slot, pl.ds(0, w_tail), :], w_sem.at[tail_slot])

    hid_copy = pltpu.make_async_copy(hid_ref, hid_v, in_sem.at[0])
    x_copy = pltpu.make_async_copy(x_ref, x_v, in_sem.at[1])
    barrier = pltpu.get_barrier_semaphore()

    def greet(i, c):
        a, b = peer(n - i)
        pl.semaphore_signal(barrier, inc=1, device_id={"tpa": a, "tpb": b}, device_id_type=MESH)
        return c
    lax.fori_loop(1, n, greet, 0)

    def start_load(g, i):
        a, b = peer(nth(g, i))
        k = a * 4 + b
        for h in (0, phases - 1) if g == 0 else (g,):
            sized(k, lambda width, h=h: load(h, k, width).start())

    for i in range(AHEAD):
        start_load(0, i)
    x_copy.start()
    pl.semaphore_wait(barrier, n - 1)

    send_phase(0)
    for g in range(1, phases - 1):
        for i in range(AHEAD):
            start_load(g, i)
    hid_copy.start()
    for c in range(W_BUFS):
        w_copy(c, c).start()
    for g in range(1, phases - 1):
        send_phase(g)

    hid_copy.wait()
    row = lax.broadcasted_iota(jnp.int32, (rows_all, rows_all), 0)
    col = lax.broadcasted_iota(jnp.int32, (rows_all, rows_all), 1)
    source = jnp.where(row < draft_rows, ((row // (n * ROWS)) * ROWS + row % ROWS) * n + (row // ROWS) % n, row)
    permute = jnp.where(col == source, 1.0, 0.0).astype(jnp.bfloat16)
    depth = hid_v.shape[1]

    def permute_columns(c, carry):
        at = pl.ds(pl.multiple_of(c * 256, 256), 256)
        hs[:, at] = jnp.dot(permute, hid_v[:, at], preferred_element_type=jnp.float32).astype(jnp.bfloat16)
        return carry
    lax.fori_loop(0, depth // 256, permute_columns, 0)

    nt = (((1,), (1,)), ((), ()))

    def logits(c, carry):
        slot = lax.rem(c, W_BUFS)
        w_copy(c, slot).wait()
        z_ref[:, pl.ds(pl.multiple_of(c * W_ROWS, W_ROWS), W_ROWS)] = lax.dot_general(
            hs[...], wbuf[slot], nt, preferred_element_type=jnp.float32) * INV_TEMP

        @pl.when(c + W_BUFS < full_chunks)
        def _():
            w_copy(c + W_BUFS, slot).start()

        @pl.when(c + W_BUFS == full_chunks)
        def _():
            tail_copy.start()
        return carry
    lax.fori_loop(0, full_chunks, logits, 0)
    tail_copy.wait()
    z_ref[:, full_chunks * W_ROWS:vl] = lax.dot_general(
        hs[...], wbuf[tail_slot, 0:w_tail, :], nt, preferred_element_type=jnp.float32) * INV_TEMP

    def row_stats(t, carry):
        rows = pl.ds(pl.multiple_of(t * ROWS, ROWS), ROWS)
        ending = z_ref[rows, part_of(tiles - 1)]
        m = z_ref[rows, part_of(0)]
        for j in range(1, tiles - 1):
            m = jnp.maximum(m, z_ref[rows, part_of(j)])
        m = jnp.maximum(jnp.max(m, axis=1, keepdims=True), jnp.max(ending, axis=1, keepdims=True))
        m = jnp.broadcast_to(m, (ROWS, LANES))
        ending = jnp.exp(ending - m[:, 0:last])
        z_ref[rows, part_of(tiles - 1)] = ending
        s = jnp.zeros((ROWS, LANES), jnp.float32)
        for j in range(tiles - 1):
            e = jnp.exp(z_ref[rows, part_of(j)] - m)
            z_ref[rows, part_of(j)] = e
            s = s + e
        s = jnp.sum(s, axis=1, keepdims=True) + jnp.sum(ending, axis=1, keepdims=True)
        colmax[rows, :] = m
        colsum[rows, :] = jnp.broadcast_to(s, (ROWS, LANES))
        return carry
    lax.fori_loop(0, rows_all // ROWS, row_stats, 0)
    chip = my_a * 2 + lax.div(my_b, 2)
    chips = n // 2

    def swap(i, ref):
        return pltpu.make_async_remote_copy(
            src_ref=ref.at[core], dst_ref=ref.at[core], send_sem=swap_s.at[i], recv_sem=swap_r.at[i],
            device_id={"tpa": my_a, "tpb": my_b + 1 - 2 * core}, device_id_type=MESH)

    def swap_arrival(i, ref):
        return pltpu.make_async_remote_copy(
            src_ref=ref.at[1 - core], dst_ref=ref.at[1 - core], send_sem=swap_s.at[i], recv_sem=swap_r.at[i],
            device_id={"tpa": my_a, "tpb": my_b}, device_id_type=MESH)

    def chip_copy(i, ref, h, slot):
        a, b = peer(2 * h)
        return pltpu.make_async_remote_copy(
            src_ref=ref.at[chip], dst_ref=ref.at[slot], send_sem=chip_s.at[i, h], recv_sem=chip_r.at[i, slot],
            device_id={"tpa": a, "tpb": b}, device_id_type=MESH)

    def chip_send(i, ref):
        for h in range(chips - 1, 0, -1):
            chip_copy(i, ref, h, chip).start()

    def chip_arrivals(i, ref):
        for h in range(1, chips):
            a, b = peer(2 * h)
            chip_copy(i, ref, h, a * 2 + lax.div(b, 2)).wait_recv()

    def combine(pairs):
        top = pairs[0][0]
        for m, _ in pairs[1:]:
            top = jnp.maximum(top, m)
        total = jnp.zeros_like(top)
        for m, s in pairs:
            total = total + s * jnp.exp(m - top)
        return top, total

    spare = colmax.shape[0] - rows_all
    colmax[rows_all:, :] = jnp.zeros((spare, LANES), jnp.float32)
    colsum[rows_all:, :] = jnp.ones((spare, LANES), jnp.float32)

    blocks = colmax.shape[0] // LANES

    def as_rows(ref):
        return jnp.concatenate([ref[i * LANES:(i + 1) * LANES, :].T[0:1, :] for i in range(blocks)], axis=0)
    my_max = as_rows(colmax)
    stat_core[core, 0] = my_max
    stat_core[core, 1] = as_rows(colsum)
    swap(0, stat_core).start()
    swap_arrival(0, stat_core).wait_recv()
    top, total = combine([(stat_core[c, 0], stat_core[c, 1]) for c in range(2)])
    half = blocks // 2
    mine = core == 0
    stat_chip[chip, 0] = jnp.where(mine, top[0:half], top[half:])
    stat_chip[chip, 1] = jnp.where(mine, total[0:half], total[half:])
    chip_send(0, stat_chip)
    send_phase(2)

    chip_arrivals(0, stat_chip)
    top, total = combine([(stat_chip[c, 0], stat_chip[c, 1]) for c in range(chips)])
    stat_half[core, 0] = top
    stat_half[core, 1] = total
    swap(1, stat_half).start()
    swap_arrival(1, stat_half).wait_recv()
    top = jnp.concatenate([stat_half[0, 0], stat_half[1, 0]], axis=0)
    total = jnp.concatenate([stat_half[0, 1], stat_half[1, 1]], axis=0)
    factor = jnp.exp(stat_core[core, 0] - top) / total
    for i in range(blocks):
        scale[i * LANES:(i + 1) * LANES, :] = jnp.broadcast_to(factor[i:i + 1, :], (LANES, LANES)).T

    for t in range(draft_rows // ROWS, rows_all // ROWS):
        rows = slice(t * ROWS, (t + 1) * ROWS)
        for j in range(tiles):
            value = z_ref[rows, part_of(j)]
            z_ref[rows, part_of(j)] = value * scale[rows, 0:value.shape[1]]

    x_copy.wait()
    lane_f = lane.astype(jnp.float32)
    num_draft = x_v.shape[1]

    def excess(g, s):
        rows = pl.ds(pl.multiple_of(g * (n * ROWS) + s * ROWS, ROWS), ROWS)
        tokens = jnp.broadcast_to(x_v[pl.ds(s, 1), :].astype(jnp.float32), (ROWS, num_draft))
        position = lax.broadcasted_iota(jnp.int32, (ROWS, num_draft), 0) + g * ROWS
        here = lax.broadcasted_iota(jnp.int32, (ROWS, num_draft), 1) == position
        token = jnp.sum(jnp.where(here, tokens, 0.0), axis=1, keepdims=True) - (me * vl).astype(jnp.float32)
        token = jnp.broadcast_to(jnp.where(token < vl, token, -1.0), (ROWS, LANES))
        sc = scale[rows, :]
        z_sum = p_pick = q_pick = jnp.zeros((ROWS, LANES), jnp.float32)
        for j in range(tiles - 1):
            q = qbuf[g, s, :, tile_of(j)]
            p = z_ref[rows, part_of(j)] * sc
            d = jnp.maximum(p - q, 0.0)
            z_ref[rows, part_of(j)] = d
            z_sum = z_sum + d
            hit = lane_f == token - float(j * LANES)
            p_pick = jnp.where(hit, p, p_pick)
            q_pick = jnp.where(hit, q, q_pick)
        j = tiles - 1
        if g < phases - 1:
            q = qbuf[g, s, :, tile_of(j)]
        else:
            q = jnp.where(lane < free, pltpu.roll(qbuf[0, s, :, tile_of(j)], free, 1),
                          pltpu.roll(qbuf[1, s, :, tile_of(j)], (free - last) % LANES, 1))
        q = q[:, 0:last]
        p = z_ref[rows, part_of(j)] * sc[:, 0:last]
        d = jnp.maximum(p - q, 0.0)
        z_ref[rows, part_of(j)] = d
        hit = (lane_f == token - float(j * LANES))[:, 0:last]
        part[0, rows, :] = z_sum
        part[1, rows, :] = p_pick
        part[2, rows, :] = q_pick
        part[0, rows, 0:last] = z_sum[:, 0:last] + d
        part[1, rows, 0:last] = jnp.where(hit, p, p_pick[:, 0:last])
        part[2, rows, 0:last] = jnp.where(hit, q, q_pick[:, 0:last])

    def z_copy(r, s):
        a, b = peer(r)
        return pltpu.make_async_remote_copy(
            src_ref=zmsg.at[me], dst_ref=zmsg.at[s], send_sem=zs_sem.at[r], recv_sem=zr_sem.at[s],
            device_id={"tpa": a, "tpb": b}, device_id_type=MESH)

    def row_sums(g):
        block = slice(g * n * ROWS, (g + 1) * n * ROWS)
        return jnp.concatenate([jnp.sum(part[i, block, :].T, axis=0, keepdims=True) for i in range(3)], axis=0)

    for g in range(phases):
        def one(i, c, g=g):
            r = arrival_order(g, i)
            a, b = peer(r)
            s = a * 4 + b

            @pl.when(r > 0)
            def _():
                q_copy(g, r, s).wait_recv()
            excess(g, s)
            return c
        lax.fori_loop(0, n, one, 0)
        if g == phases - 2:
            for h in range(2):
                sum_core[core, h] = row_sums(h)
            swap(2, sum_core).start()
            swap_arrival(2, sum_core).wait_recv()
            sum_chip[chip] = jnp.where(mine, sum_core[0, 0] + sum_core[1, 0], sum_core[0, 1] + sum_core[1, 1])
            chip_send(1, sum_chip)
    zmsg[me] = row_sums(phases - 1)
    for r in range(n - 1, 0, -1):
        z_copy(r, me).start()

    def drain(r, c):
        for g in range(phases):
            q_copy(g, r, me).wait_send()
        z_copy(r, me).wait_send()
        return c

    def divide(g):
        inverse = jnp.broadcast_to(1.0 / (tot_ref[g, 0:1, :] * SCALE), (n * ROWS, LANES)).T
        scale[0:n * ROWS, :] = inverse

        def one(s, c):
            rows = pl.ds(pl.multiple_of(g * (n * ROWS) + s * ROWS, ROWS), ROWS)
            inv = scale[pl.ds(pl.multiple_of(s * ROWS, ROWS), ROWS), :]
            for j in range(tiles):
                value = z_ref[rows, part_of(j)] * SCALE
                z_ref[rows, part_of(j)] = value * inv[:, 0:value.shape[1]]
            return c
        lax.fori_loop(0, n, one, 0)

    chip_arrivals(1, sum_chip)
    total = sum_chip[0]
    for c in range(1, chips):
        total = total + sum_chip[c]
    sum_half[core] = total
    swap(3, sum_half).start()
    swap_arrival(3, sum_half).wait_recv()
    for g in range(phases - 1):
        tot_ref[g] = sum_half[g]
        divide(g)
    lax.fori_loop(1, n, drain, 0)
    for i, ref in enumerate((stat_core, stat_half, sum_core, sum_half)):
        swap(i, ref).wait_send()
    for i, ref in enumerate((stat_chip, sum_chip)):
        for h in range(1, chips):
            chip_copy(i, ref, h, chip).wait_send()
    for r in range(1, n):
        a, b = peer(r)
        z_copy(r, a * 4 + b).wait_recv()
    total = zmsg[0]
    for s in range(1, n):
        total = total + zmsg[s]
    tot_ref[phases - 1] = total


def finish_kernel(n, phases, vl, tot_ref, z_ref, res_ref, bonus_ref, accept_ref, expected_ref, inverse, staged, sem, bonus_sem):
    width = n * ROWS
    num_draft = phases * ROWS
    last = phases - 1

    def ready_copy(g, b):
        return pltpu.make_async_copy(z_ref.at[pl.ds(pl.multiple_of(g * width + b * ROWS, ROWS), ROWS), :],
                                     res_ref.at[b, g * ROWS:(g + 1) * ROWS, :], sem.at[g, b])

    def staged_copy(b):
        return pltpu.make_async_copy(staged.at[b], res_ref.at[b, last * ROWS:, :], sem.at[last, b])

    bonus_copy = pltpu.make_async_copy(z_ref.at[phases * width:phases * width + n, :], bonus_ref, bonus_sem)

    def start(b, c):
        for g in range(last):
            ready_copy(g, b).start(priority=g % 2)
        return c
    lax.fori_loop(0, n, start, 0)
    bonus_copy.start()
    inverse[...] = jnp.broadcast_to(1.0 / (tot_ref[last, 0:1, :] * SCALE), (width, LANES)).T

    def one(b, c):
        inv = inverse[pl.ds(pl.multiple_of(b * ROWS, ROWS), ROWS), :]
        rows = pl.ds(pl.multiple_of(last * width + b * ROWS, ROWS), ROWS)
        for j in range(pl.cdiv(vl, LANES)):
            w = min(LANES, vl - j * LANES)
            staged[b, :, j * LANES:j * LANES + w] = (z_ref[rows, j * LANES:j * LANES + w] * SCALE) * inv[:, 0:w]
        staged_copy(b).start()
        return c
    lax.fori_loop(0, n, one, 0)

    seq_of = lax.broadcasted_iota(jnp.int32, (n, width), 1) // ROWS == lax.broadcasted_iota(jnp.int32, (n, width), 0)
    pos_of = lax.broadcasted_iota(jnp.int32, (ROWS, width), 1) % ROWS == lax.broadcasted_iota(jnp.int32, (ROWS, width), 0)
    to_seq = (lax.broadcasted_iota(jnp.int32, (width, n), 0) // ROWS
              == lax.broadcasted_iota(jnp.int32, (width, n), 1)).astype(jnp.float32)
    by_seq = jnp.zeros((n, num_draft), jnp.float32)
    by_pos = []
    for g in range(phases):
        a = jnp.minimum(1.0, tot_ref[g, 1:2, :] / tot_ref[g, 2:3, :])
        to_pos = (lax.broadcasted_iota(jnp.int32, (width, num_draft), 0) % ROWS + g * ROWS
                  == lax.broadcasted_iota(jnp.int32, (width, num_draft), 1)).astype(jnp.float32)
        by_seq = by_seq + jnp.dot(jnp.where(seq_of, jnp.broadcast_to(a, (n, width)), 0.0), to_pos,
                                  precision=lax.Precision.HIGHEST, preferred_element_type=jnp.float32)
        by_pos.append(jnp.dot(jnp.where(pos_of, jnp.broadcast_to(a, (ROWS, width)), 0.0), to_seq,
                              precision=lax.Precision.HIGHEST, preferred_element_type=jnp.float32))
    accept_ref[...] = by_seq
    product = by_pos[0][0:1, :]
    total = product
    for k in range(1, num_draft):
        product = product * by_pos[k // ROWS][k % ROWS:k % ROWS + 1, :]
        total = total + product
    expected_ref[...] = total

    def finished(b, c):
        for g in range(last):
            ready_copy(g, b).wait()
        staged_copy(b).wait()
        return c
    lax.fori_loop(0, n, finished, 0)
    bonus_copy.wait()


def solution(mesh):
    n = mesh.shape["tpa"] * mesh.shape["tpb"]

    def local_step(hidden, w_head, q_draft, x_draft):
        seqs, positions, depth = hidden.shape
        vl = w_head.shape[1]
        num_draft = x_draft.shape[1]
        phases = num_draft // ROWS
        vp = pl.cdiv(vl, LANES) * LANES
        rows = seqs * positions
        stat_rows = pl.cdiv(rows, LANES) * LANES
        f32 = jnp.float32
        any_spec = pl.BlockSpec(memory_space=pl.ANY)
        vmem_spec = pl.BlockSpec(memory_space=pltpu.VMEM)
        z, tot = pl.pallas_call(
            functools.partial(exchange_kernel, n, phases, vl),
            name="exchange",
            out_shape=(pltpu.VMEM((rows, vl), f32), pltpu.VMEM((phases, 3, LANES), f32)),
            in_specs=[any_spec] * 4,
            out_specs=(vmem_spec, vmem_spec),
            scratch_shapes=[
                pltpu.VMEM((rows, depth), jnp.bfloat16),
                pltpu.VMEM((rows, depth), jnp.bfloat16),
                pltpu.VMEM((W_BUFS, W_ROWS, depth), jnp.bfloat16),
                pltpu.VMEM((phases, n, ROWS, vp + LANES), f32),
                pltpu.VMEM((phases, n, ROWS, vp), f32),
                pltpu.VMEM((seqs, num_draft), jnp.int32),
                pltpu.VMEM((stat_rows, LANES), f32),
                pltpu.VMEM((stat_rows, LANES), f32),
                pltpu.VMEM((stat_rows, LANES), f32),
                pltpu.VMEM((3, phases * n * ROWS, LANES), f32),
                pltpu.VMEM((2, 2, stat_rows // LANES, LANES), f32),
                pltpu.VMEM((n // 2, 2, stat_rows // LANES // 2, LANES), f32),
                pltpu.VMEM((2, 2, stat_rows // LANES // 2, LANES), f32),
                pltpu.VMEM((2, 2, 3, LANES), f32),
                pltpu.VMEM((n // 2, 3, LANES), f32),
                pltpu.VMEM((2, 3, LANES), f32),
                pltpu.VMEM((n, 3, LANES), f32),
                pltpu.SemaphoreType.DMA((2,)),
                pltpu.SemaphoreType.DMA((W_BUFS,)),
                pltpu.SemaphoreType.DMA((phases, n)),
                pltpu.SemaphoreType.DMA((phases, n)),
                pltpu.SemaphoreType.DMA((phases, n)),
                pltpu.SemaphoreType.DMA((4,)),
                pltpu.SemaphoreType.DMA((4,)),
                pltpu.SemaphoreType.DMA((2, n // 2)),
                pltpu.SemaphoreType.DMA((2, n // 2)),
                pltpu.SemaphoreType.DMA((n,)),
                pltpu.SemaphoreType.DMA((n,)),
            ],
            compiler_params=pltpu.CompilerParams(collective_id=0, has_side_effects=True, vmem_limit_bytes=48 * 2**20),
        )(hidden.transpose(1, 0, 2).reshape(rows, depth), w_head.T, q_draft.reshape(num_draft, q_draft.shape[2]), x_draft)
        residual, bonus, accept, expected = pl.pallas_call(
            functools.partial(finish_kernel, n, phases, vl),
            name="finish",
            out_shape=(jax.ShapeDtypeStruct((seqs, num_draft, vl), f32), jax.ShapeDtypeStruct((seqs, vl), f32),
                       jax.ShapeDtypeStruct((seqs, num_draft), f32), jax.ShapeDtypeStruct((1, seqs), f32)),
            in_specs=[vmem_spec, vmem_spec],
            out_specs=(any_spec, any_spec, vmem_spec, vmem_spec),
            scratch_shapes=[pltpu.VMEM((n * ROWS, LANES), f32), pltpu.VMEM((seqs, ROWS, vl), f32),
                            pltpu.SemaphoreType.DMA((phases, seqs)), pltpu.SemaphoreType.DMA],
            compiler_params=pltpu.CompilerParams(vmem_limit_bytes=32 * 2**20),
        )(tot, z)
        return accept, expected.reshape(seqs), residual, bonus

    return jax.shard_map(
        local_step, mesh=mesh,
        in_specs=(P("dp", None, None), P(None, VOCAB_AXES), P(("dp",) + VOCAB_AXES, None, None), P("dp", None)),
        out_specs=(P("dp", None), P("dp"), P("dp", None, VOCAB_AXES), P("dp", VOCAB_AXES)),
        check_vma=False)
```

```python
import functools

import jax
import jax.numpy as jnp
from jax import lax
from jax.experimental import pallas as pl
from jax.experimental.pallas import tpu as pltpu
from jax.sharding import PartitionSpec as P

INV_TEMP = 1.25
VOCAB_AXES = ("tpa", "tpb")
MESH = pl.DeviceIdType.MESH
LANES = 128
ROWS = 8
W_ROWS = 256
W_BUFS = 4
AHEAD = 4
SCALE = 2.0 ** 64


def xor4(a, r):
    low = lax.rem(lax.rem(a, 2) + lax.rem(r, 2), 2)
    high = lax.rem(lax.div(a, 2) + lax.div(r, 2), 2)
    return low + 2 * high


def exchange_kernel(n, phases, vl, hid_ref, w_ref, q_ref, x_ref, z_ref, tot_ref,
                    hid_v, hs, wbuf, sbuf, qbuf, x_v, colmax, colsum, scale, part, stat_core, stat_chip, stat_half, sum_core, sum_chip, sum_half, zmsg,
                    in_sem, w_sem, ld_sem, qs_sem, qr_sem, swap_s, swap_r, chip_s, chip_r, zs_sem, zr_sem):
    vp = qbuf.shape[3]
    tiles = vp // LANES
    last = vl - (tiles - 1) * LANES
    rows_all = z_ref.shape[0]
    draft_rows = phases * n * ROWS
    my_a, my_b = lax.axis_index("tpa"), lax.axis_index("tpb")
    me = my_a * 4 + my_b
    lane = lax.broadcasted_iota(jnp.int32, (ROWS, LANES), 1)

    def flip(a, r):
        return (a, a + 1 - 2 * lax.rem(a, 2), lax.rem(a + 2, 4), 3 - a)[r]

    def peer(r):
        if isinstance(r, int):
            return flip(my_a, r // 4), flip(my_b, r % 4)
        return xor4(my_a, lax.div(r, 4)), xor4(my_b, lax.rem(r, 4))

    def window(k):
        col = lax.div(k * vl, LANES) * LANES
        return pl.multiple_of(col, LANES), k * vl - col

    def sized(k, body):
        _, o = window(k)
        wide = o + vl > vp
        pl.when(wide)(lambda: body(vp + LANES))
        pl.when(jnp.logical_not(wide))(lambda: body(vp))

    core = lax.rem(my_b, 2)
    inner = lax.rem(lax.div(my_a + 1, 2), 2)

    def nth(g, i):
        r = inner * lax.rem((n // 2 + 1) * (i + core) + n // 2, n) + (1 - inner) * i
        if g == phases - 1:
            far = lax.div(r, n // 2)
            r = (1 - far) * r + far * (n // 2 + lax.rem(r + (1 - inner) * (n // 4), n // 2))
        return r

    def arrival_order(g, i):
        far = lax.div(i, n // 2)
        return i if g < phases - 1 else (1 - far) * i + far * (n // 2 + lax.rem(i + n // 4, n // 2))

    def width_of(g):
        return vp if g < phases - 1 else vp - LANES

    def load(g, k, width):
        col, _ = window(k)
        return pltpu.make_async_copy(q_ref.at[g * ROWS:(g + 1) * ROWS, pl.ds(col, width)], sbuf.at[g, k, :, pl.ds(0, width)], ld_sem.at[g, k])

    def q_copy(g, r, s):
        a, b = peer(r)
        return pltpu.make_async_remote_copy(
            src_ref=sbuf.at[g, a * 4 + b, :, pl.ds(0, width_of(g))], dst_ref=qbuf.at[g, s, :, pl.ds(0, width_of(g))],
            send_sem=qs_sem.at[g, r], recv_sem=qr_sem.at[g, s],
            device_id={"tpa": a, "tpb": b}, device_id_type=MESH)

    def tile_of(j):
        return slice(j * LANES, (j + 1) * LANES)

    def part_of(j):
        return slice(j * LANES, min((j + 1) * LANES, vl))

    free = LANES - last

    def prepare(g, k):
        _, o = window(k)
        shift = lax.rem(LANES - o, LANES)

        def last_tile(h):
            return jnp.where(lane < LANES - o, pltpu.roll(sbuf[h, k, :, tile_of(tiles - 1)], shift, 1),
                             pltpu.roll(sbuf[h, k, :, tile_of(tiles)], shift, 1))
        ending = last_tile(g)
        if g < phases - 1:
            guest = pltpu.roll(last_tile(phases - 1), last if g == 0 else LANES - (free - last) % LANES, 1)
            ending = jnp.where(lane < last, ending, guest)
        this = pltpu.roll(sbuf[g, k, :, tile_of(0)], shift, 1)
        for j in range(tiles - 1):
            following = pltpu.roll(sbuf[g, k, :, tile_of(j + 1)], shift, 1)
            sbuf[g, k, :, tile_of(j)] = jnp.where(lane < LANES - o, this, following)
            this = following
        sbuf[g, k, :, tile_of(tiles - 1)] = ending

    def ready(g, i):
        if g < phases - 1:
            @pl.when(i + AHEAD < n)
            def _():
                start_load(g, i + AHEAD)
        r = nth(g, i)
        a, b = peer(r)
        k = a * 4 + b
        if g == 0:
            sized(k, lambda width: load(0, k, width).wait())
            sized(k, lambda width: load(phases - 1, k, width).wait())
        elif g < phases - 1:
            sized(k, lambda width: load(g, k, width).wait())
        prepare(g, k)

        @pl.when(r == 0)
        def _():
            for j in range(tiles):
                qbuf[g, me, :, tile_of(j)] = sbuf[g, me, :, tile_of(j)]

    def first(g):
        lax.fori_loop(0, 2, lambda i, c: (ready(g, i), c)[1], 0)

    def send_phase(g):
        def one(i, c):
            r = nth(g, i)

            @pl.when(r > 0)
            def _():
                q_copy(g, r, me).start()

            @pl.when(i + 2 < n)
            def _():
                ready(g, i + 2)
            return c
        lax.fori_loop(0, n, one, 0)

    def w_copy(c, slot):
        return pltpu.make_async_copy(w_ref.at[pl.ds(pl.multiple_of(c * W_ROWS, W_ROWS), W_ROWS), :], wbuf.at[slot], w_sem.at[slot])

    full_chunks = vl // W_ROWS
    w_tail = vl - full_chunks * W_ROWS
    tail_slot = full_chunks % W_BUFS
    tail_copy = pltpu.make_async_copy(
        w_ref.at[pl.ds(full_chunks * W_ROWS, w_tail), :], wbuf.at[tail_slot, pl.ds(0, w_tail), :], w_sem.at[tail_slot])

    hid_copy = pltpu.make_async_copy(hid_ref, hid_v, in_sem.at[0])
    x_copy = pltpu.make_async_copy(x_ref, x_v, in_sem.at[1])
    barrier = pltpu.get_barrier_semaphore()

    for r in range(n - 1, 0, -1):
        a, b = peer(r)
        pl.semaphore_signal(barrier, inc=1, device_id={"tpa": a, "tpb": b}, device_id_type=MESH)

    def start_load(g, i):
        a, b = peer(nth(g, i))
        k = a * 4 + b
        for h in (0, phases - 1) if g == 0 else (g,):
            sized(k, lambda width, h=h: load(h, k, width).start())

    for i in range(AHEAD):
        start_load(0, i)
    x_copy.start()
    first(0)
    pl.semaphore_wait(barrier, n - 1)

    send_phase(0)
    for g in range(1, phases - 1):
        for i in range(AHEAD):
            start_load(g, i)
    hid_copy.start()
    for c in range(W_BUFS):
        w_copy(c, c).start()
    for g in range(1, phases - 1):
        first(g)
        send_phase(g)

    hid_copy.wait()
    row = lax.broadcasted_iota(jnp.int32, (rows_all, rows_all), 0)
    col = lax.broadcasted_iota(jnp.int32, (rows_all, rows_all), 1)
    source = jnp.where(row < draft_rows, ((row // (n * ROWS)) * ROWS + row % ROWS) * n + (row // ROWS) % n, row)
    permute = jnp.where(col == source, 1.0, 0.0).astype(jnp.bfloat16)
    depth = hid_v.shape[1]

    def permute_columns(c, carry):
        at = pl.ds(pl.multiple_of(c * 256, 256), 256)
        hs[:, at] = jnp.dot(permute, hid_v[:, at], preferred_element_type=jnp.float32).astype(jnp.bfloat16)
        return carry
    lax.fori_loop(0, depth // 256, permute_columns, 0)

    nt = (((1,), (1,)), ((), ()))

    def logits(c, carry):
        slot = lax.rem(c, W_BUFS)
        w_copy(c, slot).wait()
        z_ref[:, pl.ds(pl.multiple_of(c * W_ROWS, W_ROWS), W_ROWS)] = lax.dot_general(
            hs[...], wbuf[slot], nt, preferred_element_type=jnp.float32) * INV_TEMP

        @pl.when(c + W_BUFS < full_chunks)
        def _():
            w_copy(c + W_BUFS, slot).start()

        @pl.when(c + W_BUFS == full_chunks)
        def _():
            tail_copy.start()
        return carry
    lax.fori_loop(0, full_chunks, logits, 0)
    tail_copy.wait()
    z_ref[:, full_chunks * W_ROWS:vl] = lax.dot_general(
        hs[...], wbuf[tail_slot, 0:w_tail, :], nt, preferred_element_type=jnp.float32) * INV_TEMP

    def row_stats(t, carry):
        rows = pl.ds(pl.multiple_of(t * ROWS, ROWS), ROWS)
        ending = z_ref[rows, part_of(tiles - 1)]
        m = z_ref[rows, part_of(0)]
        for j in range(1, tiles - 1):
            m = jnp.maximum(m, z_ref[rows, part_of(j)])
        m = jnp.maximum(jnp.max(m, axis=1, keepdims=True), jnp.max(ending, axis=1, keepdims=True))
        m = jnp.broadcast_to(m, (ROWS, LANES))
        ending = jnp.exp(ending - m[:, 0:last])
        z_ref[rows, part_of(tiles - 1)] = ending
        s = jnp.zeros((ROWS, LANES), jnp.float32)
        for j in range(tiles - 1):
            e = jnp.exp(z_ref[rows, part_of(j)] - m)
            z_ref[rows, part_of(j)] = e
            s = s + e
        s = jnp.sum(s, axis=1, keepdims=True) + jnp.sum(ending, axis=1, keepdims=True)
        colmax[rows, :] = m
        colsum[rows, :] = jnp.broadcast_to(s, (ROWS, LANES))
        return carry
    lax.fori_loop(0, rows_all // ROWS, row_stats, 0)
    chip = my_a * 2 + lax.div(my_b, 2)
    chips = n // 2

    def swap(i, ref):
        return pltpu.make_async_remote_copy(
            src_ref=ref.at[core], dst_ref=ref.at[core], send_sem=swap_s.at[i], recv_sem=swap_r.at[i],
            device_id={"tpa": my_a, "tpb": my_b + 1 - 2 * core}, device_id_type=MESH)

    def swap_arrival(i, ref):
        return pltpu.make_async_remote_copy(
            src_ref=ref.at[1 - core], dst_ref=ref.at[1 - core], send_sem=swap_s.at[i], recv_sem=swap_r.at[i],
            device_id={"tpa": my_a, "tpb": my_b}, device_id_type=MESH)

    def chip_copy(i, ref, h, slot):
        a, b = peer(2 * h)
        return pltpu.make_async_remote_copy(
            src_ref=ref.at[chip], dst_ref=ref.at[slot], send_sem=chip_s.at[i, h], recv_sem=chip_r.at[i, slot],
            device_id={"tpa": a, "tpb": b}, device_id_type=MESH)

    def chip_send(i, ref):
        for h in range(chips - 1, 0, -1):
            chip_copy(i, ref, h, chip).start()

    def chip_arrivals(i, ref):
        for h in range(1, chips):
            a, b = peer(2 * h)
            chip_copy(i, ref, h, a * 2 + lax.div(b, 2)).wait_recv()

    def combine(pairs):
        top = pairs[0][0]
        for m, _ in pairs[1:]:
            top = jnp.maximum(top, m)
        total = jnp.zeros_like(top)
        for m, s in pairs:
            total = total + s * jnp.exp(m - top)
        return top, total

    spare = colmax.shape[0] - rows_all
    colmax[rows_all:, :] = jnp.zeros((spare, LANES), jnp.float32)
    colsum[rows_all:, :] = jnp.ones((spare, LANES), jnp.float32)

    blocks = colmax.shape[0] // LANES

    def as_rows(ref):
        return jnp.concatenate([ref[i * LANES:(i + 1) * LANES, :].T[0:1, :] for i in range(blocks)], axis=0)
    my_max = as_rows(colmax)
    stat_core[core, 0] = my_max
    stat_core[core, 1] = as_rows(colsum)
    swap(0, stat_core).start()
    swap_arrival(0, stat_core).wait_recv()
    top, total = combine([(stat_core[c, 0], stat_core[c, 1]) for c in range(2)])
    half = blocks // 2
    mine = core == 0
    stat_chip[chip, 0] = jnp.where(mine, top[0:half], top[half:])
    stat_chip[chip, 1] = jnp.where(mine, total[0:half], total[half:])
    chip_send(0, stat_chip)
    first(phases - 1)
    send_phase(phases - 1)

    chip_arrivals(0, stat_chip)
    top, total = combine([(stat_chip[c, 0], stat_chip[c, 1]) for c in range(chips)])
    stat_half[core, 0] = top
    stat_half[core, 1] = total
    swap(1, stat_half).start()
    swap_arrival(1, stat_half).wait_recv()
    top = jnp.concatenate([stat_half[0, 0], stat_half[1, 0]], axis=0)
    total = jnp.concatenate([stat_half[0, 1], stat_half[1, 1]], axis=0)
    factor = jnp.exp(stat_core[core, 0] - top) / total
    for i in range(blocks):
        scale[i * LANES:(i + 1) * LANES, :] = jnp.broadcast_to(factor[i:i + 1, :], (LANES, LANES)).T

    for t in range(draft_rows // ROWS, rows_all // ROWS):
        rows = slice(t * ROWS, (t + 1) * ROWS)
        for j in range(tiles):
            value = z_ref[rows, part_of(j)]
            z_ref[rows, part_of(j)] = value * scale[rows, 0:value.shape[1]]

    x_copy.wait()
    lane_f = lane.astype(jnp.float32)
    num_draft = x_v.shape[1]

    def excess(g, s):
        rows = pl.ds(pl.multiple_of(g * (n * ROWS) + s * ROWS, ROWS), ROWS)
        tokens = jnp.broadcast_to(x_v[pl.ds(s, 1), :].astype(jnp.float32), (ROWS, num_draft))
        position = lax.broadcasted_iota(jnp.int32, (ROWS, num_draft), 0) + g * ROWS
        here = lax.broadcasted_iota(jnp.int32, (ROWS, num_draft), 1) == position
        token = jnp.sum(jnp.where(here, tokens, 0.0), axis=1, keepdims=True) - (me * vl).astype(jnp.float32)
        token = jnp.broadcast_to(jnp.where(token < vl, token, -1.0), (ROWS, LANES))
        sc = scale[rows, :]
        z_sum = p_pick = q_pick = jnp.zeros((ROWS, LANES), jnp.float32)
        for j in range(tiles - 1):
            q = qbuf[g, s, :, tile_of(j)]
            p = z_ref[rows, part_of(j)] * sc
            d = jnp.maximum(p - q, 0.0)
            z_ref[rows, part_of(j)] = d
            z_sum = z_sum + d
            hit = lane_f == token - float(j * LANES)
            p_pick = jnp.where(hit, p, p_pick)
            q_pick = jnp.where(hit, q, q_pick)
        j = tiles - 1
        if g < phases - 1:
            q = qbuf[g, s, :, tile_of(j)]
        else:
            q = jnp.where(lane < free, pltpu.roll(qbuf[0, s, :, tile_of(j)], free, 1),
                          pltpu.roll(qbuf[1, s, :, tile_of(j)], (free - last) % LANES, 1))
        q = q[:, 0:last]
        p = z_ref[rows, part_of(j)] * sc[:, 0:last]
        d = jnp.maximum(p - q, 0.0)
        z_ref[rows, part_of(j)] = d
        hit = (lane_f == token - float(j * LANES))[:, 0:last]
        sums = [jnp.sum(whole, axis=1, keepdims=True) + jnp.sum(ending, axis=1, keepdims=True)
                for whole, ending in ((z_sum, d), (p_pick, jnp.where(hit, p, 0.0)), (q_pick, jnp.where(hit, q, 0.0)))]
        part[rows, :] = jnp.where(lane == 0, sums[0], jnp.where(lane == 1, sums[1], sums[2]))

    def z_copy(r, s):
        a, b = peer(r)
        return pltpu.make_async_remote_copy(
            src_ref=zmsg.at[me], dst_ref=zmsg.at[s], send_sem=zs_sem.at[r], recv_sem=zr_sem.at[s],
            device_id={"tpa": a, "tpb": b}, device_id_type=MESH)

    def row_sums(g):
        block = slice(g * n * ROWS, (g + 1) * n * ROWS)
        return part[block, :].T[0:3, :]

    for g in range(phases):
        def one(i, c, g=g):
            r = arrival_order(g, i)
            a, b = peer(r)
            s = a * 4 + b

            @pl.when(r > 0)
            def _():
                q_copy(g, r, s).wait_recv()
            excess(g, s)
            return c
        lax.fori_loop(0, n, one, 0)
        if g == phases - 2:
            for h in range(2):
                sum_core[core, h] = row_sums(h)
            swap(2, sum_core).start()
            swap_arrival(2, sum_core).wait_recv()
            sum_chip[chip] = jnp.where(mine, sum_core[0, 0] + sum_core[1, 0], sum_core[0, 1] + sum_core[1, 1])
            chip_send(1, sum_chip)
    zmsg[me] = row_sums(phases - 1)
    for r in range(n - 1, 0, -1):
        z_copy(r, me).start()

    def drain(r, c):
        for g in range(phases):
            q_copy(g, r, me).wait_send()
        z_copy(r, me).wait_send()
        return c

    def divide(g):
        inverse = jnp.broadcast_to(1.0 / (tot_ref[g, 0:1, :] * SCALE), (n * ROWS, LANES)).T
        scale[0:n * ROWS, :] = inverse

        def one(s, c):
            rows = pl.ds(pl.multiple_of(g * (n * ROWS) + s * ROWS, ROWS), ROWS)
            inv = scale[pl.ds(pl.multiple_of(s * ROWS, ROWS), ROWS), :]
            for j in range(tiles):
                value = z_ref[rows, part_of(j)] * SCALE
                z_ref[rows, part_of(j)] = value * inv[:, 0:value.shape[1]]
            return c
        lax.fori_loop(0, n, one, 0)

    chip_arrivals(1, sum_chip)
    total = sum_chip[0]
    for c in range(1, chips):
        total = total + sum_chip[c]
    sum_half[core] = total
    swap(3, sum_half).start()
    swap_arrival(3, sum_half).wait_recv()
    for g in range(phases - 1):
        tot_ref[g] = sum_half[g]
        divide(g)
    lax.fori_loop(1, n, drain, 0)
    for i, ref in enumerate((stat_core, stat_half, sum_core, sum_half)):
        swap(i, ref).wait_send()
    for i, ref in enumerate((stat_chip, sum_chip)):
        for h in range(1, chips):
            chip_copy(i, ref, h, chip).wait_send()
    for r in range(1, n):
        a, b = peer(r)
        z_copy(r, a * 4 + b).wait_recv()
    total = zmsg[0]
    for s in range(1, n):
        total = total + zmsg[s]
    tot_ref[phases - 1] = total


def finish_kernel(n, phases, vl, tot_ref, z_ref, res_ref, bonus_ref, accept_ref, expected_ref, inverse, staged, sem, bonus_sem):
    width = n * ROWS
    num_draft = phases * ROWS
    last = phases - 1

    def ready_copy(g, b):
        return pltpu.make_async_copy(z_ref.at[pl.ds(pl.multiple_of(g * width + b * ROWS, ROWS), ROWS), :],
                                     res_ref.at[b, g * ROWS:(g + 1) * ROWS, :], sem.at[g, b])

    def staged_copy(b):
        return pltpu.make_async_copy(staged.at[b], res_ref.at[b, last * ROWS:, :], sem.at[last, b])

    bonus_copy = pltpu.make_async_copy(z_ref.at[phases * width:phases * width + n, :], bonus_ref, bonus_sem)

    def start(b, c):
        for g in range(last):
            ready_copy(g, b).start(priority=g % 2)
        return c
    lax.fori_loop(0, n, start, 0)
    bonus_copy.start()
    inverse[...] = jnp.broadcast_to(1.0 / (tot_ref[last, 0:1, :] * SCALE), (width, LANES)).T

    def one(b, c):
        inv = inverse[pl.ds(pl.multiple_of(b * ROWS, ROWS), ROWS), :]
        rows = pl.ds(pl.multiple_of(last * width + b * ROWS, ROWS), ROWS)
        for j in range(pl.cdiv(vl, LANES)):
            w = min(LANES, vl - j * LANES)
            staged[b, :, j * LANES:j * LANES + w] = (z_ref[rows, j * LANES:j * LANES + w] * SCALE) * inv[:, 0:w]
        staged_copy(b).start()
        return c
    lax.fori_loop(0, n, one, 0)

    seq_of = lax.broadcasted_iota(jnp.int32, (n, width), 1) // ROWS == lax.broadcasted_iota(jnp.int32, (n, width), 0)
    pos_of = lax.broadcasted_iota(jnp.int32, (ROWS, width), 1) % ROWS == lax.broadcasted_iota(jnp.int32, (ROWS, width), 0)
    to_seq = (lax.broadcasted_iota(jnp.int32, (width, n), 0) // ROWS
              == lax.broadcasted_iota(jnp.int32, (width, n), 1)).astype(jnp.float32)
    by_seq = jnp.zeros((n, num_draft), jnp.float32)
    by_pos = []
    for g in range(phases):
        a = jnp.minimum(1.0, tot_ref[g, 1:2, :] / tot_ref[g, 2:3, :])
        to_pos = (lax.broadcasted_iota(jnp.int32, (width, num_draft), 0) % ROWS + g * ROWS
                  == lax.broadcasted_iota(jnp.int32, (width, num_draft), 1)).astype(jnp.float32)
        by_seq = by_seq + jnp.dot(jnp.where(seq_of, jnp.broadcast_to(a, (n, width)), 0.0), to_pos,
                                  precision=lax.Precision.HIGHEST, preferred_element_type=jnp.float32)
        by_pos.append(jnp.dot(jnp.where(pos_of, jnp.broadcast_to(a, (ROWS, width)), 0.0), to_seq,
                              precision=lax.Precision.HIGHEST, preferred_element_type=jnp.float32))
    accept_ref[...] = by_seq
    product = by_pos[0][0:1, :]
    total = product
    for k in range(1, num_draft):
        product = product * by_pos[k // ROWS][k % ROWS:k % ROWS + 1, :]
        total = total + product
    expected_ref[...] = total

    def finished(b, c):
        for g in range(last):
            ready_copy(g, b).wait()
        staged_copy(b).wait()
        return c
    lax.fori_loop(0, n, finished, 0)
    bonus_copy.wait()


def solution(mesh):
    n = mesh.shape["tpa"] * mesh.shape["tpb"]

    def local_step(hidden, w_head, q_draft, x_draft):
        seqs, positions, depth = hidden.shape
        vl = w_head.shape[1]
        num_draft = x_draft.shape[1]
        phases = num_draft // ROWS
        vp = pl.cdiv(vl, LANES) * LANES
        rows = seqs * positions
        stat_rows = pl.cdiv(rows, LANES) * LANES
        f32 = jnp.float32
        any_spec = pl.BlockSpec(memory_space=pl.ANY)
        vmem_spec = pl.BlockSpec(memory_space=pltpu.VMEM)
        z, tot = pl.pallas_call(
            functools.partial(exchange_kernel, n, phases, vl),
            name="exchange",
            out_shape=(pltpu.VMEM((rows, vl), f32), pltpu.VMEM((phases, 3, LANES), f32)),
            in_specs=[any_spec] * 4,
            out_specs=(vmem_spec, vmem_spec),
            scratch_shapes=[
                pltpu.VMEM((rows, depth), jnp.bfloat16),
                pltpu.VMEM((rows, depth), jnp.bfloat16),
                pltpu.VMEM((W_BUFS, W_ROWS, depth), jnp.bfloat16),
                pltpu.VMEM((phases, n, ROWS, vp + LANES), f32),
                pltpu.VMEM((phases, n, ROWS, vp), f32),
                pltpu.VMEM((seqs, num_draft), jnp.int32),
                pltpu.VMEM((stat_rows, LANES), f32),
                pltpu.VMEM((stat_rows, LANES), f32),
                pltpu.VMEM((stat_rows, LANES), f32),
                pltpu.VMEM((phases * n * ROWS, LANES), f32),
                pltpu.VMEM((2, 2, stat_rows // LANES, LANES), f32),
                pltpu.VMEM((n // 2, 2, stat_rows // LANES // 2, LANES), f32),
                pltpu.VMEM((2, 2, stat_rows // LANES // 2, LANES), f32),
                pltpu.VMEM((2, 2, 3, LANES), f32),
                pltpu.VMEM((n // 2, 3, LANES), f32),
                pltpu.VMEM((2, 3, LANES), f32),
                pltpu.VMEM((n, 3, LANES), f32),
                pltpu.SemaphoreType.DMA((2,)),
                pltpu.SemaphoreType.DMA((W_BUFS,)),
                pltpu.SemaphoreType.DMA((phases, n)),
                pltpu.SemaphoreType.DMA((phases, n)),
                pltpu.SemaphoreType.DMA((phases, n)),
                pltpu.SemaphoreType.DMA((4,)),
                pltpu.SemaphoreType.DMA((4,)),
                pltpu.SemaphoreType.DMA((2, n // 2)),
                pltpu.SemaphoreType.DMA((2, n // 2)),
                pltpu.SemaphoreType.DMA((n,)),
                pltpu.SemaphoreType.DMA((n,)),
            ],
            compiler_params=pltpu.CompilerParams(collective_id=0, has_side_effects=True, vmem_limit_bytes=48 * 2**20),
        )(hidden.transpose(1, 0, 2).reshape(rows, depth), w_head.T, q_draft.reshape(num_draft, q_draft.shape[2]), x_draft)
        residual, bonus, accept, expected = pl.pallas_call(
            functools.partial(finish_kernel, n, phases, vl),
            name="finish",
            out_shape=(jax.ShapeDtypeStruct((seqs, num_draft, vl), f32), jax.ShapeDtypeStruct((seqs, vl), f32),
                       jax.ShapeDtypeStruct((seqs, num_draft), f32), jax.ShapeDtypeStruct((1, seqs), f32)),
            in_specs=[vmem_spec, vmem_spec],
            out_specs=(any_spec, any_spec, vmem_spec, vmem_spec),
            scratch_shapes=[pltpu.VMEM((n * ROWS, LANES), f32), pltpu.VMEM((seqs, ROWS, vl), f32),
                            pltpu.SemaphoreType.DMA((phases, seqs)), pltpu.SemaphoreType.DMA],
            compiler_params=pltpu.CompilerParams(vmem_limit_bytes=32 * 2**20),
        )(tot, z)
        return accept, expected.reshape(seqs), residual, bonus

    return jax.shard_map(
        local_step, mesh=mesh,
        in_specs=(P("dp", None, None), P(None, VOCAB_AXES), P(("dp",) + VOCAB_AXES, None, None), P("dp", None)),
        out_specs=(P("dp", None), P("dp"), P("dp", None, VOCAB_AXES), P("dp", VOCAB_AXES)),
        check_vma=False)
```

```python
import functools

import jax
import jax.numpy as jnp
from jax import lax
from jax.experimental import pallas as pl
from jax.experimental.pallas import tpu as pltpu
from jax.sharding import PartitionSpec as P

INV_TEMP = 1.25
VOCAB_AXES = ("tpa", "tpb")
MESH = pl.DeviceIdType.MESH
LANES = 128
ROWS = 8
W_ROWS = 256
W_BUFS = 4
AHEAD = 4
SCALE = 2.0 ** 64


def xor4(a, r):
    low = lax.rem(lax.rem(a, 2) + lax.rem(r, 2), 2)
    high = lax.rem(lax.div(a, 2) + lax.div(r, 2), 2)
    return low + 2 * high


def exchange_kernel(n, phases, vl, hid_ref, w_ref, q_ref, x_ref, z_ref, tot_ref,
                    hid_v, hs, wbuf, sbuf, qbuf, x_v, colmax, colsum, scale, part, stat_core, stat_chip, stat_half, sum_core, sum_chip, sum_half, zmsg,
                    in_sem, w_sem, ld_sem, qs_sem, qr_sem, swap_s, swap_r, chip_s, chip_r, zs_sem, zr_sem):
    vp = qbuf.shape[3]
    tiles = vp // LANES
    last = vl - (tiles - 1) * LANES
    rows_all = z_ref.shape[0]
    draft_rows = phases * n * ROWS
    my_a, my_b = lax.axis_index("tpa"), lax.axis_index("tpb")
    me = my_a * 4 + my_b
    lane = lax.broadcasted_iota(jnp.int32, (ROWS, LANES), 1)

    def flip(a, r):
        return (a, a + 1 - 2 * lax.rem(a, 2), lax.rem(a + 2, 4), 3 - a)[r]

    def peer(r):
        if isinstance(r, int):
            return flip(my_a, r // 4), flip(my_b, r % 4)
        return xor4(my_a, lax.div(r, 4)), xor4(my_b, lax.rem(r, 4))

    def window(k):
        col = lax.div(k * vl, LANES) * LANES
        return pl.multiple_of(col, LANES), k * vl - col

    def sized(k, body):
        _, o = window(k)
        wide = o + vl > vp
        pl.when(wide)(lambda: body(vp + LANES))
        pl.when(jnp.logical_not(wide))(lambda: body(vp))

    core = lax.rem(my_b, 2)
    inner = lax.rem(lax.div(my_a + 1, 2), 2)

    def nth(g, i):
        if g < phases - 1:
            return inner * lax.rem((n // 2 + 1) * (i + core) + n // 2, n) + (1 - inner) * i
        j = lax.div(i, 2)
        is_far = lax.rem(i + core + 1, 2)
        by_turns = is_far * jnp.where(j < n // 4, 3 * n // 4 - 1 - j, n + n // 4 - 1 - j) + (1 - is_far) * j
        in_turn = jnp.where(i < n // 2, i, n + n // 2 - 1 - i)
        return inner * by_turns + (1 - inner) * in_turn

    def arrival_order(g, i):
        far = lax.div(i, n // 2)
        return i if g < phases - 1 else (1 - far) * i + far * (n // 2 + lax.rem(i + n // 4, n // 2))

    def width_of(g):
        return vp if g < phases - 1 else vp - LANES

    def load(g, k, width):
        col, _ = window(k)
        return pltpu.make_async_copy(q_ref.at[g * ROWS:(g + 1) * ROWS, pl.ds(col, width)], sbuf.at[g, k, :, pl.ds(0, width)], ld_sem.at[g, k])

    def q_copy(g, r, s):
        a, b = peer(r)
        return pltpu.make_async_remote_copy(
            src_ref=sbuf.at[g, a * 4 + b, :, pl.ds(0, width_of(g))], dst_ref=qbuf.at[g, s, :, pl.ds(0, width_of(g))],
            send_sem=qs_sem.at[g, r], recv_sem=qr_sem.at[g, s],
            device_id={"tpa": a, "tpb": b}, device_id_type=MESH)

    def tile_of(j):
        return slice(j * LANES, (j + 1) * LANES)

    def part_of(j):
        return slice(j * LANES, min((j + 1) * LANES, vl))

    free = LANES - last

    def prepare(g, k):
        _, o = window(k)
        shift = lax.rem(LANES - o, LANES)

        def last_tile(h):
            return jnp.where(lane < LANES - o, pltpu.roll(sbuf[h, k, :, tile_of(tiles - 1)], shift, 1),
                             pltpu.roll(sbuf[h, k, :, tile_of(tiles)], shift, 1))
        ending = last_tile(g)
        if g < phases - 1:
            guest = pltpu.roll(last_tile(phases - 1), last if g == 0 else LANES - (free - last) % LANES, 1)
            ending = jnp.where(lane < last, ending, guest)
        this = pltpu.roll(sbuf[g, k, :, tile_of(0)], shift, 1)
        for j in range(tiles - 1):
            following = pltpu.roll(sbuf[g, k, :, tile_of(j + 1)], shift, 1)
            sbuf[g, k, :, tile_of(j)] = jnp.where(lane < LANES - o, this, following)
            this = following
        sbuf[g, k, :, tile_of(tiles - 1)] = ending

    def ready(g, i):
        if g < phases - 1:
            @pl.when(i + AHEAD < n)
            def _():
                start_load(g, i + AHEAD)
        r = nth(g, i)
        a, b = peer(r)
        k = a * 4 + b
        if g == 0:
            sized(k, lambda width: load(0, k, width).wait())
            sized(k, lambda width: load(phases - 1, k, width).wait())
        elif g < phases - 1:
            sized(k, lambda width: load(g, k, width).wait())
        prepare(g, k)

        @pl.when(r == 0)
        def _():
            for j in range(tiles):
                qbuf[g, me, :, tile_of(j)] = sbuf[g, me, :, tile_of(j)]

    def first(g):
        lax.fori_loop(0, 2, lambda i, c: (ready(g, i), c)[1], 0)

    def send_phase(g):
        def one(i, c):
            r = nth(g, i)

            @pl.when(r > 0)
            def _():
                q_copy(g, r, me).start()

            @pl.when(i + 2 < n)
            def _():
                ready(g, i + 2)
            return c
        lax.fori_loop(0, n, one, 0)

    def w_copy(c, slot):
        return pltpu.make_async_copy(w_ref.at[pl.ds(pl.multiple_of(c * W_ROWS, W_ROWS), W_ROWS), :], wbuf.at[slot], w_sem.at[slot])

    full_chunks = vl // W_ROWS
    w_tail = vl - full_chunks * W_ROWS
    tail_slot = full_chunks % W_BUFS
    tail_copy = pltpu.make_async_copy(
        w_ref.at[pl.ds(full_chunks * W_ROWS, w_tail), :], wbuf.at[tail_slot, pl.ds(0, w_tail), :], w_sem.at[tail_slot])

    hid_copy = pltpu.make_async_copy(hid_ref, hid_v, in_sem.at[0])
    x_copy = pltpu.make_async_copy(x_ref, x_v, in_sem.at[1])
    barrier = pltpu.get_barrier_semaphore()

    for r in range(n - 1, 0, -1):
        a, b = peer(r)
        pl.semaphore_signal(barrier, inc=1, device_id={"tpa": a, "tpb": b}, device_id_type=MESH)

    def start_load(g, i):
        a, b = peer(nth(g, i))
        k = a * 4 + b
        for h in (0, phases - 1) if g == 0 else (g,):
            sized(k, lambda width, h=h: load(h, k, width).start())

    for i in range(AHEAD):
        start_load(0, i)
    x_copy.start()
    first(0)
    pl.semaphore_wait(barrier, n - 1)

    send_phase(0)
    for g in range(1, phases - 1):
        for i in range(AHEAD):
            start_load(g, i)
    hid_copy.start()
    for c in range(W_BUFS):
        w_copy(c, c).start()
    for g in range(1, phases - 1):
        first(g)
        send_phase(g)

    hid_copy.wait()
    row = lax.broadcasted_iota(jnp.int32, (rows_all, rows_all), 0)
    col = lax.broadcasted_iota(jnp.int32, (rows_all, rows_all), 1)
    source = jnp.where(row < draft_rows, ((row // (n * ROWS)) * ROWS + row % ROWS) * n + (row // ROWS) % n, row)
    permute = jnp.where(col == source, 1.0, 0.0).astype(jnp.bfloat16)
    depth = hid_v.shape[1]

    def permute_columns(c, carry):
        at = pl.ds(pl.multiple_of(c * 256, 256), 256)
        hs[:, at] = jnp.dot(permute, hid_v[:, at], preferred_element_type=jnp.float32).astype(jnp.bfloat16)
        return carry
    lax.fori_loop(0, depth // 256, permute_columns, 0)

    nt = (((1,), (1,)), ((), ()))

    def logits(c, carry):
        slot = lax.rem(c, W_BUFS)
        w_copy(c, slot).wait()
        z_ref[:, pl.ds(pl.multiple_of(c * W_ROWS, W_ROWS), W_ROWS)] = lax.dot_general(
            hs[...], wbuf[slot], nt, preferred_element_type=jnp.float32) * INV_TEMP

        @pl.when(c + W_BUFS < full_chunks)
        def _():
            w_copy(c + W_BUFS, slot).start()

        @pl.when(c + W_BUFS == full_chunks)
        def _():
            tail_copy.start()
        return carry
    lax.fori_loop(0, full_chunks, logits, 0)
    tail_copy.wait()
    z_ref[:, full_chunks * W_ROWS:vl] = lax.dot_general(
        hs[...], wbuf[tail_slot, 0:w_tail, :], nt, preferred_element_type=jnp.float32) * INV_TEMP

    def row_stats(t, carry):
        rows = pl.ds(pl.multiple_of(t * ROWS, ROWS), ROWS)
        ending = z_ref[rows, part_of(tiles - 1)]
        m = z_ref[rows, part_of(0)]
        for j in range(1, tiles - 1):
            m = jnp.maximum(m, z_ref[rows, part_of(j)])
        m = jnp.maximum(jnp.max(m, axis=1, keepdims=True), jnp.max(ending, axis=1, keepdims=True))
        m = jnp.broadcast_to(m, (ROWS, LANES))
        ending = jnp.exp(ending - m[:, 0:last])
        z_ref[rows, part_of(tiles - 1)] = ending
        s = jnp.zeros((ROWS, LANES), jnp.float32)
        for j in range(tiles - 1):
            e = jnp.exp(z_ref[rows, part_of(j)] - m)
            z_ref[rows, part_of(j)] = e
            s = s + e
        s = jnp.sum(s, axis=1, keepdims=True) + jnp.sum(ending, axis=1, keepdims=True)
        colmax[rows, :] = m
        colsum[rows, :] = jnp.broadcast_to(s, (ROWS, LANES))
        return carry
    lax.fori_loop(0, rows_all // ROWS, row_stats, 0)
    chip = my_a * 2 + lax.div(my_b, 2)
    chips = n // 2

    def swap(i, ref):
        return pltpu.make_async_remote_copy(
            src_ref=ref.at[core], dst_ref=ref.at[core], send_sem=swap_s.at[i], recv_sem=swap_r.at[i],
            device_id={"tpa": my_a, "tpb": my_b + 1 - 2 * core}, device_id_type=MESH)

    def swap_arrival(i, ref):
        return pltpu.make_async_remote_copy(
            src_ref=ref.at[1 - core], dst_ref=ref.at[1 - core], send_sem=swap_s.at[i], recv_sem=swap_r.at[i],
            device_id={"tpa": my_a, "tpb": my_b}, device_id_type=MESH)

    def chip_copy(i, ref, h, slot):
        a, b = peer(2 * h)
        return pltpu.make_async_remote_copy(
            src_ref=ref.at[chip], dst_ref=ref.at[slot], send_sem=chip_s.at[i, h], recv_sem=chip_r.at[i, slot],
            device_id={"tpa": a, "tpb": b}, device_id_type=MESH)

    def chip_send(i, ref):
        for h in range(chips - 1, 0, -1):
            chip_copy(i, ref, h, chip).start()

    def chip_arrivals(i, ref):
        for h in range(1, chips):
            a, b = peer(2 * h)
            chip_copy(i, ref, h, a * 2 + lax.div(b, 2)).wait_recv()

    def combine(pairs):
        top = pairs[0][0]
        for m, _ in pairs[1:]:
            top = jnp.maximum(top, m)
        total = jnp.zeros_like(top)
        for m, s in pairs:
            total = total + s * jnp.exp(m - top)
        return top, total

    spare = colmax.shape[0] - rows_all
    colmax[rows_all:, :] = jnp.zeros((spare, LANES), jnp.float32)
    colsum[rows_all:, :] = jnp.ones((spare, LANES), jnp.float32)

    blocks = colmax.shape[0] // LANES

    def as_rows(ref):
        return jnp.concatenate([ref[i * LANES:(i + 1) * LANES, :].T[0:1, :] for i in range(blocks)], axis=0)
    my_max = as_rows(colmax)
    stat_core[core, 0] = my_max
    stat_core[core, 1] = as_rows(colsum)
    swap(0, stat_core).start()
    swap_arrival(0, stat_core).wait_recv()
    top, total = combine([(stat_core[c, 0], stat_core[c, 1]) for c in range(2)])
    half = blocks // 2
    mine = core == 0
    stat_chip[chip, 0] = jnp.where(mine, top[0:half], top[half:])
    stat_chip[chip, 1] = jnp.where(mine, total[0:half], total[half:])
    chip_send(0, stat_chip)
    first(phases - 1)
    send_phase(phases - 1)

    chip_arrivals(0, stat_chip)
    top, total = combine([(stat_chip[c, 0], stat_chip[c, 1]) for c in range(chips)])
    stat_half[core, 0] = top
    stat_half[core, 1] = total
    swap(1, stat_half).start()
    swap_arrival(1, stat_half).wait_recv()
    top = jnp.concatenate([stat_half[0, 0], stat_half[1, 0]], axis=0)
    total = jnp.concatenate([stat_half[0, 1], stat_half[1, 1]], axis=0)
    factor = jnp.exp(stat_core[core, 0] - top) / total
    for i in range(blocks):
        scale[i * LANES:(i + 1) * LANES, :] = jnp.broadcast_to(factor[i:i + 1, :], (LANES, LANES)).T

    for t in range(draft_rows // ROWS, rows_all // ROWS):
        rows = slice(t * ROWS, (t + 1) * ROWS)
        for j in range(tiles):
            value = z_ref[rows, part_of(j)]
            z_ref[rows, part_of(j)] = value * scale[rows, 0:value.shape[1]]

    x_copy.wait()
    lane_f = lane.astype(jnp.float32)
    num_draft = x_v.shape[1]

    def excess(g, s):
        rows = pl.ds(pl.multiple_of(g * (n * ROWS) + s * ROWS, ROWS), ROWS)
        tokens = jnp.broadcast_to(x_v[pl.ds(s, 1), :].astype(jnp.float32), (ROWS, num_draft))
        position = lax.broadcasted_iota(jnp.int32, (ROWS, num_draft), 0) + g * ROWS
        here = lax.broadcasted_iota(jnp.int32, (ROWS, num_draft), 1) == position
        token = jnp.sum(jnp.where(here, tokens, 0.0), axis=1, keepdims=True) - (me * vl).astype(jnp.float32)
        token = jnp.broadcast_to(jnp.where(token < vl, token, -1.0), (ROWS, LANES))
        sc = scale[rows, :]
        z_sum = p_pick = q_pick = jnp.zeros((ROWS, LANES), jnp.float32)
        for j in range(tiles - 1):
            q = qbuf[g, s, :, tile_of(j)]
            p = z_ref[rows, part_of(j)] * sc
            d = jnp.maximum(p - q, 0.0)
            z_ref[rows, part_of(j)] = d
            z_sum = z_sum + d
            hit = lane_f == token - float(j * LANES)
            p_pick = jnp.where(hit, p, p_pick)
            q_pick = jnp.where(hit, q, q_pick)
        j = tiles - 1
        if g < phases - 1:
            q = qbuf[g, s, :, tile_of(j)]
        else:
            q = jnp.where(lane < free, pltpu.roll(qbuf[0, s, :, tile_of(j)], free, 1),
                          pltpu.roll(qbuf[1, s, :, tile_of(j)], (free - last) % LANES, 1))
        q = q[:, 0:last]
        p = z_ref[rows, part_of(j)] * sc[:, 0:last]
        d = jnp.maximum(p - q, 0.0)
        z_ref[rows, part_of(j)] = d
        hit = (lane_f == token - float(j * LANES))[:, 0:last]
        sums = [jnp.sum(whole, axis=1, keepdims=True) + jnp.sum(ending, axis=1, keepdims=True)
                for whole, ending in ((z_sum, d), (p_pick, jnp.where(hit, p, 0.0)), (q_pick, jnp.where(hit, q, 0.0)))]
        part[rows, :] = jnp.where(lane == 0, sums[0], jnp.where(lane == 1, sums[1], sums[2]))

    def z_copy(r, s):
        a, b = peer(r)
        return pltpu.make_async_remote_copy(
            src_ref=zmsg.at[me], dst_ref=zmsg.at[s], send_sem=zs_sem.at[r], recv_sem=zr_sem.at[s],
            device_id={"tpa": a, "tpb": b}, device_id_type=MESH)

    def row_sums(g):
        block = slice(g * n * ROWS, (g + 1) * n * ROWS)
        return part[block, :].T[0:3, :]

    for g in range(phases):
        def one(i, c, g=g):
            r = arrival_order(g, i)
            a, b = peer(r)
            s = a * 4 + b

            @pl.when(r > 0)
            def _():
                q_copy(g, r, s).wait_recv()
            excess(g, s)
            return c
        lax.fori_loop(0, n, one, 0)
        if g == phases - 2:
            for h in range(2):
                sum_core[core, h] = row_sums(h)
            swap(2, sum_core).start()
            swap_arrival(2, sum_core).wait_recv()
            sum_chip[chip] = jnp.where(mine, sum_core[0, 0] + sum_core[1, 0], sum_core[0, 1] + sum_core[1, 1])
            chip_send(1, sum_chip)
    zmsg[me] = row_sums(phases - 1)
    for r in range(n - 1, 0, -1):
        z_copy(r, me).start()

    def drain(r, c):
        for g in range(phases):
            q_copy(g, r, me).wait_send()
        z_copy(r, me).wait_send()
        return c

    def divide(g):
        inverse = jnp.broadcast_to(1.0 / (tot_ref[g, 0:1, :] * SCALE), (n * ROWS, LANES)).T
        scale[0:n * ROWS, :] = inverse

        def one(s, c):
            rows = pl.ds(pl.multiple_of(g * (n * ROWS) + s * ROWS, ROWS), ROWS)
            inv = scale[pl.ds(pl.multiple_of(s * ROWS, ROWS), ROWS), :]
            for j in range(tiles):
                value = z_ref[rows, part_of(j)] * SCALE
                z_ref[rows, part_of(j)] = value * inv[:, 0:value.shape[1]]
            return c
        lax.fori_loop(0, n, one, 0)

    chip_arrivals(1, sum_chip)
    total = sum_chip[0]
    for c in range(1, chips):
        total = total + sum_chip[c]
    sum_half[core] = total
    swap(3, sum_half).start()
    swap_arrival(3, sum_half).wait_recv()
    for g in range(phases - 1):
        tot_ref[g] = sum_half[g]
        divide(g)
    lax.fori_loop(1, n, drain, 0)
    for i, ref in enumerate((stat_core, stat_half, sum_core, sum_half)):
        swap(i, ref).wait_send()
    for i, ref in enumerate((stat_chip, sum_chip)):
        for h in range(1, chips):
            chip_copy(i, ref, h, chip).wait_send()
    for r in range(1, n):
        a, b = peer(r)
        z_copy(r, a * 4 + b).wait_recv()
    total = zmsg[0]
    for s in range(1, n):
        total = total + zmsg[s]
    tot_ref[phases - 1] = total


def finish_kernel(n, phases, vl, tot_ref, z_ref, res_ref, bonus_ref, accept_ref, expected_ref, inverse, staged, accepted, expected, sem, bonus_sem, small_sem):
    width = n * ROWS
    num_draft = phases * ROWS
    last = phases - 1

    def ready_copy(g, b):
        return pltpu.make_async_copy(z_ref.at[pl.ds(pl.multiple_of(g * width + b * ROWS, ROWS), ROWS), :],
                                     res_ref.at[b, g * ROWS:(g + 1) * ROWS, :], sem.at[g, b])

    def staged_copy(b):
        return pltpu.make_async_copy(staged.at[b], res_ref.at[b, last * ROWS:, :], sem.at[last, b])

    bonus_copy = pltpu.make_async_copy(z_ref.at[phases * width:phases * width + n, :], bonus_ref, bonus_sem)

    def start(b, c):
        for g in range(last):
            ready_copy(g, b).start(priority=g % 2)
        return c
    lax.fori_loop(0, n, start, 0)
    bonus_copy.start()
    inverse[...] = jnp.broadcast_to(1.0 / (tot_ref[last, 0:1, :] * SCALE), (width, LANES)).T

    def one(b, c):
        inv = inverse[pl.ds(pl.multiple_of(b * ROWS, ROWS), ROWS), :]
        rows = pl.ds(pl.multiple_of(last * width + b * ROWS, ROWS), ROWS)
        for j in range(pl.cdiv(vl, LANES)):
            w = min(LANES, vl - j * LANES)
            staged[b, :, j * LANES:j * LANES + w] = (z_ref[rows, j * LANES:j * LANES + w] * SCALE) * inv[:, 0:w]
        staged_copy(b).start()
        return c
    lax.fori_loop(0, n, one, 0)

    seq_of = lax.broadcasted_iota(jnp.int32, (n, width), 1) // ROWS == lax.broadcasted_iota(jnp.int32, (n, width), 0)
    pos_of = lax.broadcasted_iota(jnp.int32, (ROWS, width), 1) % ROWS == lax.broadcasted_iota(jnp.int32, (ROWS, width), 0)
    to_seq = (lax.broadcasted_iota(jnp.int32, (width, n), 0) // ROWS
              == lax.broadcasted_iota(jnp.int32, (width, n), 1)).astype(jnp.float32)
    by_seq = jnp.zeros((n, num_draft), jnp.float32)
    by_pos = []
    for g in range(phases):
        a = jnp.minimum(1.0, tot_ref[g, 1:2, :] / tot_ref[g, 2:3, :])
        to_pos = (lax.broadcasted_iota(jnp.int32, (width, num_draft), 0) % ROWS + g * ROWS
                  == lax.broadcasted_iota(jnp.int32, (width, num_draft), 1)).astype(jnp.float32)
        by_seq = by_seq + jnp.dot(jnp.where(seq_of, jnp.broadcast_to(a, (n, width)), 0.0), to_pos,
                                  precision=lax.Precision.HIGHEST, preferred_element_type=jnp.float32)
        by_pos.append(jnp.dot(jnp.where(pos_of, jnp.broadcast_to(a, (ROWS, width)), 0.0), to_seq,
                              precision=lax.Precision.HIGHEST, preferred_element_type=jnp.float32))
    accepted[...] = by_seq
    accept_copy = pltpu.make_async_copy(accepted, accept_ref, small_sem.at[0])
    accept_copy.start()
    product = by_pos[0][0:1, :]
    total = product
    for k in range(1, num_draft):
        product = product * by_pos[k // ROWS][k % ROWS:k % ROWS + 1, :]
        total = total + product
    expected[...] = total
    expected_copy = pltpu.make_async_copy(expected, expected_ref, small_sem.at[1])
    expected_copy.start()

    def finished(b, c):
        for g in range(last):
            ready_copy(g, b).wait()
        staged_copy(b).wait()
        return c
    lax.fori_loop(0, n, finished, 0)
    bonus_copy.wait()
    accept_copy.wait()
    expected_copy.wait()


def solution(mesh):
    n = mesh.shape["tpa"] * mesh.shape["tpb"]

    def local_step(hidden, w_head, q_draft, x_draft):
        seqs, positions, depth = hidden.shape
        vl = w_head.shape[1]
        num_draft = x_draft.shape[1]
        phases = num_draft // ROWS
        vp = pl.cdiv(vl, LANES) * LANES
        rows = seqs * positions
        stat_rows = pl.cdiv(rows, LANES) * LANES
        f32 = jnp.float32
        any_spec = pl.BlockSpec(memory_space=pl.ANY)
        vmem_spec = pl.BlockSpec(memory_space=pltpu.VMEM)
        z, tot = pl.pallas_call(
            functools.partial(exchange_kernel, n, phases, vl),
            name="exchange",
            out_shape=(pltpu.VMEM((rows, vl), f32), pltpu.VMEM((phases, 3, LANES), f32)),
            in_specs=[any_spec] * 4,
            out_specs=(vmem_spec, vmem_spec),
            scratch_shapes=[
                pltpu.VMEM((rows, depth), jnp.bfloat16),
                pltpu.VMEM((rows, depth), jnp.bfloat16),
                pltpu.VMEM((W_BUFS, W_ROWS, depth), jnp.bfloat16),
                pltpu.VMEM((phases, n, ROWS, vp + LANES), f32),
                pltpu.VMEM((phases, n, ROWS, vp), f32),
                pltpu.VMEM((seqs, num_draft), jnp.int32),
                pltpu.VMEM((stat_rows, LANES), f32),
                pltpu.VMEM((stat_rows, LANES), f32),
                pltpu.VMEM((stat_rows, LANES), f32),
                pltpu.VMEM((phases * n * ROWS, LANES), f32),
                pltpu.VMEM((2, 2, stat_rows // LANES, LANES), f32),
                pltpu.VMEM((n // 2, 2, stat_rows // LANES // 2, LANES), f32),
                pltpu.VMEM((2, 2, stat_rows // LANES // 2, LANES), f32),
                pltpu.VMEM((2, 2, 3, LANES), f32),
                pltpu.VMEM((n // 2, 3, LANES), f32),
                pltpu.VMEM((2, 3, LANES), f32),
                pltpu.VMEM((n, 3, LANES), f32),
                pltpu.SemaphoreType.DMA((2,)),
                pltpu.SemaphoreType.DMA((W_BUFS,)),
                pltpu.SemaphoreType.DMA((phases, n)),
                pltpu.SemaphoreType.DMA((phases, n)),
                pltpu.SemaphoreType.DMA((phases, n)),
                pltpu.SemaphoreType.DMA((4,)),
                pltpu.SemaphoreType.DMA((4,)),
                pltpu.SemaphoreType.DMA((2, n // 2)),
                pltpu.SemaphoreType.DMA((2, n // 2)),
                pltpu.SemaphoreType.DMA((n,)),
                pltpu.SemaphoreType.DMA((n,)),
            ],
            compiler_params=pltpu.CompilerParams(collective_id=0, has_side_effects=True, vmem_limit_bytes=48 * 2**20),
        )(hidden.transpose(1, 0, 2).reshape(rows, depth), w_head.T, q_draft.reshape(num_draft, q_draft.shape[2]), x_draft)
        residual, bonus, accept, expected = pl.pallas_call(
            functools.partial(finish_kernel, n, phases, vl),
            name="finish",
            out_shape=(jax.ShapeDtypeStruct((seqs, num_draft, vl), f32), jax.ShapeDtypeStruct((seqs, vl), f32),
                       jax.ShapeDtypeStruct((seqs, num_draft), f32), jax.ShapeDtypeStruct((1, seqs), f32)),
            in_specs=[vmem_spec, vmem_spec],
            out_specs=(any_spec,) * 4,
            scratch_shapes=[pltpu.VMEM((n * ROWS, LANES), f32), pltpu.VMEM((seqs, ROWS, vl), f32),
                            pltpu.VMEM((seqs, num_draft), f32), pltpu.VMEM((1, seqs), f32),
                            pltpu.SemaphoreType.DMA((phases, seqs)), pltpu.SemaphoreType.DMA, pltpu.SemaphoreType.DMA((2,))],
            compiler_params=pltpu.CompilerParams(vmem_limit_bytes=32 * 2**20),
        )(tot, z)
        return accept, expected.reshape(seqs), residual, bonus

    return jax.shard_map(
        local_step, mesh=mesh,
        in_specs=(P("dp", None, None), P(None, VOCAB_AXES), P(("dp",) + VOCAB_AXES, None, None), P("dp", None)),
        out_specs=(P("dp", None), P("dp"), P("dp", None, VOCAB_AXES), P("dp", VOCAB_AXES)),
        check_vma=False)
```

```python
import functools

import jax
import jax.numpy as jnp
from jax import lax
from jax.experimental import pallas as pl
from jax.experimental.pallas import tpu as pltpu
from jax.sharding import PartitionSpec as P

INV_TEMP = 1.25
VOCAB_AXES = ("tpa", "tpb")
MESH = pl.DeviceIdType.MESH
LANES = 128
ROWS = 8
W_ROWS = 256
W_BUFS = 4
AHEAD = 4
SCALE = 2.0 ** 64


def xor4(a, r):
    low = lax.rem(lax.rem(a, 2) + lax.rem(r, 2), 2)
    high = lax.rem(lax.div(a, 2) + lax.div(r, 2), 2)
    return low + 2 * high


def exchange_kernel(n, phases, vl, hid_ref, w_ref, q_ref, x_ref, z_ref, tot_ref,
                    hid_v, hs, wbuf, sbuf, qbuf, x_v, colmax, colsum, scale, part, stat_core, stat_chip, stat_half, sum_core, sum_chip, sum_half, zmsg,
                    in_sem, w_sem, ld_sem, qs_sem, qr_sem, swap_s, swap_r, chip_s, chip_r, zs_sem, zr_sem):
    vp = qbuf.shape[3]
    tiles = vp // LANES
    last = vl - (tiles - 1) * LANES
    rows_all = z_ref.shape[0]
    draft_rows = phases * n * ROWS
    my_a, my_b = lax.axis_index("tpa"), lax.axis_index("tpb")
    me = my_a * 4 + my_b
    lane = lax.broadcasted_iota(jnp.int32, (ROWS, LANES), 1)

    def flip(a, r):
        return (a, a + 1 - 2 * lax.rem(a, 2), lax.rem(a + 2, 4), 3 - a)[r]

    def peer(r):
        if isinstance(r, int):
            return flip(my_a, r // 4), flip(my_b, r % 4)
        return xor4(my_a, lax.div(r, 4)), xor4(my_b, lax.rem(r, 4))

    def window(k):
        col = lax.div(k * vl, LANES) * LANES
        return pl.multiple_of(col, LANES), k * vl - col

    def sized(k, body):
        _, o = window(k)
        wide = o + vl > vp
        pl.when(wide)(lambda: body(vp + LANES))
        pl.when(jnp.logical_not(wide))(lambda: body(vp))

    core = lax.rem(my_b, 2)
    inner = lax.rem(lax.div(my_a + 1, 2), 2)

    def far_peer(f):
        return n // 2 + n // 4 * lax.rem(f + core, 2) + lax.div(f, 2)

    def nth(i):
        j = lax.div(i, 2)
        by_turns = jnp.where(lax.rem(i + core, 2) == 0, far_peer(j), j)
        in_turn = jnp.where(i < n // 2, i, far_peer(lax.rem(i, n // 2)))
        return jnp.where(inner == 1, by_turns, in_turn)

    def arrival_order(i):
        return jnp.where(i < n // 2, i, far_peer(lax.rem(i, n // 2)))

    def width_of(g):
        return vp if g < phases - 1 else vp - LANES

    def load(g, k, width):
        col, _ = window(k)
        return pltpu.make_async_copy(q_ref.at[g * ROWS:(g + 1) * ROWS, pl.ds(col, width)], sbuf.at[g, k, :, pl.ds(0, width)], ld_sem.at[g, k])

    def q_copy(g, r, s):
        a, b = peer(r)
        return pltpu.make_async_remote_copy(
            src_ref=sbuf.at[g, a * 4 + b, :, pl.ds(0, width_of(g))], dst_ref=qbuf.at[g, s, :, pl.ds(0, width_of(g))],
            send_sem=qs_sem.at[g, r], recv_sem=qr_sem.at[g, s],
            device_id={"tpa": a, "tpb": b}, device_id_type=MESH)

    def tile_of(j):
        return slice(j * LANES, (j + 1) * LANES)

    def part_of(j):
        return slice(j * LANES, min((j + 1) * LANES, vl))

    free = LANES - last

    def prepare(g, k):
        _, o = window(k)
        shift = lax.rem(LANES - o, LANES)

        def last_tile(h):
            return jnp.where(lane < LANES - o, pltpu.roll(sbuf[h, k, :, tile_of(tiles - 1)], shift, 1),
                             pltpu.roll(sbuf[h, k, :, tile_of(tiles)], shift, 1))
        ending = last_tile(g)
        if g < phases - 1:
            guest = pltpu.roll(last_tile(phases - 1), last if g == 0 else LANES - (free - last) % LANES, 1)
            ending = jnp.where(lane < last, ending, guest)
        this = pltpu.roll(sbuf[g, k, :, tile_of(0)], shift, 1)
        for j in range(tiles - 1):
            following = pltpu.roll(sbuf[g, k, :, tile_of(j + 1)], shift, 1)
            sbuf[g, k, :, tile_of(j)] = jnp.where(lane < LANES - o, this, following)
            this = following
        sbuf[g, k, :, tile_of(tiles - 1)] = ending

    def ready(g, i):
        if g < phases - 1:
            @pl.when(i + AHEAD < n)
            def _():
                start_load(g, i + AHEAD)
        r = nth(i)
        a, b = peer(r)
        k = a * 4 + b
        if g == 0:
            sized(k, lambda width: load(0, k, width).wait())
            sized(k, lambda width: load(phases - 1, k, width).wait())
        elif g < phases - 1:
            sized(k, lambda width: load(g, k, width).wait())
        prepare(g, k)

        @pl.when(r == 0)
        def _():
            for j in range(tiles):
                qbuf[g, me, :, tile_of(j)] = sbuf[g, me, :, tile_of(j)]

    def first(g):
        lax.fori_loop(0, 2, lambda i, c: (ready(g, i), c)[1], 0)

    def send_phase(g):
        def one(i, c):
            r = nth(i)

            @pl.when(r > 0)
            def _():
                q_copy(g, r, me).start()

            @pl.when(i + 2 < n)
            def _():
                ready(g, i + 2)
            return c
        lax.fori_loop(0, n, one, 0)

    def w_copy(c, slot):
        return pltpu.make_async_copy(w_ref.at[pl.ds(pl.multiple_of(c * W_ROWS, W_ROWS), W_ROWS), :], wbuf.at[slot], w_sem.at[slot])

    full_chunks = vl // W_ROWS
    w_tail = vl - full_chunks * W_ROWS
    tail_slot = full_chunks % W_BUFS
    tail_copy = pltpu.make_async_copy(
        w_ref.at[pl.ds(full_chunks * W_ROWS, w_tail), :], wbuf.at[tail_slot, pl.ds(0, w_tail), :], w_sem.at[tail_slot])

    hid_copy = pltpu.make_async_copy(hid_ref, hid_v, in_sem.at[0])
    x_copy = pltpu.make_async_copy(x_ref, x_v, in_sem.at[1])
    barrier = pltpu.get_barrier_semaphore()

    for r in range(n - 1, 0, -1):
        a, b = peer(r)
        pl.semaphore_signal(barrier, inc=1, device_id={"tpa": a, "tpb": b}, device_id_type=MESH)

    def start_load(g, i):
        a, b = peer(nth(i))
        k = a * 4 + b
        for h in (0, phases - 1) if g == 0 else (g,):
            sized(k, lambda width, h=h: load(h, k, width).start())

    for i in range(AHEAD):
        start_load(0, i)
    x_copy.start()
    first(0)
    pl.semaphore_wait(barrier, n - 1)

    send_phase(0)
    for g in range(1, phases - 1):
        for i in range(AHEAD):
            start_load(g, i)
    hid_copy.start()
    for c in range(W_BUFS):
        w_copy(c, c).start()
    for g in range(1, phases - 1):
        first(g)
        send_phase(g)

    hid_copy.wait()
    row = lax.broadcasted_iota(jnp.int32, (rows_all, rows_all), 0)
    col = lax.broadcasted_iota(jnp.int32, (rows_all, rows_all), 1)
    source = jnp.where(row < draft_rows, ((row // (n * ROWS)) * ROWS + row % ROWS) * n + (row // ROWS) % n, row)
    permute = jnp.where(col == source, 1.0, 0.0).astype(jnp.bfloat16)
    depth = hid_v.shape[1]

    def permute_columns(c, carry):
        at = pl.ds(pl.multiple_of(c * 256, 256), 256)
        hs[:, at] = jnp.dot(permute, hid_v[:, at], preferred_element_type=jnp.float32).astype(jnp.bfloat16)
        return carry
    lax.fori_loop(0, depth // 256, permute_columns, 0)

    nt = (((1,), (1,)), ((), ()))

    def logits(c, carry):
        slot = lax.rem(c, W_BUFS)
        w_copy(c, slot).wait()
        z_ref[:, pl.ds(pl.multiple_of(c * W_ROWS, W_ROWS), W_ROWS)] = lax.dot_general(
            hs[...], wbuf[slot], nt, preferred_element_type=jnp.float32) * INV_TEMP

        @pl.when(c + W_BUFS < full_chunks)
        def _():
            w_copy(c + W_BUFS, slot).start()

        @pl.when(c + W_BUFS == full_chunks)
        def _():
            tail_copy.start()
        return carry
    lax.fori_loop(0, full_chunks, logits, 0)
    tail_copy.wait()
    z_ref[:, full_chunks * W_ROWS:vl] = lax.dot_general(
        hs[...], wbuf[tail_slot, 0:w_tail, :], nt, preferred_element_type=jnp.float32) * INV_TEMP

    def row_stats(t, carry):
        rows = pl.ds(pl.multiple_of(t * ROWS, ROWS), ROWS)
        ending = z_ref[rows, part_of(tiles - 1)]
        m = z_ref[rows, part_of(0)]
        for j in range(1, tiles - 1):
            m = jnp.maximum(m, z_ref[rows, part_of(j)])
        m = jnp.maximum(jnp.max(m, axis=1, keepdims=True), jnp.max(ending, axis=1, keepdims=True))
        m = jnp.broadcast_to(m, (ROWS, LANES))
        ending = jnp.exp(ending - m[:, 0:last])
        z_ref[rows, part_of(tiles - 1)] = ending
        s = jnp.zeros((ROWS, LANES), jnp.float32)
        for j in range(tiles - 1):
            e = jnp.exp(z_ref[rows, part_of(j)] - m)
            z_ref[rows, part_of(j)] = e
            s = s + e
        s = jnp.sum(s, axis=1, keepdims=True) + jnp.sum(ending, axis=1, keepdims=True)
        colmax[rows, :] = m
        colsum[rows, :] = jnp.broadcast_to(s, (ROWS, LANES))
        return carry
    lax.fori_loop(0, rows_all // ROWS, row_stats, 0)
    chip = my_a * 2 + lax.div(my_b, 2)
    chips = n // 2

    def swap(i, ref):
        return pltpu.make_async_remote_copy(
            src_ref=ref.at[core], dst_ref=ref.at[core], send_sem=swap_s.at[i], recv_sem=swap_r.at[i],
            device_id={"tpa": my_a, "tpb": my_b + 1 - 2 * core}, device_id_type=MESH)

    def swap_arrival(i, ref):
        return pltpu.make_async_remote_copy(
            src_ref=ref.at[1 - core], dst_ref=ref.at[1 - core], send_sem=swap_s.at[i], recv_sem=swap_r.at[i],
            device_id={"tpa": my_a, "tpb": my_b}, device_id_type=MESH)

    def chip_copy(i, ref, h, slot):
        a, b = peer(2 * h)
        return pltpu.make_async_remote_copy(
            src_ref=ref.at[chip], dst_ref=ref.at[slot], send_sem=chip_s.at[i, h], recv_sem=chip_r.at[i, slot],
            device_id={"tpa": a, "tpb": b}, device_id_type=MESH)

    def chip_send(i, ref):
        for h in range(chips - 1, 0, -1):
            chip_copy(i, ref, h, chip).start()

    def chip_arrivals(i, ref):
        for h in range(1, chips):
            a, b = peer(2 * h)
            chip_copy(i, ref, h, a * 2 + lax.div(b, 2)).wait_recv()

    def combine(pairs):
        top = pairs[0][0]
        for m, _ in pairs[1:]:
            top = jnp.maximum(top, m)
        total = jnp.zeros_like(top)
        for m, s in pairs:
            total = total + s * jnp.exp(m - top)
        return top, total

    spare = colmax.shape[0] - rows_all
    colmax[rows_all:, :] = jnp.zeros((spare, LANES), jnp.float32)
    colsum[rows_all:, :] = jnp.ones((spare, LANES), jnp.float32)

    blocks = colmax.shape[0] // LANES

    def as_rows(ref):
        return jnp.concatenate([ref[i * LANES:(i + 1) * LANES, :].T[0:1, :] for i in range(blocks)], axis=0)
    my_max = as_rows(colmax)
    stat_core[core, 0] = my_max
    stat_core[core, 1] = as_rows(colsum)
    swap(0, stat_core).start()
    swap_arrival(0, stat_core).wait_recv()
    top, total = combine([(stat_core[c, 0], stat_core[c, 1]) for c in range(2)])
    half = blocks // 2
    mine = core == 0
    stat_chip[chip, 0] = jnp.where(mine, top[0:half], top[half:])
    stat_chip[chip, 1] = jnp.where(mine, total[0:half], total[half:])
    chip_send(0, stat_chip)
    first(phases - 1)
    send_phase(phases - 1)

    chip_arrivals(0, stat_chip)
    top, total = combine([(stat_chip[c, 0], stat_chip[c, 1]) for c in range(chips)])
    stat_half[core, 0] = top
    stat_half[core, 1] = total
    swap(1, stat_half).start()
    swap_arrival(1, stat_half).wait_recv()
    top = jnp.concatenate([stat_half[0, 0], stat_half[1, 0]], axis=0)
    total = jnp.concatenate([stat_half[0, 1], stat_half[1, 1]], axis=0)
    factor = jnp.exp(stat_core[core, 0] - top) / total
    for i in range(blocks):
        scale[i * LANES:(i + 1) * LANES, :] = jnp.broadcast_to(factor[i:i + 1, :], (LANES, LANES)).T

    for t in range(draft_rows // ROWS, rows_all // ROWS):
        rows = slice(t * ROWS, (t + 1) * ROWS)
        for j in range(tiles):
            value = z_ref[rows, part_of(j)]
            z_ref[rows, part_of(j)] = value * scale[rows, 0:value.shape[1]]

    x_copy.wait()
    lane_f = lane.astype(jnp.float32)
    num_draft = x_v.shape[1]

    def excess(g, s):
        rows = pl.ds(pl.multiple_of(g * (n * ROWS) + s * ROWS, ROWS), ROWS)
        tokens = jnp.broadcast_to(x_v[pl.ds(s, 1), :].astype(jnp.float32), (ROWS, num_draft))
        position = lax.broadcasted_iota(jnp.int32, (ROWS, num_draft), 0) + g * ROWS
        here = lax.broadcasted_iota(jnp.int32, (ROWS, num_draft), 1) == position
        token = jnp.sum(jnp.where(here, tokens, 0.0), axis=1, keepdims=True) - (me * vl).astype(jnp.float32)
        token = jnp.broadcast_to(jnp.where(token < vl, token, -1.0), (ROWS, LANES))
        sc = scale[rows, :]
        z_sum = p_pick = q_pick = jnp.zeros((ROWS, LANES), jnp.float32)
        for j in range(tiles - 1):
            q = qbuf[g, s, :, tile_of(j)]
            p = z_ref[rows, part_of(j)] * sc
            d = jnp.maximum(p - q, 0.0)
            z_ref[rows, part_of(j)] = d
            z_sum = z_sum + d
            hit = lane_f == token - float(j * LANES)
            p_pick = jnp.where(hit, p, p_pick)
            q_pick = jnp.where(hit, q, q_pick)
        j = tiles - 1
        if g < phases - 1:
            q = qbuf[g, s, :, tile_of(j)]
        else:
            q = jnp.where(lane < free, pltpu.roll(qbuf[0, s, :, tile_of(j)], free, 1),
                          pltpu.roll(qbuf[1, s, :, tile_of(j)], (free - last) % LANES, 1))
        q = q[:, 0:last]
        p = z_ref[rows, part_of(j)] * sc[:, 0:last]
        d = jnp.maximum(p - q, 0.0)
        z_ref[rows, part_of(j)] = d
        hit = (lane_f == token - float(j * LANES))[:, 0:last]
        sums = [jnp.sum(whole, axis=1, keepdims=True) + jnp.sum(ending, axis=1, keepdims=True)
                for whole, ending in ((z_sum, d), (p_pick, jnp.where(hit, p, 0.0)), (q_pick, jnp.where(hit, q, 0.0)))]
        part[rows, :] = jnp.where(lane == 0, sums[0], jnp.where(lane == 1, sums[1], sums[2]))

    def z_copy(r, s):
        a, b = peer(r)
        return pltpu.make_async_remote_copy(
            src_ref=zmsg.at[me], dst_ref=zmsg.at[s], send_sem=zs_sem.at[r], recv_sem=zr_sem.at[s],
            device_id={"tpa": a, "tpb": b}, device_id_type=MESH)

    def row_sums(g):
        block = slice(g * n * ROWS, (g + 1) * n * ROWS)
        return part[block, :].T[0:3, :]

    for g in range(phases):
        def one(i, c, g=g):
            r = arrival_order(i)
            a, b = peer(r)
            s = a * 4 + b

            @pl.when(r > 0)
            def _():
                q_copy(g, r, s).wait_recv()
            excess(g, s)
            return c
        lax.fori_loop(0, n, one, 0)
        if g == phases - 2:
            for h in range(2):
                sum_core[core, h] = row_sums(h)
            swap(2, sum_core).start()
            swap_arrival(2, sum_core).wait_recv()
            sum_chip[chip] = jnp.where(mine, sum_core[0, 0] + sum_core[1, 0], sum_core[0, 1] + sum_core[1, 1])
            chip_send(1, sum_chip)
    zmsg[me] = row_sums(phases - 1)
    for r in range(n - 1, 0, -1):
        z_copy(r, me).start()

    def drain(r, c):
        for g in range(phases):
            q_copy(g, r, me).wait_send()
        z_copy(r, me).wait_send()
        return c

    def divide(g):
        inverse = jnp.broadcast_to(1.0 / (tot_ref[g, 0:1, :] * SCALE), (n * ROWS, LANES)).T
        scale[0:n * ROWS, :] = inverse

        def one(s, c):
            rows = pl.ds(pl.multiple_of(g * (n * ROWS) + s * ROWS, ROWS), ROWS)
            inv = scale[pl.ds(pl.multiple_of(s * ROWS, ROWS), ROWS), :]
            for j in range(tiles):
                value = z_ref[rows, part_of(j)] * SCALE
                z_ref[rows, part_of(j)] = value * inv[:, 0:value.shape[1]]
            return c
        lax.fori_loop(0, n, one, 0)

    chip_arrivals(1, sum_chip)
    total = sum_chip[0]
    for c in range(1, chips):
        total = total + sum_chip[c]
    sum_half[core] = total
    swap(3, sum_half).start()
    swap_arrival(3, sum_half).wait_recv()
    for g in range(phases - 1):
        tot_ref[g] = sum_half[g]
        divide(g)
    lax.fori_loop(1, n, drain, 0)
    for i, ref in enumerate((stat_core, stat_half, sum_core, sum_half)):
        swap(i, ref).wait_send()
    for i, ref in enumerate((stat_chip, sum_chip)):
        for h in range(1, chips):
            chip_copy(i, ref, h, chip).wait_send()
    for r in range(1, n):
        a, b = peer(r)
        z_copy(r, a * 4 + b).wait_recv()
    total = zmsg[0]
    for s in range(1, n):
        total = total + zmsg[s]
    tot_ref[phases - 1] = total


def finish_kernel(n, phases, vl, tot_ref, z_ref, res_ref, bonus_ref, accept_ref, expected_ref, inverse, staged, accepted, expected, sem, bonus_sem, small_sem):
    width = n * ROWS
    num_draft = phases * ROWS
    last = phases - 1

    def ready_copy(g, b):
        return pltpu.make_async_copy(z_ref.at[pl.ds(pl.multiple_of(g * width + b * ROWS, ROWS), ROWS), :],
                                     res_ref.at[b, g * ROWS:(g + 1) * ROWS, :], sem.at[g, b])

    def staged_copy(b):
        return pltpu.make_async_copy(staged.at[b], res_ref.at[b, last * ROWS:, :], sem.at[last, b])

    bonus_copy = pltpu.make_async_copy(z_ref.at[phases * width:phases * width + n, :], bonus_ref, bonus_sem)

    def start(b, c):
        for g in range(last):
            ready_copy(g, b).start(priority=g % 2)
        return c
    lax.fori_loop(0, n, start, 0)
    bonus_copy.start()
    inverse[...] = jnp.broadcast_to(1.0 / (tot_ref[last, 0:1, :] * SCALE), (width, LANES)).T

    def one(b, c):
        inv = inverse[pl.ds(pl.multiple_of(b * ROWS, ROWS), ROWS), :]
        rows = pl.ds(pl.multiple_of(last * width + b * ROWS, ROWS), ROWS)
        for j in range(pl.cdiv(vl, LANES)):
            w = min(LANES, vl - j * LANES)
            staged[b, :, j * LANES:j * LANES + w] = (z_ref[rows, j * LANES:j * LANES + w] * SCALE) * inv[:, 0:w]
        staged_copy(b).start()
        return c
    lax.fori_loop(0, n, one, 0)

    seq_of = lax.broadcasted_iota(jnp.int32, (n, width), 1) // ROWS == lax.broadcasted_iota(jnp.int32, (n, width), 0)
    pos_of = lax.broadcasted_iota(jnp.int32, (ROWS, width), 1) % ROWS == lax.broadcasted_iota(jnp.int32, (ROWS, width), 0)
    to_seq = (lax.broadcasted_iota(jnp.int32, (width, n), 0) // ROWS
              == lax.broadcasted_iota(jnp.int32, (width, n), 1)).astype(jnp.float32)
    by_seq = jnp.zeros((n, num_draft), jnp.float32)
    by_pos = []
    for g in range(phases):
        a = jnp.minimum(1.0, tot_ref[g, 1:2, :] / tot_ref[g, 2:3, :])
        to_pos = (lax.broadcasted_iota(jnp.int32, (width, num_draft), 0) % ROWS + g * ROWS
                  == lax.broadcasted_iota(jnp.int32, (width, num_draft), 1)).astype(jnp.float32)
        by_seq = by_seq + jnp.dot(jnp.where(seq_of, jnp.broadcast_to(a, (n, width)), 0.0), to_pos,
                                  precision=lax.Precision.HIGHEST, preferred_element_type=jnp.float32)
        by_pos.append(jnp.dot(jnp.where(pos_of, jnp.broadcast_to(a, (ROWS, width)), 0.0), to_seq,
                              precision=lax.Precision.HIGHEST, preferred_element_type=jnp.float32))
    accepted[...] = by_seq
    accept_copy = pltpu.make_async_copy(accepted, accept_ref, small_sem.at[0])
    accept_copy.start()
    product = by_pos[0][0:1, :]
    total = product
    for k in range(1, num_draft):
        product = product * by_pos[k // ROWS][k % ROWS:k % ROWS + 1, :]
        total = total + product
    expected[...] = total
    expected_copy = pltpu.make_async_copy(expected, expected_ref, small_sem.at[1])
    expected_copy.start()

    def finished(b, c):
        for g in range(last):
            ready_copy(g, b).wait()
        staged_copy(b).wait()
        return c
    lax.fori_loop(0, n, finished, 0)
    bonus_copy.wait()
    accept_copy.wait()
    expected_copy.wait()


def solution(mesh):
    n = mesh.shape["tpa"] * mesh.shape["tpb"]

    def local_step(hidden, w_head, q_draft, x_draft):
        seqs, positions, depth = hidden.shape
        vl = w_head.shape[1]
        num_draft = x_draft.shape[1]
        phases = num_draft // ROWS
        vp = pl.cdiv(vl, LANES) * LANES
        rows = seqs * positions
        stat_rows = pl.cdiv(rows, LANES) * LANES
        f32 = jnp.float32
        any_spec = pl.BlockSpec(memory_space=pl.ANY)
        vmem_spec = pl.BlockSpec(memory_space=pltpu.VMEM)
        z, tot = pl.pallas_call(
            functools.partial(exchange_kernel, n, phases, vl),
            name="exchange",
            out_shape=(pltpu.VMEM((rows, vl), f32), pltpu.VMEM((phases, 3, LANES), f32)),
            in_specs=[any_spec] * 4,
            out_specs=(vmem_spec, vmem_spec),
            scratch_shapes=[
                pltpu.VMEM((rows, depth), jnp.bfloat16),
                pltpu.VMEM((rows, depth), jnp.bfloat16),
                pltpu.VMEM((W_BUFS, W_ROWS, depth), jnp.bfloat16),
                pltpu.VMEM((phases, n, ROWS, vp + LANES), f32),
                pltpu.VMEM((phases, n, ROWS, vp), f32),
                pltpu.VMEM((seqs, num_draft), jnp.int32),
                pltpu.VMEM((stat_rows, LANES), f32),
                pltpu.VMEM((stat_rows, LANES), f32),
                pltpu.VMEM((stat_rows, LANES), f32),
                pltpu.VMEM((phases * n * ROWS, LANES), f32),
                pltpu.VMEM((2, 2, stat_rows // LANES, LANES), f32),
                pltpu.VMEM((n // 2, 2, stat_rows // LANES // 2, LANES), f32),
                pltpu.VMEM((2, 2, stat_rows // LANES // 2, LANES), f32),
                pltpu.VMEM((2, 2, 3, LANES), f32),
                pltpu.VMEM((n // 2, 3, LANES), f32),
                pltpu.VMEM((2, 3, LANES), f32),
                pltpu.VMEM((n, 3, LANES), f32),
                pltpu.SemaphoreType.DMA((2,)),
                pltpu.SemaphoreType.DMA((W_BUFS,)),
                pltpu.SemaphoreType.DMA((phases, n)),
                pltpu.SemaphoreType.DMA((phases, n)),
                pltpu.SemaphoreType.DMA((phases, n)),
                pltpu.SemaphoreType.DMA((4,)),
                pltpu.SemaphoreType.DMA((4,)),
                pltpu.SemaphoreType.DMA((2, n // 2)),
                pltpu.SemaphoreType.DMA((2, n // 2)),
                pltpu.SemaphoreType.DMA((n,)),
                pltpu.SemaphoreType.DMA((n,)),
            ],
            compiler_params=pltpu.CompilerParams(collective_id=0, has_side_effects=True, vmem_limit_bytes=48 * 2**20),
        )(hidden.transpose(1, 0, 2).reshape(rows, depth), w_head.T, q_draft.reshape(num_draft, q_draft.shape[2]), x_draft)
        residual, bonus, accept, expected = pl.pallas_call(
            functools.partial(finish_kernel, n, phases, vl),
            name="finish",
            out_shape=(jax.ShapeDtypeStruct((seqs, num_draft, vl), f32), jax.ShapeDtypeStruct((seqs, vl), f32),
                       jax.ShapeDtypeStruct((seqs, num_draft), f32), jax.ShapeDtypeStruct((1, seqs), f32)),
            in_specs=[vmem_spec, vmem_spec],
            out_specs=(any_spec,) * 4,
            scratch_shapes=[pltpu.VMEM((n * ROWS, LANES), f32), pltpu.VMEM((seqs, ROWS, vl), f32),
                            pltpu.VMEM((seqs, num_draft), f32), pltpu.VMEM((1, seqs), f32),
                            pltpu.SemaphoreType.DMA((phases, seqs)), pltpu.SemaphoreType.DMA, pltpu.SemaphoreType.DMA((2,))],
            compiler_params=pltpu.CompilerParams(vmem_limit_bytes=32 * 2**20),
        )(tot, z)
        return accept, expected.reshape(seqs), residual, bonus

    return jax.shard_map(
        local_step, mesh=mesh,
        in_specs=(P("dp", None, None), P(None, VOCAB_AXES), P(("dp",) + VOCAB_AXES, None, None), P("dp", None)),
        out_specs=(P("dp", None), P("dp"), P("dp", None, VOCAB_AXES), P("dp", VOCAB_AXES)),
        check_vma=False)
```

```python
import functools

import jax
import jax.numpy as jnp
from jax import lax
from jax.experimental import pallas as pl
from jax.experimental.pallas import tpu as pltpu
from jax.sharding import PartitionSpec as P

INV_TEMP = 1.25
VOCAB_AXES = ("tpa", "tpb")
MESH = pl.DeviceIdType.MESH
LANES = 128
ROWS = 8
W_ROWS = 256
W_BUFS = 4
AHEAD = 4
SCALE = 2.0 ** 64


def xor4(a, r):
    low = lax.rem(lax.rem(a, 2) + lax.rem(r, 2), 2)
    high = lax.rem(lax.div(a, 2) + lax.div(r, 2), 2)
    return low + 2 * high


def exchange_kernel(n, phases, vl, hid_ref, w_ref, q_ref, x_ref, z_ref, tot_ref,
                    hid_v, hs, wbuf, sbuf, qbuf, x_v, colmax, colsum, scale, part, stat_core, stat_chip, stat_half, sum_core, sum_chip, sum_half, zmsg,
                    in_sem, w_sem, ld_sem, qs_sem, qr_sem, swap_s, swap_r, chip_s, chip_r, zs_sem, zr_sem):
    vp = qbuf.shape[3]
    tiles = vp // LANES
    last = vl - (tiles - 1) * LANES
    rows_all = z_ref.shape[0]
    draft_rows = phases * n * ROWS
    my_a, my_b = lax.axis_index("tpa"), lax.axis_index("tpb")
    me = my_a * 4 + my_b
    lane = lax.broadcasted_iota(jnp.int32, (ROWS, LANES), 1)

    def flip(a, r):
        return (a, a + 1 - 2 * lax.rem(a, 2), lax.rem(a + 2, 4), 3 - a)[r]

    def peer(r):
        if isinstance(r, int):
            return flip(my_a, r // 4), flip(my_b, r % 4)
        return xor4(my_a, lax.div(r, 4)), xor4(my_b, lax.rem(r, 4))

    def window(k):
        col = lax.div(k * vl, LANES) * LANES
        return pl.multiple_of(col, LANES), k * vl - col

    def sized(k, body):
        _, o = window(k)
        wide = o + vl > vp
        pl.when(wide)(lambda: body(vp + LANES))
        pl.when(jnp.logical_not(wide))(lambda: body(vp))

    core = lax.rem(my_b, 2)
    inner = lax.rem(lax.div(my_a + 1, 2), 2)

    def nth(stage, i):
        r = inner * lax.rem((n // 2 + 1) * (i + core) + n // 2, n) + (1 - inner) * i
        if stage == 1:
            far = lax.div(r, n // 2)
            r = (1 - far) * r + far * (n // 2 + lax.rem(r + (1 - inner) * (n // 4), n // 2))
        return r

    def arrival_order(g, i):
        far = lax.div(i, n // 2)
        return i if g < phases - 1 else (1 - far) * i + far * (n // 2 + lax.rem(i + n // 4, n // 2))

    def load(g, k, width):
        col, _ = window(k)
        return pltpu.make_async_copy(q_ref.at[g * ROWS:(g + 1) * ROWS, pl.ds(col, width)], sbuf.at[g, k, :, pl.ds(0, width)], ld_sem.at[g, k])

    def q_copy(stage, r, s):
        a, b = peer(r)
        k = a * 4 + b
        if stage == 0:
            src, dst = sbuf.at[0:phases - 1, k, :, pl.ds(0, vp)], qbuf.at[0:phases - 1, s]
        else:
            src, dst = sbuf.at[phases - 1, k, :, pl.ds(0, vp - LANES)], qbuf.at[phases - 1, s, :, pl.ds(0, vp - LANES)]
        return pltpu.make_async_remote_copy(
            src_ref=src, dst_ref=dst, send_sem=qs_sem.at[stage, r], recv_sem=qr_sem.at[stage, s],
            device_id={"tpa": a, "tpb": b}, device_id_type=MESH)

    def tile_of(j):
        return slice(j * LANES, (j + 1) * LANES)

    def part_of(j):
        return slice(j * LANES, min((j + 1) * LANES, vl))

    free = LANES - last

    def prepare(g, k):
        _, o = window(k)
        shift = lax.rem(LANES - o, LANES)

        def last_tile(h):
            return jnp.where(lane < LANES - o, pltpu.roll(sbuf[h, k, :, tile_of(tiles - 1)], shift, 1),
                             pltpu.roll(sbuf[h, k, :, tile_of(tiles)], shift, 1))
        ending = last_tile(g)
        if g < phases - 1:
            guest = pltpu.roll(last_tile(phases - 1), last if g == 0 else LANES - (free - last) % LANES, 1)
            ending = jnp.where(lane < last, ending, guest)
        this = pltpu.roll(sbuf[g, k, :, tile_of(0)], shift, 1)
        for j in range(tiles - 1):
            following = pltpu.roll(sbuf[g, k, :, tile_of(j + 1)], shift, 1)
            sbuf[g, k, :, tile_of(j)] = jnp.where(lane < LANES - o, this, following)
            this = following
        sbuf[g, k, :, tile_of(tiles - 1)] = ending

    def ready(stage, i):
        r = nth(stage, i)
        a, b = peer(r)
        k = a * 4 + b
        if stage == 0:
            @pl.when(i + AHEAD < n)
            def _():
                start_load(i + AHEAD)
            for g in range(phases):
                sized(k, lambda width, g=g: load(g, k, width).wait())
        for g in range(phases - 1) if stage == 0 else (phases - 1,):
            prepare(g, k)

            @pl.when(r == 0)
            def _(g=g):
                for j in range(tiles):
                    qbuf[g, me, :, tile_of(j)] = sbuf[g, me, :, tile_of(j)]

    def first(stage):
        lax.fori_loop(0, 2, lambda i, c: (ready(stage, i), c)[1], 0)

    def send_stage(stage):
        def one(i, c):
            r = nth(stage, i)

            @pl.when(r > 0)
            def _():
                q_copy(stage, r, me).start()

            @pl.when(i + 2 < n)
            def _():
                ready(stage, i + 2)
            return c
        lax.fori_loop(0, n, one, 0)

    def w_copy(c, slot):
        return pltpu.make_async_copy(w_ref.at[pl.ds(pl.multiple_of(c * W_ROWS, W_ROWS), W_ROWS), :], wbuf.at[slot], w_sem.at[slot])

    full_chunks = vl // W_ROWS
    w_tail = vl - full_chunks * W_ROWS
    tail_slot = full_chunks % W_BUFS
    tail_copy = pltpu.make_async_copy(
        w_ref.at[pl.ds(full_chunks * W_ROWS, w_tail), :], wbuf.at[tail_slot, pl.ds(0, w_tail), :], w_sem.at[tail_slot])

    hid_copy = pltpu.make_async_copy(hid_ref, hid_v, in_sem.at[0])
    x_copy = pltpu.make_async_copy(x_ref, x_v, in_sem.at[1])
    barrier = pltpu.get_barrier_semaphore()

    for r in range(n - 1, 0, -1):
        a, b = peer(r)
        pl.semaphore_signal(barrier, inc=1, device_id={"tpa": a, "tpb": b}, device_id_type=MESH)

    def start_load(i):
        a, b = peer(nth(0, i))
        k = a * 4 + b
        for g in range(phases):
            sized(k, lambda width, g=g: load(g, k, width).start())

    for i in range(AHEAD):
        start_load(i)
    x_copy.start()
    first(0)
    pl.semaphore_wait(barrier, n - 1)

    send_stage(0)
    hid_copy.start()
    for c in range(W_BUFS):
        w_copy(c, c).start()

    hid_copy.wait()
    row = lax.broadcasted_iota(jnp.int32, (rows_all, rows_all), 0)
    col = lax.broadcasted_iota(jnp.int32, (rows_all, rows_all), 1)
    source = jnp.where(row < draft_rows, ((row // (n * ROWS)) * ROWS + row % ROWS) * n + (row // ROWS) % n, row)
    permute = jnp.where(col == source, 1.0, 0.0).astype(jnp.bfloat16)
    depth = hid_v.shape[1]

    def permute_columns(c, carry):
        at = pl.ds(pl.multiple_of(c * 256, 256), 256)
        hs[:, at] = jnp.dot(permute, hid_v[:, at], preferred_element_type=jnp.float32).astype(jnp.bfloat16)
        return carry
    lax.fori_loop(0, depth // 256, permute_columns, 0)

    nt = (((1,), (1,)), ((), ()))

    def logits(c, carry):
        slot = lax.rem(c, W_BUFS)
        w_copy(c, slot).wait()
        z_ref[:, pl.ds(pl.multiple_of(c * W_ROWS, W_ROWS), W_ROWS)] = lax.dot_general(
            hs[...], wbuf[slot], nt, preferred_element_type=jnp.float32) * INV_TEMP

        @pl.when(c + W_BUFS < full_chunks)
        def _():
            w_copy(c + W_BUFS, slot).start()

        @pl.when(c + W_BUFS == full_chunks)
        def _():
            tail_copy.start()
        return carry
    lax.fori_loop(0, full_chunks, logits, 0)
    tail_copy.wait()
    z_ref[:, full_chunks * W_ROWS:vl] = lax.dot_general(
        hs[...], wbuf[tail_slot, 0:w_tail, :], nt, preferred_element_type=jnp.float32) * INV_TEMP

    def row_stats(t, carry):
        rows = pl.ds(pl.multiple_of(t * ROWS, ROWS), ROWS)
        ending = z_ref[rows, part_of(tiles - 1)]
        m = z_ref[rows, part_of(0)]
        for j in range(1, tiles - 1):
            m = jnp.maximum(m, z_ref[rows, part_of(j)])
        m = jnp.maximum(jnp.max(m, axis=1, keepdims=True), jnp.max(ending, axis=1, keepdims=True))
        m = jnp.broadcast_to(m, (ROWS, LANES))
        ending = jnp.exp(ending - m[:, 0:last])
        z_ref[rows, part_of(tiles - 1)] = ending
        s = jnp.zeros((ROWS, LANES), jnp.float32)
        for j in range(tiles - 1):
            e = jnp.exp(z_ref[rows, part_of(j)] - m)
            z_ref[rows, part_of(j)] = e
            s = s + e
        s = jnp.sum(s, axis=1, keepdims=True) + jnp.sum(ending, axis=1, keepdims=True)
        colmax[rows, :] = m
        colsum[rows, :] = jnp.broadcast_to(s, (ROWS, LANES))
        return carry
    lax.fori_loop(0, rows_all // ROWS, row_stats, 0)
    chip = my_a * 2 + lax.div(my_b, 2)
    chips = n // 2

    def swap(i, ref):
        return pltpu.make_async_remote_copy(
            src_ref=ref.at[core], dst_ref=ref.at[core], send_sem=swap_s.at[i], recv_sem=swap_r.at[i],
            device_id={"tpa": my_a, "tpb": my_b + 1 - 2 * core}, device_id_type=MESH)

    def swap_arrival(i, ref):
        return pltpu.make_async_remote_copy(
            src_ref=ref.at[1 - core], dst_ref=ref.at[1 - core], send_sem=swap_s.at[i], recv_sem=swap_r.at[i],
            device_id={"tpa": my_a, "tpb": my_b}, device_id_type=MESH)

    def chip_copy(i, ref, h, slot):
        a, b = peer(2 * h)
        return pltpu.make_async_remote_copy(
            src_ref=ref.at[chip], dst_ref=ref.at[slot], send_sem=chip_s.at[i, h], recv_sem=chip_r.at[i, slot],
            device_id={"tpa": a, "tpb": b}, device_id_type=MESH)

    def chip_send(i, ref):
        for h in range(chips - 1, 0, -1):
            chip_copy(i, ref, h, chip).start()

    def chip_arrivals(i, ref):
        for h in range(1, chips):
            a, b = peer(2 * h)
            chip_copy(i, ref, h, a * 2 + lax.div(b, 2)).wait_recv()

    def combine(pairs):
        top = pairs[0][0]
        for m, _ in pairs[1:]:
            top = jnp.maximum(top, m)
        total = jnp.zeros_like(top)
        for m, s in pairs:
            total = total + s * jnp.exp(m - top)
        return top, total

    spare = colmax.shape[0] - rows_all
    colmax[rows_all:, :] = jnp.zeros((spare, LANES), jnp.float32)
    colsum[rows_all:, :] = jnp.ones((spare, LANES), jnp.float32)

    blocks = colmax.shape[0] // LANES

    def as_rows(ref):
        return jnp.concatenate([ref[i * LANES:(i + 1) * LANES, :].T[0:1, :] for i in range(blocks)], axis=0)
    my_max = as_rows(colmax)
    stat_core[core, 0] = my_max
    stat_core[core, 1] = as_rows(colsum)
    swap(0, stat_core).start()
    swap_arrival(0, stat_core).wait_recv()
    top, total = combine([(stat_core[c, 0], stat_core[c, 1]) for c in range(2)])
    half = blocks // 2
    mine = core == 0
    stat_chip[chip, 0] = jnp.where(mine, top[0:half], top[half:])
    stat_chip[chip, 1] = jnp.where(mine, total[0:half], total[half:])
    chip_send(0, stat_chip)
    first(1)
    send_stage(1)

    chip_arrivals(0, stat_chip)
    top, total = combine([(stat_chip[c, 0], stat_chip[c, 1]) for c in range(chips)])
    stat_half[core, 0] = top
    stat_half[core, 1] = total
    swap(1, stat_half).start()
    swap_arrival(1, stat_half).wait_recv()
    top = jnp.concatenate([stat_half[0, 0], stat_half[1, 0]], axis=0)
    total = jnp.concatenate([stat_half[0, 1], stat_half[1, 1]], axis=0)
    factor = jnp.exp(stat_core[core, 0] - top) / total
    for i in range(blocks):
        scale[i * LANES:(i + 1) * LANES, :] = jnp.broadcast_to(factor[i:i + 1, :], (LANES, LANES)).T

    for t in range(draft_rows // ROWS, rows_all // ROWS):
        rows = slice(t * ROWS, (t + 1) * ROWS)
        for j in range(tiles):
            value = z_ref[rows, part_of(j)]
            z_ref[rows, part_of(j)] = value * scale[rows, 0:value.shape[1]]

    x_copy.wait()
    lane_f = lane.astype(jnp.float32)
    num_draft = x_v.shape[1]

    def excess(g, s):
        rows = pl.ds(pl.multiple_of(g * (n * ROWS) + s * ROWS, ROWS), ROWS)
        tokens = jnp.broadcast_to(x_v[pl.ds(s, 1), :].astype(jnp.float32), (ROWS, num_draft))
        position = lax.broadcasted_iota(jnp.int32, (ROWS, num_draft), 0) + g * ROWS
        here = lax.broadcasted_iota(jnp.int32, (ROWS, num_draft), 1) == position
        token = jnp.sum(jnp.where(here, tokens, 0.0), axis=1, keepdims=True) - (me * vl).astype(jnp.float32)
        token = jnp.broadcast_to(jnp.where(token < vl, token, -1.0), (ROWS, LANES))
        sc = scale[rows, :]
        z_sum = p_pick = q_pick = jnp.zeros((ROWS, LANES), jnp.float32)
        for j in range(tiles - 1):
            q = qbuf[g, s, :, tile_of(j)]
            p = z_ref[rows, part_of(j)] * sc
            d = jnp.maximum(p - q, 0.0)
            z_ref[rows, part_of(j)] = d
            z_sum = z_sum + d
            hit = lane_f == token - float(j * LANES)
            p_pick = jnp.where(hit, p, p_pick)
            q_pick = jnp.where(hit, q, q_pick)
        j = tiles - 1
        if g < phases - 1:
            q = qbuf[g, s, :, tile_of(j)]
        else:
            q = jnp.where(lane < free, pltpu.roll(qbuf[0, s, :, tile_of(j)], free, 1),
                          pltpu.roll(qbuf[1, s, :, tile_of(j)], (free - last) % LANES, 1))
        q = q[:, 0:last]
        p = z_ref[rows, part_of(j)] * sc[:, 0:last]
        d = jnp.maximum(p - q, 0.0)
        z_ref[rows, part_of(j)] = d
        hit = (lane_f == token - float(j * LANES))[:, 0:last]
        sums = [jnp.sum(whole, axis=1, keepdims=True) + jnp.sum(ending, axis=1, keepdims=True)
                for whole, ending in ((z_sum, d), (p_pick, jnp.where(hit, p, 0.0)), (q_pick, jnp.where(hit, q, 0.0)))]
        part[rows, :] = jnp.where(lane == 0, sums[0], jnp.where(lane == 1, sums[1], sums[2]))

    def z_copy(r, s):
        a, b = peer(r)
        return pltpu.make_async_remote_copy(
            src_ref=zmsg.at[me], dst_ref=zmsg.at[s], send_sem=zs_sem.at[r], recv_sem=zr_sem.at[s],
            device_id={"tpa": a, "tpb": b}, device_id_type=MESH)

    def row_sums(g):
        block = slice(g * n * ROWS, (g + 1) * n * ROWS)
        return part[block, :].T[0:3, :]

    for g in range(phases):
        def one(i, c, g=g):
            r = arrival_order(g, i)
            a, b = peer(r)
            s = a * 4 + b

            if g in (0, phases - 1):
                @pl.when(r > 0)
                def _():
                    q_copy(min(g, 1), r, s).wait_recv()
            excess(g, s)
            return c
        lax.fori_loop(0, n, one, 0)
        if g == phases - 2:
            for h in range(2):
                sum_core[core, h] = row_sums(h)
            swap(2, sum_core).start()
            swap_arrival(2, sum_core).wait_recv()
            sum_chip[chip] = jnp.where(mine, sum_core[0, 0] + sum_core[1, 0], sum_core[0, 1] + sum_core[1, 1])
            chip_send(1, sum_chip)
    zmsg[me] = row_sums(phases - 1)
    for r in range(n - 1, 0, -1):
        z_copy(r, me).start()

    def drain(r, c):
        for stage in range(2):
            q_copy(stage, r, me).wait_send()
        z_copy(r, me).wait_send()
        return c

    def divide(g):
        inverse = jnp.broadcast_to(1.0 / (tot_ref[g, 0:1, :] * SCALE), (n * ROWS, LANES)).T
        scale[0:n * ROWS, :] = inverse

        def one(s, c):
            rows = pl.ds(pl.multiple_of(g * (n * ROWS) + s * ROWS, ROWS), ROWS)
            inv = scale[pl.ds(pl.multiple_of(s * ROWS, ROWS), ROWS), :]
            for j in range(tiles):
                value = z_ref[rows, part_of(j)] * SCALE
                z_ref[rows, part_of(j)] = value * inv[:, 0:value.shape[1]]
            return c
        lax.fori_loop(0, n, one, 0)

    chip_arrivals(1, sum_chip)
    total = sum_chip[0]
    for c in range(1, chips):
        total = total + sum_chip[c]
    sum_half[core] = total
    swap(3, sum_half).start()
    swap_arrival(3, sum_half).wait_recv()
    for g in range(phases - 1):
        tot_ref[g] = sum_half[g]
        divide(g)
    lax.fori_loop(1, n, drain, 0)
    for i, ref in enumerate((stat_core, stat_half, sum_core, sum_half)):
        swap(i, ref).wait_send()
    for i, ref in enumerate((stat_chip, sum_chip)):
        for h in range(1, chips):
            chip_copy(i, ref, h, chip).wait_send()
    for r in range(1, n):
        a, b = peer(r)
        z_copy(r, a * 4 + b).wait_recv()
    total = zmsg[0]
    for s in range(1, n):
        total = total + zmsg[s]
    tot_ref[phases - 1] = total


def finish_kernel(n, phases, vl, tot_ref, z_ref, res_ref, bonus_ref, accept_ref, expected_ref, inverse, staged, accepted, expected, sem, bonus_sem, small_sem):
    width = n * ROWS
    num_draft = phases * ROWS
    last = phases - 1

    def ready_copy(g, b):
        return pltpu.make_async_copy(z_ref.at[pl.ds(pl.multiple_of(g * width + b * ROWS, ROWS), ROWS), :],
                                     res_ref.at[b, g * ROWS:(g + 1) * ROWS, :], sem.at[g, b])

    def staged_copy(b):
        return pltpu.make_async_copy(staged.at[b], res_ref.at[b, last * ROWS:, :], sem.at[last, b])

    bonus_copy = pltpu.make_async_copy(z_ref.at[phases * width:phases * width + n, :], bonus_ref, bonus_sem)

    def start(b, c):
        for g in range(last):
            ready_copy(g, b).start(priority=g % 2)
        return c
    lax.fori_loop(0, n, start, 0)
    bonus_copy.start()
    inverse[...] = jnp.broadcast_to(1.0 / (tot_ref[last, 0:1, :] * SCALE), (width, LANES)).T

    def one(b, c):
        inv = inverse[pl.ds(pl.multiple_of(b * ROWS, ROWS), ROWS), :]
        rows = pl.ds(pl.multiple_of(last * width + b * ROWS, ROWS), ROWS)
        for j in range(pl.cdiv(vl, LANES)):
            w = min(LANES, vl - j * LANES)
            staged[b, :, j * LANES:j * LANES + w] = (z_ref[rows, j * LANES:j * LANES + w] * SCALE) * inv[:, 0:w]
        staged_copy(b).start()
        return c
    lax.fori_loop(0, n, one, 0)

    seq_of = lax.broadcasted_iota(jnp.int32, (n, width), 1) // ROWS == lax.broadcasted_iota(jnp.int32, (n, width), 0)
    pos_of = lax.broadcasted_iota(jnp.int32, (ROWS, width), 1) % ROWS == lax.broadcasted_iota(jnp.int32, (ROWS, width), 0)
    to_seq = (lax.broadcasted_iota(jnp.int32, (width, n), 0) // ROWS
              == lax.broadcasted_iota(jnp.int32, (width, n), 1)).astype(jnp.float32)
    by_seq = jnp.zeros((n, num_draft), jnp.float32)
    by_pos = []
    for g in range(phases):
        a = jnp.minimum(1.0, tot_ref[g, 1:2, :] / tot_ref[g, 2:3, :])
        to_pos = (lax.broadcasted_iota(jnp.int32, (width, num_draft), 0) % ROWS + g * ROWS
                  == lax.broadcasted_iota(jnp.int32, (width, num_draft), 1)).astype(jnp.float32)
        by_seq = by_seq + jnp.dot(jnp.where(seq_of, jnp.broadcast_to(a, (n, width)), 0.0), to_pos,
                                  precision=lax.Precision.HIGHEST, preferred_element_type=jnp.float32)
        by_pos.append(jnp.dot(jnp.where(pos_of, jnp.broadcast_to(a, (ROWS, width)), 0.0), to_seq,
                              precision=lax.Precision.HIGHEST, preferred_element_type=jnp.float32))
    accepted[...] = by_seq
    accept_copy = pltpu.make_async_copy(accepted, accept_ref, small_sem.at[0])
    accept_copy.start()
    product = by_pos[0][0:1, :]
    total = product
    for k in range(1, num_draft):
        product = product * by_pos[k // ROWS][k % ROWS:k % ROWS + 1, :]
        total = total + product
    expected[...] = total
    expected_copy = pltpu.make_async_copy(expected, expected_ref, small_sem.at[1])
    expected_copy.start()

    def finished(b, c):
        for g in range(last):
            ready_copy(g, b).wait()
        staged_copy(b).wait()
        return c
    lax.fori_loop(0, n, finished, 0)
    bonus_copy.wait()
    accept_copy.wait()
    expected_copy.wait()


def solution(mesh):
    n = mesh.shape["tpa"] * mesh.shape["tpb"]

    def local_step(hidden, w_head, q_draft, x_draft):
        seqs, positions, depth = hidden.shape
        vl = w_head.shape[1]
        num_draft = x_draft.shape[1]
        phases = num_draft // ROWS
        vp = pl.cdiv(vl, LANES) * LANES
        rows = seqs * positions
        stat_rows = pl.cdiv(rows, LANES) * LANES
        f32 = jnp.float32
        any_spec = pl.BlockSpec(memory_space=pl.ANY)
        vmem_spec = pl.BlockSpec(memory_space=pltpu.VMEM)
        z, tot = pl.pallas_call(
            functools.partial(exchange_kernel, n, phases, vl),
            name="exchange",
            out_shape=(pltpu.VMEM((rows, vl), f32), pltpu.VMEM((phases, 3, LANES), f32)),
            in_specs=[any_spec] * 4,
            out_specs=(vmem_spec, vmem_spec),
            scratch_shapes=[
                pltpu.VMEM((rows, depth), jnp.bfloat16),
                pltpu.VMEM((rows, depth), jnp.bfloat16),
                pltpu.VMEM((W_BUFS, W_ROWS, depth), jnp.bfloat16),
                pltpu.VMEM((phases, n, ROWS, vp + LANES), f32),
                pltpu.VMEM((phases, n, ROWS, vp), f32),
                pltpu.VMEM((seqs, num_draft), jnp.int32),
                pltpu.VMEM((stat_rows, LANES), f32),
                pltpu.VMEM((stat_rows, LANES), f32),
                pltpu.VMEM((stat_rows, LANES), f32),
                pltpu.VMEM((phases * n * ROWS, LANES), f32),
                pltpu.VMEM((2, 2, stat_rows // LANES, LANES), f32),
                pltpu.VMEM((n // 2, 2, stat_rows // LANES // 2, LANES), f32),
                pltpu.VMEM((2, 2, stat_rows // LANES // 2, LANES), f32),
                pltpu.VMEM((2, 2, 3, LANES), f32),
                pltpu.VMEM((n // 2, 3, LANES), f32),
                pltpu.VMEM((2, 3, LANES), f32),
                pltpu.VMEM((n, 3, LANES), f32),
                pltpu.SemaphoreType.DMA((2,)),
                pltpu.SemaphoreType.DMA((W_BUFS,)),
                pltpu.SemaphoreType.DMA((phases, n)),
                pltpu.SemaphoreType.DMA((2, n)),
                pltpu.SemaphoreType.DMA((2, n)),
                pltpu.SemaphoreType.DMA((4,)),
                pltpu.SemaphoreType.DMA((4,)),
                pltpu.SemaphoreType.DMA((2, n // 2)),
                pltpu.SemaphoreType.DMA((2, n // 2)),
                pltpu.SemaphoreType.DMA((n,)),
                pltpu.SemaphoreType.DMA((n,)),
            ],
            compiler_params=pltpu.CompilerParams(collective_id=0, has_side_effects=True, vmem_limit_bytes=48 * 2**20),
        )(hidden.transpose(1, 0, 2).reshape(rows, depth), w_head.T, q_draft.reshape(num_draft, q_draft.shape[2]), x_draft)
        residual, bonus, accept, expected = pl.pallas_call(
            functools.partial(finish_kernel, n, phases, vl),
            name="finish",
            out_shape=(jax.ShapeDtypeStruct((seqs, num_draft, vl), f32), jax.ShapeDtypeStruct((seqs, vl), f32),
                       jax.ShapeDtypeStruct((seqs, num_draft), f32), jax.ShapeDtypeStruct((1, seqs), f32)),
            in_specs=[vmem_spec, vmem_spec],
            out_specs=(any_spec,) * 4,
            scratch_shapes=[pltpu.VMEM((n * ROWS, LANES), f32), pltpu.VMEM((seqs, ROWS, vl), f32),
                            pltpu.VMEM((seqs, num_draft), f32), pltpu.VMEM((1, seqs), f32),
                            pltpu.SemaphoreType.DMA((phases, seqs)), pltpu.SemaphoreType.DMA, pltpu.SemaphoreType.DMA((2,))],
            compiler_params=pltpu.CompilerParams(vmem_limit_bytes=32 * 2**20),
        )(tot, z)
        return accept, expected.reshape(seqs), residual, bonus

    return jax.shard_map(
        local_step, mesh=mesh,
        in_specs=(P("dp", None, None), P(None, VOCAB_AXES), P(("dp",) + VOCAB_AXES, None, None), P("dp", None)),
        out_specs=(P("dp", None), P("dp"), P("dp", None, VOCAB_AXES), P("dp", VOCAB_AXES)),
        check_vma=False)
```

```python
import functools

import jax
import jax.numpy as jnp
from jax import lax
from jax.experimental import pallas as pl
from jax.experimental.pallas import tpu as pltpu
from jax.sharding import PartitionSpec as P

INV_TEMP = 1.25
VOCAB_AXES = ("tpa", "tpb")
MESH = pl.DeviceIdType.MESH
LANES = 128
ROWS = 8
W_ROWS = 256
W_BUFS = 4
PIECES = 2
AHEAD = 4
SCALE = 2.0 ** 64


def xor4(a, r):
    low = lax.rem(lax.rem(a, 2) + lax.rem(r, 2), 2)
    high = lax.rem(lax.div(a, 2) + lax.div(r, 2), 2)
    return low + 2 * high


def exchange_kernel(n, phases, vl, hid_ref, w_ref, q_ref, x_ref, z_ref, tot_ref,
                    hid_v, hs, wbuf, sbuf, qbuf, x_v, colmax, colsum, scale, part, stat_core, stat_chip, stat_half, sum_core, sum_chip, sum_half, zmsg,
                    in_sem, w_sem, ld_sem, qs_sem, qr_sem, swap_s, swap_r, chip_s, chip_r, zs_sem, zr_sem):
    vp = qbuf.shape[3]
    tiles = vp // LANES
    last = vl - (tiles - 1) * LANES
    rows_all = z_ref.shape[0]
    draft_rows = phases * n * ROWS
    my_a, my_b = lax.axis_index("tpa"), lax.axis_index("tpb")
    me = my_a * 4 + my_b
    lane = lax.broadcasted_iota(jnp.int32, (ROWS, LANES), 1)

    def flip(a, r):
        return (a, a + 1 - 2 * lax.rem(a, 2), lax.rem(a + 2, 4), 3 - a)[r]

    def peer(r):
        if isinstance(r, int):
            return flip(my_a, r // 4), flip(my_b, r % 4)
        return xor4(my_a, lax.div(r, 4)), xor4(my_b, lax.rem(r, 4))

    def window(k):
        col = lax.div(k * vl, LANES) * LANES
        return pl.multiple_of(col, LANES), k * vl - col

    def sized(k, body):
        _, o = window(k)
        wide = o + vl > vp
        pl.when(wide)(lambda: body(vp + LANES))
        pl.when(jnp.logical_not(wide))(lambda: body(vp))

    core = lax.rem(my_b, 2)
    inner = lax.rem(lax.div(my_a + 1, 2), 2)

    def nth(g, i):
        r = inner * lax.rem((n // 2 + 1) * (i + core) + n // 2, n) + (1 - inner) * i
        if g == phases - 1:
            far = lax.div(r, n // 2)
            r = (1 - far) * r + far * (n // 2 + lax.rem(r + (1 - inner) * (n // 4), n // 2))
        return r

    def arrival_order(g, i):
        far = lax.div(i, n // 2)
        return i if g < phases - 1 else (1 - far) * i + far * (n // 2 + lax.rem(i + n // 4, n // 2))

    def width_of(g):
        return vp if g < phases - 1 else vp - LANES

    def load(g, k, width):
        col, _ = window(k)
        return pltpu.make_async_copy(q_ref.at[g * ROWS:(g + 1) * ROWS, pl.ds(col, width)], sbuf.at[g, k, :, pl.ds(0, width)], ld_sem.at[g, k])

    def q_copy(g, r, s):
        a, b = peer(r)
        return pltpu.make_async_remote_copy(
            src_ref=sbuf.at[g, a * 4 + b, :, pl.ds(0, width_of(g))], dst_ref=qbuf.at[g, s, :, pl.ds(0, width_of(g))],
            send_sem=qs_sem.at[g, r], recv_sem=qr_sem.at[g, s],
            device_id={"tpa": a, "tpb": b}, device_id_type=MESH)

    def q_piece(g, r, h):
        a, b = peer(r)
        cut = [tiles * i // PIECES * LANES for i in range(PIECES)] + [width_of(g)]
        at = pl.ds(cut[h], cut[h + 1] - cut[h])
        return pltpu.make_async_remote_copy(
            src_ref=sbuf.at[g, a * 4 + b, :, at], dst_ref=qbuf.at[g, me, :, at],
            send_sem=qs_sem.at[g, r], recv_sem=qr_sem.at[g, me],
            device_id={"tpa": a, "tpb": b}, device_id_type=MESH)

    def tile_of(j):
        return slice(j * LANES, (j + 1) * LANES)

    def part_of(j):
        return slice(j * LANES, min((j + 1) * LANES, vl))

    free = LANES - last

    def prepare(g, k):
        _, o = window(k)
        shift = lax.rem(LANES - o, LANES)

        def last_tile(h):
            return jnp.where(lane < LANES - o, pltpu.roll(sbuf[h, k, :, tile_of(tiles - 1)], shift, 1),
                             pltpu.roll(sbuf[h, k, :, tile_of(tiles)], shift, 1))
        ending = last_tile(g)
        if g < phases - 1:
            guest = pltpu.roll(last_tile(phases - 1), last if g == 0 else LANES - (free - last) % LANES, 1)
            ending = jnp.where(lane < last, ending, guest)
        this = pltpu.roll(sbuf[g, k, :, tile_of(0)], shift, 1)
        for j in range(tiles - 1):
            following = pltpu.roll(sbuf[g, k, :, tile_of(j + 1)], shift, 1)
            sbuf[g, k, :, tile_of(j)] = jnp.where(lane < LANES - o, this, following)
            this = following
        sbuf[g, k, :, tile_of(tiles - 1)] = ending

    def ready(g, i):
        if g < phases - 1:
            @pl.when(i + AHEAD < n)
            def _():
                start_load(g, i + AHEAD)
        r = nth(g, i)
        a, b = peer(r)
        k = a * 4 + b
        if g == 0:
            sized(k, lambda width: load(0, k, width).wait())
            sized(k, lambda width: load(phases - 1, k, width).wait())
        elif g < phases - 1:
            sized(k, lambda width: load(g, k, width).wait())
        prepare(g, k)

        @pl.when(r == 0)
        def _():
            for j in range(tiles):
                qbuf[g, me, :, tile_of(j)] = sbuf[g, me, :, tile_of(j)]

    def first(g):
        lax.fori_loop(0, 2, lambda i, c: (ready(g, i), c)[1], 0)

    def send_phase(g):
        for h in range(PIECES):
            def one(i, c, h=h):
                r = nth(g, i)

                @pl.when(r > 0)
                def _():
                    q_piece(g, r, h).start()

                if h == 0:
                    @pl.when(i + 2 < n)
                    def _():
                        ready(g, i + 2)
                return c
            lax.fori_loop(0, n, one, 0)

    def w_copy(c, slot):
        return pltpu.make_async_copy(w_ref.at[pl.ds(pl.multiple_of(c * W_ROWS, W_ROWS), W_ROWS), :], wbuf.at[slot], w_sem.at[slot])

    full_chunks = vl // W_ROWS
    w_tail = vl - full_chunks * W_ROWS
    tail_slot = full_chunks % W_BUFS
    tail_copy = pltpu.make_async_copy(
        w_ref.at[pl.ds(full_chunks * W_ROWS, w_tail), :], wbuf.at[tail_slot, pl.ds(0, w_tail), :], w_sem.at[tail_slot])

    hid_copy = pltpu.make_async_copy(hid_ref, hid_v, in_sem.at[0])
    x_copy = pltpu.make_async_copy(x_ref, x_v, in_sem.at[1])
    barrier = pltpu.get_barrier_semaphore()

    for r in range(n - 1, 0, -1):
        a, b = peer(r)
        pl.semaphore_signal(barrier, inc=1, device_id={"tpa": a, "tpb": b}, device_id_type=MESH)

    def start_load(g, i):
        a, b = peer(nth(g, i))
        k = a * 4 + b
        for h in (0, phases - 1) if g == 0 else (g,):
            sized(k, lambda width, h=h: load(h, k, width).start())

    for i in range(AHEAD):
        start_load(0, i)
    x_copy.start()
    first(0)
    pl.semaphore_wait(barrier, n - 1)

    send_phase(0)
    for g in range(1, phases - 1):
        for i in range(AHEAD):
            start_load(g, i)
    hid_copy.start()
    for c in range(W_BUFS):
        w_copy(c, c).start()
    for g in range(1, phases - 1):
        first(g)
        send_phase(g)

    hid_copy.wait()
    row = lax.broadcasted_iota(jnp.int32, (rows_all, rows_all), 0)
    col = lax.broadcasted_iota(jnp.int32, (rows_all, rows_all), 1)
    source = jnp.where(row < draft_rows, ((row // (n * ROWS)) * ROWS + row % ROWS) * n + (row // ROWS) % n, row)
    permute = jnp.where(col == source, 1.0, 0.0).astype(jnp.bfloat16)
    depth = hid_v.shape[1]

    def permute_columns(c, carry):
        at = pl.ds(pl.multiple_of(c * 256, 256), 256)
        hs[:, at] = jnp.dot(permute, hid_v[:, at], preferred_element_type=jnp.float32).astype(jnp.bfloat16)
        return carry
    lax.fori_loop(0, depth // 256, permute_columns, 0)

    nt = (((1,), (1,)), ((), ()))

    def logits(c, carry):
        slot = lax.rem(c, W_BUFS)
        w_copy(c, slot).wait()
        z_ref[:, pl.ds(pl.multiple_of(c * W_ROWS, W_ROWS), W_ROWS)] = lax.dot_general(
            hs[...], wbuf[slot], nt, preferred_element_type=jnp.float32) * INV_TEMP

        @pl.when(c + W_BUFS < full_chunks)
        def _():
            w_copy(c + W_BUFS, slot).start()

        @pl.when(c + W_BUFS == full_chunks)
        def _():
            tail_copy.start()
        return carry
    lax.fori_loop(0, full_chunks, logits, 0)
    tail_copy.wait()
    z_ref[:, full_chunks * W_ROWS:vl] = lax.dot_general(
        hs[...], wbuf[tail_slot, 0:w_tail, :], nt, preferred_element_type=jnp.float32) * INV_TEMP

    def row_stats(t, carry):
        rows = pl.ds(pl.multiple_of(t * ROWS, ROWS), ROWS)
        ending = z_ref[rows, part_of(tiles - 1)]
        m = z_ref[rows, part_of(0)]
        for j in range(1, tiles - 1):
            m = jnp.maximum(m, z_ref[rows, part_of(j)])
        m = jnp.maximum(jnp.max(m, axis=1, keepdims=True), jnp.max(ending, axis=1, keepdims=True))
        m = jnp.broadcast_to(m, (ROWS, LANES))
        ending = jnp.exp(ending - m[:, 0:last])
        z_ref[rows, part_of(tiles - 1)] = ending
        s = jnp.zeros((ROWS, LANES), jnp.float32)
        for j in range(tiles - 1):
            e = jnp.exp(z_ref[rows, part_of(j)] - m)
            z_ref[rows, part_of(j)] = e
            s = s + e
        s = jnp.sum(s, axis=1, keepdims=True) + jnp.sum(ending, axis=1, keepdims=True)
        colmax[rows, :] = m
        colsum[rows, :] = jnp.broadcast_to(s, (ROWS, LANES))
        return carry
    lax.fori_loop(0, rows_all // ROWS, row_stats, 0)
    chip = my_a * 2 + lax.div(my_b, 2)
    chips = n // 2

    def swap(i, ref):
        return pltpu.make_async_remote_copy(
            src_ref=ref.at[core], dst_ref=ref.at[core], send_sem=swap_s.at[i], recv_sem=swap_r.at[i],
            device_id={"tpa": my_a, "tpb": my_b + 1 - 2 * core}, device_id_type=MESH)

    def swap_arrival(i, ref):
        return pltpu.make_async_remote_copy(
            src_ref=ref.at[1 - core], dst_ref=ref.at[1 - core], send_sem=swap_s.at[i], recv_sem=swap_r.at[i],
            device_id={"tpa": my_a, "tpb": my_b}, device_id_type=MESH)

    def chip_copy(i, ref, h, slot):
        a, b = peer(2 * h)
        return pltpu.make_async_remote_copy(
            src_ref=ref.at[chip], dst_ref=ref.at[slot], send_sem=chip_s.at[i, h], recv_sem=chip_r.at[i, slot],
            device_id={"tpa": a, "tpb": b}, device_id_type=MESH)

    def chip_send(i, ref):
        for h in range(chips - 1, 0, -1):
            chip_copy(i, ref, h, chip).start()

    def chip_arrivals(i, ref):
        for h in range(1, chips):
            a, b = peer(2 * h)
            chip_copy(i, ref, h, a * 2 + lax.div(b, 2)).wait_recv()

    def combine(pairs):
        top = pairs[0][0]
        for m, _ in pairs[1:]:
            top = jnp.maximum(top, m)
        total = jnp.zeros_like(top)
        for m, s in pairs:
            total = total + s * jnp.exp(m - top)
        return top, total

    spare = colmax.shape[0] - rows_all
    colmax[rows_all:, :] = jnp.zeros((spare, LANES), jnp.float32)
    colsum[rows_all:, :] = jnp.ones((spare, LANES), jnp.float32)

    blocks = colmax.shape[0] // LANES

    def as_rows(ref):
        return jnp.concatenate([ref[i * LANES:(i + 1) * LANES, :].T[0:1, :] for i in range(blocks)], axis=0)
    my_max = as_rows(colmax)
    stat_core[core, 0] = my_max
    stat_core[core, 1] = as_rows(colsum)
    swap(0, stat_core).start()
    swap_arrival(0, stat_core).wait_recv()
    top, total = combine([(stat_core[c, 0], stat_core[c, 1]) for c in range(2)])
    half = blocks // 2
    mine = core == 0
    stat_chip[chip, 0] = jnp.where(mine, top[0:half], top[half:])
    stat_chip[chip, 1] = jnp.where(mine, total[0:half], total[half:])
    chip_send(0, stat_chip)
    first(phases - 1)
    send_phase(phases - 1)

    chip_arrivals(0, stat_chip)
    top, total = combine([(stat_chip[c, 0], stat_chip[c, 1]) for c in range(chips)])
    stat_half[core, 0] = top
    stat_half[core, 1] = total
    swap(1, stat_half).start()
    swap_arrival(1, stat_half).wait_recv()
    top = jnp.concatenate([stat_half[0, 0], stat_half[1, 0]], axis=0)
    total = jnp.concatenate([stat_half[0, 1], stat_half[1, 1]], axis=0)
    factor = jnp.exp(stat_core[core, 0] - top) / total
    for i in range(blocks):
        scale[i * LANES:(i + 1) * LANES, :] = jnp.broadcast_to(factor[i:i + 1, :], (LANES, LANES)).T

    for t in range(draft_rows // ROWS, rows_all // ROWS):
        rows = slice(t * ROWS, (t + 1) * ROWS)
        for j in range(tiles):
            value = z_ref[rows, part_of(j)]
            z_ref[rows, part_of(j)] = value * scale[rows, 0:value.shape[1]]

    x_copy.wait()
    lane_f = lane.astype(jnp.float32)
    num_draft = x_v.shape[1]

    def excess(g, s):
        rows = pl.ds(pl.multiple_of(g * (n * ROWS) + s * ROWS, ROWS), ROWS)
        tokens = jnp.broadcast_to(x_v[pl.ds(s, 1), :].astype(jnp.float32), (ROWS, num_draft))
        position = lax.broadcasted_iota(jnp.int32, (ROWS, num_draft), 0) + g * ROWS
        here = lax.broadcasted_iota(jnp.int32, (ROWS, num_draft), 1) == position
        token = jnp.sum(jnp.where(here, tokens, 0.0), axis=1, keepdims=True) - (me * vl).astype(jnp.float32)
        token = jnp.broadcast_to(jnp.where(token < vl, token, -1.0), (ROWS, LANES))
        sc = scale[rows, :]
        z_sum = p_pick = q_pick = jnp.zeros((ROWS, LANES), jnp.float32)
        for j in range(tiles - 1):
            q = qbuf[g, s, :, tile_of(j)]
            p = z_ref[rows, part_of(j)] * sc
            d = jnp.maximum(p - q, 0.0)
            z_ref[rows, part_of(j)] = d
            z_sum = z_sum + d
            hit = lane_f == token - float(j * LANES)
            p_pick = jnp.where(hit, p, p_pick)
            q_pick = jnp.where(hit, q, q_pick)
        j = tiles - 1
        if g < phases - 1:
            q = qbuf[g, s, :, tile_of(j)]
        else:
            q = jnp.where(lane < free, pltpu.roll(qbuf[0, s, :, tile_of(j)], free, 1),
                          pltpu.roll(qbuf[1, s, :, tile_of(j)], (free - last) % LANES, 1))
        q = q[:, 0:last]
        p = z_ref[rows, part_of(j)] * sc[:, 0:last]
        d = jnp.maximum(p - q, 0.0)
        z_ref[rows, part_of(j)] = d
        hit = (lane_f == token - float(j * LANES))[:, 0:last]
        sums = [jnp.sum(whole, axis=1, keepdims=True) + jnp.sum(ending, axis=1, keepdims=True)
                for whole, ending in ((z_sum, d), (p_pick, jnp.where(hit, p, 0.0)), (q_pick, jnp.where(hit, q, 0.0)))]
        part[rows, :] = jnp.where(lane == 0, sums[0], jnp.where(lane == 1, sums[1], sums[2]))

    def z_copy(r, s):
        a, b = peer(r)
        return pltpu.make_async_remote_copy(
            src_ref=zmsg.at[me], dst_ref=zmsg.at[s], send_sem=zs_sem.at[r], recv_sem=zr_sem.at[s],
            device_id={"tpa": a, "tpb": b}, device_id_type=MESH)

    def row_sums(g):
        block = slice(g * n * ROWS, (g + 1) * n * ROWS)
        return part[block, :].T[0:3, :]

    for g in range(phases):
        def one(i, c, g=g):
            r = arrival_order(g, i)
            a, b = peer(r)
            s = a * 4 + b

            @pl.when(r > 0)
            def _():
                q_copy(g, r, s).wait_recv()
            excess(g, s)
            return c
        lax.fori_loop(0, n, one, 0)
        if g == phases - 2:
            for h in range(2):
                sum_core[core, h] = row_sums(h)
            swap(2, sum_core).start()
            swap_arrival(2, sum_core).wait_recv()
            sum_chip[chip] = jnp.where(mine, sum_core[0, 0] + sum_core[1, 0], sum_core[0, 1] + sum_core[1, 1])
            chip_send(1, sum_chip)
    zmsg[me] = row_sums(phases - 1)
    for r in range(n - 1, 0, -1):
        z_copy(r, me).start()

    def drain(r, c):
        for g in range(phases):
            q_copy(g, r, me).wait_send()
        z_copy(r, me).wait_send()
        return c

    def divide(g):
        inverse = jnp.broadcast_to(1.0 / (tot_ref[g, 0:1, :] * SCALE), (n * ROWS, LANES)).T
        scale[0:n * ROWS, :] = inverse

        def one(s, c):
            rows = pl.ds(pl.multiple_of(g * (n * ROWS) + s * ROWS, ROWS), ROWS)
            inv = scale[pl.ds(pl.multiple_of(s * ROWS, ROWS), ROWS), :]
            for j in range(tiles):
                value = z_ref[rows, part_of(j)] * SCALE
                z_ref[rows, part_of(j)] = value * inv[:, 0:value.shape[1]]
            return c
        lax.fori_loop(0, n, one, 0)

    chip_arrivals(1, sum_chip)
    total = sum_chip[0]
    for c in range(1, chips):
        total = total + sum_chip[c]
    sum_half[core] = total
    swap(3, sum_half).start()
    swap_arrival(3, sum_half).wait_recv()
    for g in range(phases - 1):
        tot_ref[g] = sum_half[g]
        divide(g)
    lax.fori_loop(1, n, drain, 0)
    for i, ref in enumerate((stat_core, stat_half, sum_core, sum_half)):
        swap(i, ref).wait_send()
    for i, ref in enumerate((stat_chip, sum_chip)):
        for h in range(1, chips):
            chip_copy(i, ref, h, chip).wait_send()
    for r in range(1, n):
        a, b = peer(r)
        z_copy(r, a * 4 + b).wait_recv()
    total = zmsg[0]
    for s in range(1, n):
        total = total + zmsg[s]
    tot_ref[phases - 1] = total


def finish_kernel(n, phases, vl, tot_ref, z_ref, res_ref, bonus_ref, accept_ref, expected_ref, inverse, staged, accepted, expected, sem, bonus_sem, small_sem):
    width = n * ROWS
    num_draft = phases * ROWS
    last = phases - 1

    def ready_copy(g, b):
        return pltpu.make_async_copy(z_ref.at[pl.ds(pl.multiple_of(g * width + b * ROWS, ROWS), ROWS), :],
                                     res_ref.at[b, g * ROWS:(g + 1) * ROWS, :], sem.at[g, b])

    def staged_copy(b):
        return pltpu.make_async_copy(staged.at[b], res_ref.at[b, last * ROWS:, :], sem.at[last, b])

    bonus_copy = pltpu.make_async_copy(z_ref.at[phases * width:phases * width + n, :], bonus_ref, bonus_sem)

    def start(b, c):
        for g in range(last):
            ready_copy(g, b).start(priority=g % 2)
        return c
    lax.fori_loop(0, n, start, 0)
    bonus_copy.start()
    inverse[...] = jnp.broadcast_to(1.0 / (tot_ref[last, 0:1, :] * SCALE), (width, LANES)).T

    def one(b, c):
        inv = inverse[pl.ds(pl.multiple_of(b * ROWS, ROWS), ROWS), :]
        rows = pl.ds(pl.multiple_of(last * width + b * ROWS, ROWS), ROWS)
        for j in range(pl.cdiv(vl, LANES)):
            w = min(LANES, vl - j * LANES)
            staged[b, :, j * LANES:j * LANES + w] = (z_ref[rows, j * LANES:j * LANES + w] * SCALE) * inv[:, 0:w]
        staged_copy(b).start()
        return c
    lax.fori_loop(0, n, one, 0)

    seq_of = lax.broadcasted_iota(jnp.int32, (n, width), 1) // ROWS == lax.broadcasted_iota(jnp.int32, (n, width), 0)
    pos_of = lax.broadcasted_iota(jnp.int32, (ROWS, width), 1) % ROWS == lax.broadcasted_iota(jnp.int32, (ROWS, width), 0)
    to_seq = (lax.broadcasted_iota(jnp.int32, (width, n), 0) // ROWS
              == lax.broadcasted_iota(jnp.int32, (width, n), 1)).astype(jnp.float32)
    by_seq = jnp.zeros((n, num_draft), jnp.float32)
    by_pos = []
    for g in range(phases):
        a = jnp.minimum(1.0, tot_ref[g, 1:2, :] / tot_ref[g, 2:3, :])
        to_pos = (lax.broadcasted_iota(jnp.int32, (width, num_draft), 0) % ROWS + g * ROWS
                  == lax.broadcasted_iota(jnp.int32, (width, num_draft), 1)).astype(jnp.float32)
        by_seq = by_seq + jnp.dot(jnp.where(seq_of, jnp.broadcast_to(a, (n, width)), 0.0), to_pos,
                                  precision=lax.Precision.HIGHEST, preferred_element_type=jnp.float32)
        by_pos.append(jnp.dot(jnp.where(pos_of, jnp.broadcast_to(a, (ROWS, width)), 0.0), to_seq,
                              precision=lax.Precision.HIGHEST, preferred_element_type=jnp.float32))
    accepted[...] = by_seq
    accept_copy = pltpu.make_async_copy(accepted, accept_ref, small_sem.at[0])
    accept_copy.start()
    product = by_pos[0][0:1, :]
    total = product
    for k in range(1, num_draft):
        product = product * by_pos[k // ROWS][k % ROWS:k % ROWS + 1, :]
        total = total + product
    expected[...] = total
    expected_copy = pltpu.make_async_copy(expected, expected_ref, small_sem.at[1])
    expected_copy.start()

    def finished(b, c):
        for g in range(last):
            ready_copy(g, b).wait()
        staged_copy(b).wait()
        return c
    lax.fori_loop(0, n, finished, 0)
    bonus_copy.wait()
    accept_copy.wait()
    expected_copy.wait()


def solution(mesh):
    n = mesh.shape["tpa"] * mesh.shape["tpb"]

    def local_step(hidden, w_head, q_draft, x_draft):
        seqs, positions, depth = hidden.shape
        vl = w_head.shape[1]
        num_draft = x_draft.shape[1]
        phases = num_draft // ROWS
        vp = pl.cdiv(vl, LANES) * LANES
        rows = seqs * positions
        stat_rows = pl.cdiv(rows, LANES) * LANES
        f32 = jnp.float32
        any_spec = pl.BlockSpec(memory_space=pl.ANY)
        vmem_spec = pl.BlockSpec(memory_space=pltpu.VMEM)
        z, tot = pl.pallas_call(
            functools.partial(exchange_kernel, n, phases, vl),
            name="exchange",
            out_shape=(pltpu.VMEM((rows, vl), f32), pltpu.VMEM((phases, 3, LANES), f32)),
            in_specs=[any_spec] * 4,
            out_specs=(vmem_spec, vmem_spec),
            scratch_shapes=[
                pltpu.VMEM((rows, depth), jnp.bfloat16),
                pltpu.VMEM((rows, depth), jnp.bfloat16),
                pltpu.VMEM((W_BUFS, W_ROWS, depth), jnp.bfloat16),
                pltpu.VMEM((phases, n, ROWS, vp + LANES), f32),
                pltpu.VMEM((phases, n, ROWS, vp), f32),
                pltpu.VMEM((seqs, num_draft), jnp.int32),
                pltpu.VMEM((stat_rows, LANES), f32),
                pltpu.VMEM((stat_rows, LANES), f32),
                pltpu.VMEM((stat_rows, LANES), f32),
                pltpu.VMEM((phases * n * ROWS, LANES), f32),
                pltpu.VMEM((2, 2, stat_rows // LANES, LANES), f32),
                pltpu.VMEM((n // 2, 2, stat_rows // LANES // 2, LANES), f32),
                pltpu.VMEM((2, 2, stat_rows // LANES // 2, LANES), f32),
                pltpu.VMEM((2, 2, 3, LANES), f32),
                pltpu.VMEM((n // 2, 3, LANES), f32),
                pltpu.VMEM((2, 3, LANES), f32),
                pltpu.VMEM((n, 3, LANES), f32),
                pltpu.SemaphoreType.DMA((2,)),
                pltpu.SemaphoreType.DMA((W_BUFS,)),
                pltpu.SemaphoreType.DMA((phases, n)),
                pltpu.SemaphoreType.DMA((phases, n)),
                pltpu.SemaphoreType.DMA((phases, n)),
                pltpu.SemaphoreType.DMA((4,)),
                pltpu.SemaphoreType.DMA((4,)),
                pltpu.SemaphoreType.DMA((2, n // 2)),
                pltpu.SemaphoreType.DMA((2, n // 2)),
                pltpu.SemaphoreType.DMA((n,)),
                pltpu.SemaphoreType.DMA((n,)),
            ],
            compiler_params=pltpu.CompilerParams(collective_id=0, has_side_effects=True, vmem_limit_bytes=48 * 2**20),
        )(hidden.transpose(1, 0, 2).reshape(rows, depth), w_head.T, q_draft.reshape(num_draft, q_draft.shape[2]), x_draft)
        residual, bonus, accept, expected = pl.pallas_call(
            functools.partial(finish_kernel, n, phases, vl),
            name="finish",
            out_shape=(jax.ShapeDtypeStruct((seqs, num_draft, vl), f32), jax.ShapeDtypeStruct((seqs, vl), f32),
                       jax.ShapeDtypeStruct((seqs, num_draft), f32), jax.ShapeDtypeStruct((1, seqs), f32)),
            in_specs=[vmem_spec, vmem_spec],
            out_specs=(any_spec,) * 4,
            scratch_shapes=[pltpu.VMEM((n * ROWS, LANES), f32), pltpu.VMEM((seqs, ROWS, vl), f32),
                            pltpu.VMEM((seqs, num_draft), f32), pltpu.VMEM((1, seqs), f32),
                            pltpu.SemaphoreType.DMA((phases, seqs)), pltpu.SemaphoreType.DMA, pltpu.SemaphoreType.DMA((2,))],
            compiler_params=pltpu.CompilerParams(vmem_limit_bytes=32 * 2**20),
        )(tot, z)
        return accept, expected.reshape(seqs), residual, bonus

    return jax.shard_map(
        local_step, mesh=mesh,
        in_specs=(P("dp", None, None), P(None, VOCAB_AXES), P(("dp",) + VOCAB_AXES, None, None), P("dp", None)),
        out_specs=(P("dp", None), P("dp"), P("dp", None, VOCAB_AXES), P("dp", VOCAB_AXES)),
        check_vma=False)
```

```python
import functools

import jax
import jax.numpy as jnp
from jax import lax
from jax.experimental import pallas as pl
from jax.experimental.pallas import tpu as pltpu
from jax.sharding import PartitionSpec as P

INV_TEMP = 1.25
VOCAB_AXES = ("tpa", "tpb")
MESH = pl.DeviceIdType.MESH
LANES = 128
ROWS = 8
W_ROWS = 256
W_BUFS = 4
PIECES = 4
AHEAD = 4
SCALE = 2.0 ** 64


def xor4(a, r):
    low = lax.rem(lax.rem(a, 2) + lax.rem(r, 2), 2)
    high = lax.rem(lax.div(a, 2) + lax.div(r, 2), 2)
    return low + 2 * high


def exchange_kernel(n, phases, vl, hid_ref, w_ref, q_ref, x_ref, z_ref, tot_ref,
                    hid_v, hs, wbuf, sbuf, qbuf, x_v, colmax, colsum, scale, part, stat_core, stat_chip, stat_half, sum_core, sum_chip, sum_half, zmsg,
                    in_sem, w_sem, ld_sem, qs_sem, qr_sem, swap_s, swap_r, chip_s, chip_r, zs_sem, zr_sem):
    vp = qbuf.shape[3]
    tiles = vp // LANES
    last = vl - (tiles - 1) * LANES
    rows_all = z_ref.shape[0]
    draft_rows = phases * n * ROWS
    my_a, my_b = lax.axis_index("tpa"), lax.axis_index("tpb")
    me = my_a * 4 + my_b
    lane = lax.broadcasted_iota(jnp.int32, (ROWS, LANES), 1)

    def flip(a, r):
        return (a, a + 1 - 2 * lax.rem(a, 2), lax.rem(a + 2, 4), 3 - a)[r]

    def peer(r):
        if isinstance(r, int):
            return flip(my_a, r // 4), flip(my_b, r % 4)
        return xor4(my_a, lax.div(r, 4)), xor4(my_b, lax.rem(r, 4))

    def window(k):
        col = lax.div(k * vl, LANES) * LANES
        return pl.multiple_of(col, LANES), k * vl - col

    def sized(k, body):
        _, o = window(k)
        wide = o + vl > vp
        pl.when(wide)(lambda: body(vp + LANES))
        pl.when(jnp.logical_not(wide))(lambda: body(vp))

    core = lax.rem(my_b, 2)
    inner = lax.rem(lax.div(my_a + 1, 2), 2)

    def nth(g, i):
        r = inner * lax.rem((n // 2 + 1) * (i + core) + n // 2, n) + (1 - inner) * i
        if g == phases - 1:
            far = lax.div(r, n // 2)
            r = (1 - far) * r + far * (n // 2 + lax.rem(r + (1 - inner) * (n // 4), n // 2))
        return r

    def arrival_order(g, i):
        far = lax.div(i, n // 2)
        return i if g < phases - 1 else (1 - far) * i + far * (n // 2 + lax.rem(i + n // 4, n // 2))

    def width_of(g):
        return vp if g < phases - 1 else vp - LANES

    def load(g, k, width):
        col, _ = window(k)
        return pltpu.make_async_copy(q_ref.at[g * ROWS:(g + 1) * ROWS, pl.ds(col, width)], sbuf.at[g, k, :, pl.ds(0, width)], ld_sem.at[g, k])

    def q_copy(g, r, s):
        a, b = peer(r)
        return pltpu.make_async_remote_copy(
            src_ref=sbuf.at[g, a * 4 + b, :, pl.ds(0, width_of(g))], dst_ref=qbuf.at[g, s, :, pl.ds(0, width_of(g))],
            send_sem=qs_sem.at[g, r], recv_sem=qr_sem.at[g, s],
            device_id={"tpa": a, "tpb": b}, device_id_type=MESH)

    def q_piece(g, r, h):
        a, b = peer(r)
        cut = [tiles * i // PIECES * LANES for i in range(PIECES)] + [width_of(g)]
        at = pl.ds(cut[h], cut[h + 1] - cut[h])
        return pltpu.make_async_remote_copy(
            src_ref=sbuf.at[g, a * 4 + b, :, at], dst_ref=qbuf.at[g, me, :, at],
            send_sem=qs_sem.at[g, r], recv_sem=qr_sem.at[g, me],
            device_id={"tpa": a, "tpb": b}, device_id_type=MESH)

    def tile_of(j):
        return slice(j * LANES, (j + 1) * LANES)

    def part_of(j):
        return slice(j * LANES, min((j + 1) * LANES, vl))

    free = LANES - last

    def prepare(g, k):
        _, o = window(k)
        shift = lax.rem(LANES - o, LANES)

        def last_tile(h):
            return jnp.where(lane < LANES - o, pltpu.roll(sbuf[h, k, :, tile_of(tiles - 1)], shift, 1),
                             pltpu.roll(sbuf[h, k, :, tile_of(tiles)], shift, 1))
        ending = last_tile(g)
        if g < phases - 1:
            guest = pltpu.roll(last_tile(phases - 1), last if g == 0 else LANES - (free - last) % LANES, 1)
            ending = jnp.where(lane < last, ending, guest)
        this = pltpu.roll(sbuf[g, k, :, tile_of(0)], shift, 1)
        for j in range(tiles - 1):
            following = pltpu.roll(sbuf[g, k, :, tile_of(j + 1)], shift, 1)
            sbuf[g, k, :, tile_of(j)] = jnp.where(lane < LANES - o, this, following)
            this = following
        sbuf[g, k, :, tile_of(tiles - 1)] = ending

    def ready(g, i):
        if g < phases - 1:
            @pl.when(i + AHEAD < n)
            def _():
                start_load(g, i + AHEAD)
        r = nth(g, i)
        a, b = peer(r)
        k = a * 4 + b
        if g == 0:
            sized(k, lambda width: load(0, k, width).wait())
            sized(k, lambda width: load(phases - 1, k, width).wait())
        elif g < phases - 1:
            sized(k, lambda width: load(g, k, width).wait())
        prepare(g, k)

        @pl.when(r == 0)
        def _():
            for j in range(tiles):
                qbuf[g, me, :, tile_of(j)] = sbuf[g, me, :, tile_of(j)]

    def first(g):
        lax.fori_loop(0, 2, lambda i, c: (ready(g, i), c)[1], 0)

    def send_phase(g):
        for h in range(PIECES):
            def one(i, c, h=h):
                r = nth(g, i)

                @pl.when(r > 0)
                def _():
                    q_piece(g, r, h).start()

                if h == 0:
                    @pl.when(i + 2 < n)
                    def _():
                        ready(g, i + 2)
                return c
            lax.fori_loop(0, n, one, 0)

    def w_copy(c, slot):
        return pltpu.make_async_copy(w_ref.at[pl.ds(pl.multiple_of(c * W_ROWS, W_ROWS), W_ROWS), :], wbuf.at[slot], w_sem.at[slot])

    full_chunks = vl // W_ROWS
    w_tail = vl - full_chunks * W_ROWS
    tail_slot = full_chunks % W_BUFS
    tail_copy = pltpu.make_async_copy(
        w_ref.at[pl.ds(full_chunks * W_ROWS, w_tail), :], wbuf.at[tail_slot, pl.ds(0, w_tail), :], w_sem.at[tail_slot])

    hid_copy = pltpu.make_async_copy(hid_ref, hid_v, in_sem.at[0])
    x_copy = pltpu.make_async_copy(x_ref, x_v, in_sem.at[1])
    barrier = pltpu.get_barrier_semaphore()

    for r in range(n - 1, 0, -1):
        a, b = peer(r)
        pl.semaphore_signal(barrier, inc=1, device_id={"tpa": a, "tpb": b}, device_id_type=MESH)

    def start_load(g, i):
        a, b = peer(nth(g, i))
        k = a * 4 + b
        for h in (0, phases - 1) if g == 0 else (g,):
            sized(k, lambda width, h=h: load(h, k, width).start())

    for i in range(AHEAD):
        start_load(0, i)
    x_copy.start()
    first(0)
    pl.semaphore_wait(barrier, n - 1)

    send_phase(0)
    for g in range(1, phases - 1):
        for i in range(AHEAD):
            start_load(g, i)
    hid_copy.start()
    for c in range(W_BUFS):
        w_copy(c, c).start()
    for g in range(1, phases - 1):
        first(g)
        send_phase(g)

    hid_copy.wait()
    row = lax.broadcasted_iota(jnp.int32, (rows_all, rows_all), 0)
    col = lax.broadcasted_iota(jnp.int32, (rows_all, rows_all), 1)
    source = jnp.where(row < draft_rows, ((row // (n * ROWS)) * ROWS + row % ROWS) * n + (row // ROWS) % n, row)
    permute = jnp.where(col == source, 1.0, 0.0).astype(jnp.bfloat16)
    depth = hid_v.shape[1]

    def permute_columns(c, carry):
        at = pl.ds(pl.multiple_of(c * 256, 256), 256)
        hs[:, at] = jnp.dot(permute, hid_v[:, at], preferred_element_type=jnp.float32).astype(jnp.bfloat16)
        return carry
    lax.fori_loop(0, depth // 256, permute_columns, 0)

    nt = (((1,), (1,)), ((), ()))

    def logits(c, carry):
        slot = lax.rem(c, W_BUFS)
        w_copy(c, slot).wait()
        z_ref[:, pl.ds(pl.multiple_of(c * W_ROWS, W_ROWS), W_ROWS)] = lax.dot_general(
            hs[...], wbuf[slot], nt, preferred_element_type=jnp.float32) * INV_TEMP

        @pl.when(c + W_BUFS < full_chunks)
        def _():
            w_copy(c + W_BUFS, slot).start()

        @pl.when(c + W_BUFS == full_chunks)
        def _():
            tail_copy.start()
        return carry
    lax.fori_loop(0, full_chunks, logits, 0)
    tail_copy.wait()
    z_ref[:, full_chunks * W_ROWS:vl] = lax.dot_general(
        hs[...], wbuf[tail_slot, 0:w_tail, :], nt, preferred_element_type=jnp.float32) * INV_TEMP

    def row_stats(t, carry):
        rows = pl.ds(pl.multiple_of(t * ROWS, ROWS), ROWS)
        ending = z_ref[rows, part_of(tiles - 1)]
        m = z_ref[rows, part_of(0)]
        for j in range(1, tiles - 1):
            m = jnp.maximum(m, z_ref[rows, part_of(j)])
        m = jnp.maximum(jnp.max(m, axis=1, keepdims=True), jnp.max(ending, axis=1, keepdims=True))
        m = jnp.broadcast_to(m, (ROWS, LANES))
        ending = jnp.exp(ending - m[:, 0:last])
        z_ref[rows, part_of(tiles - 1)] = ending
        s = jnp.zeros((ROWS, LANES), jnp.float32)
        for j in range(tiles - 1):
            e = jnp.exp(z_ref[rows, part_of(j)] - m)
            z_ref[rows, part_of(j)] = e
            s = s + e
        s = jnp.sum(s, axis=1, keepdims=True) + jnp.sum(ending, axis=1, keepdims=True)
        colmax[rows, :] = m
        colsum[rows, :] = jnp.broadcast_to(s, (ROWS, LANES))
        return carry
    lax.fori_loop(0, rows_all // ROWS, row_stats, 0)
    chip = my_a * 2 + lax.div(my_b, 2)
    chips = n // 2

    def swap(i, ref):
        return pltpu.make_async_remote_copy(
            src_ref=ref.at[core], dst_ref=ref.at[core], send_sem=swap_s.at[i], recv_sem=swap_r.at[i],
            device_id={"tpa": my_a, "tpb": my_b + 1 - 2 * core}, device_id_type=MESH)

    def swap_arrival(i, ref):
        return pltpu.make_async_remote_copy(
            src_ref=ref.at[1 - core], dst_ref=ref.at[1 - core], send_sem=swap_s.at[i], recv_sem=swap_r.at[i],
            device_id={"tpa": my_a, "tpb": my_b}, device_id_type=MESH)

    def chip_copy(i, ref, h, slot):
        a, b = peer(2 * h)
        return pltpu.make_async_remote_copy(
            src_ref=ref.at[chip], dst_ref=ref.at[slot], send_sem=chip_s.at[i, h], recv_sem=chip_r.at[i, slot],
            device_id={"tpa": a, "tpb": b}, device_id_type=MESH)

    def chip_send(i, ref):
        for h in range(chips - 1, 0, -1):
            chip_copy(i, ref, h, chip).start()

    def chip_arrivals(i, ref):
        for h in range(1, chips):
            a, b = peer(2 * h)
            chip_copy(i, ref, h, a * 2 + lax.div(b, 2)).wait_recv()

    def combine(pairs):
        top = pairs[0][0]
        for m, _ in pairs[1:]:
            top = jnp.maximum(top, m)
        total = jnp.zeros_like(top)
        for m, s in pairs:
            total = total + s * jnp.exp(m - top)
        return top, total

    spare = colmax.shape[0] - rows_all
    colmax[rows_all:, :] = jnp.zeros((spare, LANES), jnp.float32)
    colsum[rows_all:, :] = jnp.ones((spare, LANES), jnp.float32)

    blocks = colmax.shape[0] // LANES

    def as_rows(ref):
        return jnp.concatenate([ref[i * LANES:(i + 1) * LANES, :].T[0:1, :] for i in range(blocks)], axis=0)
    my_max = as_rows(colmax)
    stat_core[core, 0] = my_max
    stat_core[core, 1] = as_rows(colsum)
    swap(0, stat_core).start()
    swap_arrival(0, stat_core).wait_recv()
    top, total = combine([(stat_core[c, 0], stat_core[c, 1]) for c in range(2)])
    half = blocks // 2
    mine = core == 0
    stat_chip[chip, 0] = jnp.where(mine, top[0:half], top[half:])
    stat_chip[chip, 1] = jnp.where(mine, total[0:half], total[half:])
    chip_send(0, stat_chip)
    first(phases - 1)
    send_phase(phases - 1)

    chip_arrivals(0, stat_chip)
    top, total = combine([(stat_chip[c, 0], stat_chip[c, 1]) for c in range(chips)])
    stat_half[core, 0] = top
    stat_half[core, 1] = total
    swap(1, stat_half).start()
    swap_arrival(1, stat_half).wait_recv()
    top = jnp.concatenate([stat_half[0, 0], stat_half[1, 0]], axis=0)
    total = jnp.concatenate([stat_half[0, 1], stat_half[1, 1]], axis=0)
    factor = jnp.exp(stat_core[core, 0] - top) / total
    for i in range(blocks):
        scale[i * LANES:(i + 1) * LANES, :] = jnp.broadcast_to(factor[i:i + 1, :], (LANES, LANES)).T

    for t in range(draft_rows // ROWS, rows_all // ROWS):
        rows = slice(t * ROWS, (t + 1) * ROWS)
        for j in range(tiles):
            value = z_ref[rows, part_of(j)]
            z_ref[rows, part_of(j)] = value * scale[rows, 0:value.shape[1]]

    x_copy.wait()
    lane_f = lane.astype(jnp.float32)
    num_draft = x_v.shape[1]

    def excess(g, s):
        rows = pl.ds(pl.multiple_of(g * (n * ROWS) + s * ROWS, ROWS), ROWS)
        tokens = jnp.broadcast_to(x_v[pl.ds(s, 1), :].astype(jnp.float32), (ROWS, num_draft))
        position = lax.broadcasted_iota(jnp.int32, (ROWS, num_draft), 0) + g * ROWS
        here = lax.broadcasted_iota(jnp.int32, (ROWS, num_draft), 1) == position
        token = jnp.sum(jnp.where(here, tokens, 0.0), axis=1, keepdims=True) - (me * vl).astype(jnp.float32)
        token = jnp.broadcast_to(jnp.where(token < vl, token, -1.0), (ROWS, LANES))
        sc = scale[rows, :]
        z_sum = p_pick = q_pick = jnp.zeros((ROWS, LANES), jnp.float32)
        for j in range(tiles - 1):
            q = qbuf[g, s, :, tile_of(j)]
            p = z_ref[rows, part_of(j)] * sc
            d = jnp.maximum(p - q, 0.0)
            z_ref[rows, part_of(j)] = d
            z_sum = z_sum + d
            hit = lane_f == token - float(j * LANES)
            p_pick = jnp.where(hit, p, p_pick)
            q_pick = jnp.where(hit, q, q_pick)
        j = tiles - 1
        if g < phases - 1:
            q = qbuf[g, s, :, tile_of(j)]
        else:
            q = jnp.where(lane < free, pltpu.roll(qbuf[0, s, :, tile_of(j)], free, 1),
                          pltpu.roll(qbuf[1, s, :, tile_of(j)], (free - last) % LANES, 1))
        q = q[:, 0:last]
        p = z_ref[rows, part_of(j)] * sc[:, 0:last]
        d = jnp.maximum(p - q, 0.0)
        z_ref[rows, part_of(j)] = d
        hit = (lane_f == token - float(j * LANES))[:, 0:last]
        sums = [jnp.sum(whole, axis=1, keepdims=True) + jnp.sum(ending, axis=1, keepdims=True)
                for whole, ending in ((z_sum, d), (p_pick, jnp.where(hit, p, 0.0)), (q_pick, jnp.where(hit, q, 0.0)))]
        part[rows, :] = jnp.where(lane == 0, sums[0], jnp.where(lane == 1, sums[1], sums[2]))

    def z_copy(r, s):
        a, b = peer(r)
        return pltpu.make_async_remote_copy(
            src_ref=zmsg.at[me], dst_ref=zmsg.at[s], send_sem=zs_sem.at[r], recv_sem=zr_sem.at[s],
            device_id={"tpa": a, "tpb": b}, device_id_type=MESH)

    def row_sums(g):
        block = slice(g * n * ROWS, (g + 1) * n * ROWS)
        return part[block, :].T[0:3, :]

    for g in range(phases):
        def one(i, c, g=g):
            r = arrival_order(g, i)
            a, b = peer(r)
            s = a * 4 + b

            @pl.when(r > 0)
            def _():
                q_copy(g, r, s).wait_recv()
            excess(g, s)
            return c
        lax.fori_loop(0, n, one, 0)
        if g == phases - 2:
            for h in range(2):
                sum_core[core, h] = row_sums(h)
            swap(2, sum_core).start()
            swap_arrival(2, sum_core).wait_recv()
            sum_chip[chip] = jnp.where(mine, sum_core[0, 0] + sum_core[1, 0], sum_core[0, 1] + sum_core[1, 1])
            chip_send(1, sum_chip)
    zmsg[me] = row_sums(phases - 1)
    for r in range(n - 1, 0, -1):
        z_copy(r, me).start()

    def drain(r, c):
        for g in range(phases):
            q_copy(g, r, me).wait_send()
        z_copy(r, me).wait_send()
        return c

    def divide(g):
        inverse = jnp.broadcast_to(1.0 / (tot_ref[g, 0:1, :] * SCALE), (n * ROWS, LANES)).T
        scale[0:n * ROWS, :] = inverse

        def one(s, c):
            rows = pl.ds(pl.multiple_of(g * (n * ROWS) + s * ROWS, ROWS), ROWS)
            inv = scale[pl.ds(pl.multiple_of(s * ROWS, ROWS), ROWS), :]
            for j in range(tiles):
                value = z_ref[rows, part_of(j)] * SCALE
                z_ref[rows, part_of(j)] = value * inv[:, 0:value.shape[1]]
            return c
        lax.fori_loop(0, n, one, 0)

    chip_arrivals(1, sum_chip)
    total = sum_chip[0]
    for c in range(1, chips):
        total = total + sum_chip[c]
    sum_half[core] = total
    swap(3, sum_half).start()
    swap_arrival(3, sum_half).wait_recv()
    for g in range(phases - 1):
        tot_ref[g] = sum_half[g]
        divide(g)
    lax.fori_loop(1, n, drain, 0)
    for i, ref in enumerate((stat_core, stat_half, sum_core, sum_half)):
        swap(i, ref).wait_send()
    for i, ref in enumerate((stat_chip, sum_chip)):
        for h in range(1, chips):
            chip_copy(i, ref, h, chip).wait_send()
    for r in range(1, n):
        a, b = peer(r)
        z_copy(r, a * 4 + b).wait_recv()
    total = zmsg[0]
    for s in range(1, n):
        total = total + zmsg[s]
    tot_ref[phases - 1] = total


def finish_kernel(n, phases, vl, tot_ref, z_ref, res_ref, bonus_ref, accept_ref, expected_ref, inverse, staged, accepted, expected, sem, bonus_sem, small_sem):
    width = n * ROWS
    num_draft = phases * ROWS
    last = phases - 1

    def ready_copy(g, b):
        return pltpu.make_async_copy(z_ref.at[pl.ds(pl.multiple_of(g * width + b * ROWS, ROWS), ROWS), :],
                                     res_ref.at[b, g * ROWS:(g + 1) * ROWS, :], sem.at[g, b])

    def staged_copy(b):
        return pltpu.make_async_copy(staged.at[b], res_ref.at[b, last * ROWS:, :], sem.at[last, b])

    bonus_copy = pltpu.make_async_copy(z_ref.at[phases * width:phases * width + n, :], bonus_ref, bonus_sem)

    def start(b, c):
        for g in range(last):
            ready_copy(g, b).start(priority=g % 2)
        return c
    lax.fori_loop(0, n, start, 0)
    bonus_copy.start()
    inverse[...] = jnp.broadcast_to(1.0 / (tot_ref[last, 0:1, :] * SCALE), (width, LANES)).T

    def one(b, c):
        inv = inverse[pl.ds(pl.multiple_of(b * ROWS, ROWS), ROWS), :]
        rows = pl.ds(pl.multiple_of(last * width + b * ROWS, ROWS), ROWS)
        for j in range(pl.cdiv(vl, LANES)):
            w = min(LANES, vl - j * LANES)
            staged[b, :, j * LANES:j * LANES + w] = (z_ref[rows, j * LANES:j * LANES + w] * SCALE) * inv[:, 0:w]
        staged_copy(b).start()
        return c
    lax.fori_loop(0, n, one, 0)

    seq_of = lax.broadcasted_iota(jnp.int32, (n, width), 1) // ROWS == lax.broadcasted_iota(jnp.int32, (n, width), 0)
    pos_of = lax.broadcasted_iota(jnp.int32, (ROWS, width), 1) % ROWS == lax.broadcasted_iota(jnp.int32, (ROWS, width), 0)
    to_seq = (lax.broadcasted_iota(jnp.int32, (width, n), 0) // ROWS
              == lax.broadcasted_iota(jnp.int32, (width, n), 1)).astype(jnp.float32)
    by_seq = jnp.zeros((n, num_draft), jnp.float32)
    by_pos = []
    for g in range(phases):
        a = jnp.minimum(1.0, tot_ref[g, 1:2, :] / tot_ref[g, 2:3, :])
        to_pos = (lax.broadcasted_iota(jnp.int32, (width, num_draft), 0) % ROWS + g * ROWS
                  == lax.broadcasted_iota(jnp.int32, (width, num_draft), 1)).astype(jnp.float32)
        by_seq = by_seq + jnp.dot(jnp.where(seq_of, jnp.broadcast_to(a, (n, width)), 0.0), to_pos,
                                  precision=lax.Precision.HIGHEST, preferred_element_type=jnp.float32)
        by_pos.append(jnp.dot(jnp.where(pos_of, jnp.broadcast_to(a, (ROWS, width)), 0.0), to_seq,
                              precision=lax.Precision.HIGHEST, preferred_element_type=jnp.float32))
    accepted[...] = by_seq
    accept_copy = pltpu.make_async_copy(accepted, accept_ref, small_sem.at[0])
    accept_copy.start()
    product = by_pos[0][0:1, :]
    total = product
    for k in range(1, num_draft):
        product = product * by_pos[k // ROWS][k % ROWS:k % ROWS + 1, :]
        total = total + product
    expected[...] = total
    expected_copy = pltpu.make_async_copy(expected, expected_ref, small_sem.at[1])
    expected_copy.start()

    def finished(b, c):
        for g in range(last):
            ready_copy(g, b).wait()
        staged_copy(b).wait()
        return c
    lax.fori_loop(0, n, finished, 0)
    bonus_copy.wait()
    accept_copy.wait()
    expected_copy.wait()


def solution(mesh):
    n = mesh.shape["tpa"] * mesh.shape["tpb"]

    def local_step(hidden, w_head, q_draft, x_draft):
        seqs, positions, depth = hidden.shape
        vl = w_head.shape[1]
        num_draft = x_draft.shape[1]
        phases = num_draft // ROWS
        vp = pl.cdiv(vl, LANES) * LANES
        rows = seqs * positions
        stat_rows = pl.cdiv(rows, LANES) * LANES
        f32 = jnp.float32
        any_spec = pl.BlockSpec(memory_space=pl.ANY)
        vmem_spec = pl.BlockSpec(memory_space=pltpu.VMEM)
        z, tot = pl.pallas_call(
            functools.partial(exchange_kernel, n, phases, vl),
            name="exchange",
            out_shape=(pltpu.VMEM((rows, vl), f32), pltpu.VMEM((phases, 3, LANES), f32)),
            in_specs=[any_spec] * 4,
            out_specs=(vmem_spec, vmem_spec),
            scratch_shapes=[
                pltpu.VMEM((rows, depth), jnp.bfloat16),
                pltpu.VMEM((rows, depth), jnp.bfloat16),
                pltpu.VMEM((W_BUFS, W_ROWS, depth), jnp.bfloat16),
                pltpu.VMEM((phases, n, ROWS, vp + LANES), f32),
                pltpu.VMEM((phases, n, ROWS, vp), f32),
                pltpu.VMEM((seqs, num_draft), jnp.int32),
                pltpu.VMEM((stat_rows, LANES), f32),
                pltpu.VMEM((stat_rows, LANES), f32),
                pltpu.VMEM((stat_rows, LANES), f32),
                pltpu.VMEM((phases * n * ROWS, LANES), f32),
                pltpu.VMEM((2, 2, stat_rows // LANES, LANES), f32),
                pltpu.VMEM((n // 2, 2, stat_rows // LANES // 2, LANES), f32),
                pltpu.VMEM((2, 2, stat_rows // LANES // 2, LANES), f32),
                pltpu.VMEM((2, 2, 3, LANES), f32),
                pltpu.VMEM((n // 2, 3, LANES), f32),
                pltpu.VMEM((2, 3, LANES), f32),
                pltpu.VMEM((n, 3, LANES), f32),
                pltpu.SemaphoreType.DMA((2,)),
                pltpu.SemaphoreType.DMA((W_BUFS,)),
                pltpu.SemaphoreType.DMA((phases, n)),
                pltpu.SemaphoreType.DMA((phases, n)),
                pltpu.SemaphoreType.DMA((phases, n)),
                pltpu.SemaphoreType.DMA((4,)),
                pltpu.SemaphoreType.DMA((4,)),
                pltpu.SemaphoreType.DMA((2, n // 2)),
                pltpu.SemaphoreType.DMA((2, n // 2)),
                pltpu.SemaphoreType.DMA((n,)),
                pltpu.SemaphoreType.DMA((n,)),
            ],
            compiler_params=pltpu.CompilerParams(collective_id=0, has_side_effects=True, vmem_limit_bytes=48 * 2**20),
        )(hidden.transpose(1, 0, 2).reshape(rows, depth), w_head.T, q_draft.reshape(num_draft, q_draft.shape[2]), x_draft)
        residual, bonus, accept, expected = pl.pallas_call(
            functools.partial(finish_kernel, n, phases, vl),
            name="finish",
            out_shape=(jax.ShapeDtypeStruct((seqs, num_draft, vl), f32), jax.ShapeDtypeStruct((seqs, vl), f32),
                       jax.ShapeDtypeStruct((seqs, num_draft), f32), jax.ShapeDtypeStruct((1, seqs), f32)),
            in_specs=[vmem_spec, vmem_spec],
            out_specs=(any_spec,) * 4,
            scratch_shapes=[pltpu.VMEM((n * ROWS, LANES), f32), pltpu.VMEM((seqs, ROWS, vl), f32),
                            pltpu.VMEM((seqs, num_draft), f32), pltpu.VMEM((1, seqs), f32),
                            pltpu.SemaphoreType.DMA((phases, seqs)), pltpu.SemaphoreType.DMA, pltpu.SemaphoreType.DMA((2,))],
            compiler_params=pltpu.CompilerParams(vmem_limit_bytes=32 * 2**20),
        )(tot, z)
        return accept, expected.reshape(seqs), residual, bonus

    return jax.shard_map(
        local_step, mesh=mesh,
        in_specs=(P("dp", None, None), P(None, VOCAB_AXES), P(("dp",) + VOCAB_AXES, None, None), P("dp", None)),
        out_specs=(P("dp", None), P("dp"), P("dp", None, VOCAB_AXES), P("dp", VOCAB_AXES)),
        check_vma=False)
```

```python
import functools

import jax
import jax.numpy as jnp
from jax import lax
from jax.experimental import pallas as pl
from jax.experimental.pallas import tpu as pltpu
from jax.sharding import PartitionSpec as P

INV_TEMP = 1.25
VOCAB_AXES = ("tpa", "tpb")
MESH = pl.DeviceIdType.MESH
LANES = 128
ROWS = 8
W_ROWS = 256
W_BUFS = 4
PIECES = 8
AHEAD = 4
SCALE = 2.0 ** 64


def xor4(a, r):
    low = lax.rem(lax.rem(a, 2) + lax.rem(r, 2), 2)
    high = lax.rem(lax.div(a, 2) + lax.div(r, 2), 2)
    return low + 2 * high


def exchange_kernel(n, phases, vl, hid_ref, w_ref, q_ref, x_ref, z_ref, tot_ref,
                    hid_v, hs, wbuf, sbuf, qbuf, x_v, colmax, colsum, scale, part, stat_core, stat_chip, stat_half, sum_core, sum_chip, sum_half, zmsg,
                    in_sem, w_sem, ld_sem, qs_sem, qr_sem, swap_s, swap_r, chip_s, chip_r, zs_sem, zr_sem):
    vp = qbuf.shape[3]
    tiles = vp // LANES
    last = vl - (tiles - 1) * LANES
    rows_all = z_ref.shape[0]
    draft_rows = phases * n * ROWS
    my_a, my_b = lax.axis_index("tpa"), lax.axis_index("tpb")
    me = my_a * 4 + my_b
    lane = lax.broadcasted_iota(jnp.int32, (ROWS, LANES), 1)

    def flip(a, r):
        return (a, a + 1 - 2 * lax.rem(a, 2), lax.rem(a + 2, 4), 3 - a)[r]

    def peer(r):
        if isinstance(r, int):
            return flip(my_a, r // 4), flip(my_b, r % 4)
        return xor4(my_a, lax.div(r, 4)), xor4(my_b, lax.rem(r, 4))

    def window(k):
        col = lax.div(k * vl, LANES) * LANES
        return pl.multiple_of(col, LANES), k * vl - col

    def sized(k, body):
        _, o = window(k)
        wide = o + vl > vp
        pl.when(wide)(lambda: body(vp + LANES))
        pl.when(jnp.logical_not(wide))(lambda: body(vp))

    core = lax.rem(my_b, 2)
    inner = lax.rem(lax.div(my_a + 1, 2), 2)

    def nth(g, i):
        r = inner * lax.rem((n // 2 + 1) * (i + core) + n // 2, n) + (1 - inner) * i
        if g == phases - 1:
            far = lax.div(r, n // 2)
            r = (1 - far) * r + far * (n // 2 + lax.rem(r + (1 - inner) * (n // 4), n // 2))
        return r

    def arrival_order(g, i):
        far = lax.div(i, n // 2)
        return i if g < phases - 1 else (1 - far) * i + far * (n // 2 + lax.rem(i + n // 4, n // 2))

    def width_of(g):
        return vp if g < phases - 1 else vp - LANES

    def load(g, k, width):
        col, _ = window(k)
        return pltpu.make_async_copy(q_ref.at[g * ROWS:(g + 1) * ROWS, pl.ds(col, width)], sbuf.at[g, k, :, pl.ds(0, width)], ld_sem.at[g, k])

    def q_copy(g, r, s):
        a, b = peer(r)
        return pltpu.make_async_remote_copy(
            src_ref=sbuf.at[g, a * 4 + b, :, pl.ds(0, width_of(g))], dst_ref=qbuf.at[g, s, :, pl.ds(0, width_of(g))],
            send_sem=qs_sem.at[g, r], recv_sem=qr_sem.at[g, s],
            device_id={"tpa": a, "tpb": b}, device_id_type=MESH)

    def q_piece(g, r, h):
        a, b = peer(r)
        cut = [tiles * i // PIECES * LANES for i in range(PIECES)] + [width_of(g)]
        at = pl.ds(cut[h], cut[h + 1] - cut[h])
        return pltpu.make_async_remote_copy(
            src_ref=sbuf.at[g, a * 4 + b, :, at], dst_ref=qbuf.at[g, me, :, at],
            send_sem=qs_sem.at[g, r], recv_sem=qr_sem.at[g, me],
            device_id={"tpa": a, "tpb": b}, device_id_type=MESH)

    def tile_of(j):
        return slice(j * LANES, (j + 1) * LANES)

    def part_of(j):
        return slice(j * LANES, min((j + 1) * LANES, vl))

    free = LANES - last

    def prepare(g, k):
        _, o = window(k)
        shift = lax.rem(LANES - o, LANES)

        def last_tile(h):
            return jnp.where(lane < LANES - o, pltpu.roll(sbuf[h, k, :, tile_of(tiles - 1)], shift, 1),
                             pltpu.roll(sbuf[h, k, :, tile_of(tiles)], shift, 1))
        ending = last_tile(g)
        if g < phases - 1:
            guest = pltpu.roll(last_tile(phases - 1), last if g == 0 else LANES - (free - last) % LANES, 1)
            ending = jnp.where(lane < last, ending, guest)
        this = pltpu.roll(sbuf[g, k, :, tile_of(0)], shift, 1)
        for j in range(tiles - 1):
            following = pltpu.roll(sbuf[g, k, :, tile_of(j + 1)], shift, 1)
            sbuf[g, k, :, tile_of(j)] = jnp.where(lane < LANES - o, this, following)
            this = following
        sbuf[g, k, :, tile_of(tiles - 1)] = ending

    def ready(g, i):
        if g < phases - 1:
            @pl.when(i + AHEAD < n)
            def _():
                start_load(g, i + AHEAD)
        r = nth(g, i)
        a, b = peer(r)
        k = a * 4 + b
        if g == 0:
            sized(k, lambda width: load(0, k, width).wait())
            sized(k, lambda width: load(phases - 1, k, width).wait())
        elif g < phases - 1:
            sized(k, lambda width: load(g, k, width).wait())
        prepare(g, k)

        @pl.when(r == 0)
        def _():
            for j in range(tiles):
                qbuf[g, me, :, tile_of(j)] = sbuf[g, me, :, tile_of(j)]

    def first(g):
        lax.fori_loop(0, 2, lambda i, c: (ready(g, i), c)[1], 0)

    def send_phase(g):
        for h in range(PIECES):
            def one(i, c, h=h):
                r = nth(g, i)

                @pl.when(r > 0)
                def _():
                    q_piece(g, r, h).start()

                if h == 0:
                    @pl.when(i + 2 < n)
                    def _():
                        ready(g, i + 2)
                return c
            lax.fori_loop(0, n, one, 0)

    def w_copy(c, slot):
        return pltpu.make_async_copy(w_ref.at[pl.ds(pl.multiple_of(c * W_ROWS, W_ROWS), W_ROWS), :], wbuf.at[slot], w_sem.at[slot])

    full_chunks = vl // W_ROWS
    w_tail = vl - full_chunks * W_ROWS
    tail_slot = full_chunks % W_BUFS
    tail_copy = pltpu.make_async_copy(
        w_ref.at[pl.ds(full_chunks * W_ROWS, w_tail), :], wbuf.at[tail_slot, pl.ds(0, w_tail), :], w_sem.at[tail_slot])

    hid_copy = pltpu.make_async_copy(hid_ref, hid_v, in_sem.at[0])
    x_copy = pltpu.make_async_copy(x_ref, x_v, in_sem.at[1])
    barrier = pltpu.get_barrier_semaphore()

    for r in range(n - 1, 0, -1):
        a, b = peer(r)
        pl.semaphore_signal(barrier, inc=1, device_id={"tpa": a, "tpb": b}, device_id_type=MESH)

    def start_load(g, i):
        a, b = peer(nth(g, i))
        k = a * 4 + b
        for h in (0, phases - 1) if g == 0 else (g,):
            sized(k, lambda width, h=h: load(h, k, width).start())

    for i in range(AHEAD):
        start_load(0, i)
    x_copy.start()
    first(0)
    pl.semaphore_wait(barrier, n - 1)

    send_phase(0)
    for g in range(1, phases - 1):
        for i in range(AHEAD):
            start_load(g, i)
    hid_copy.start()
    for c in range(W_BUFS):
        w_copy(c, c).start()
    for g in range(1, phases - 1):
        first(g)
        send_phase(g)

    hid_copy.wait()
    row = lax.broadcasted_iota(jnp.int32, (rows_all, rows_all), 0)
    col = lax.broadcasted_iota(jnp.int32, (rows_all, rows_all), 1)
    source = jnp.where(row < draft_rows, ((row // (n * ROWS)) * ROWS + row % ROWS) * n + (row // ROWS) % n, row)
    permute = jnp.where(col == source, 1.0, 0.0).astype(jnp.bfloat16)
    depth = hid_v.shape[1]

    def permute_columns(c, carry):
        at = pl.ds(pl.multiple_of(c * 256, 256), 256)
        hs[:, at] = jnp.dot(permute, hid_v[:, at], preferred_element_type=jnp.float32).astype(jnp.bfloat16)
        return carry
    lax.fori_loop(0, depth // 256, permute_columns, 0)

    nt = (((1,), (1,)), ((), ()))

    def logits(c, carry):
        slot = lax.rem(c, W_BUFS)
        w_copy(c, slot).wait()
        z_ref[:, pl.ds(pl.multiple_of(c * W_ROWS, W_ROWS), W_ROWS)] = lax.dot_general(
            hs[...], wbuf[slot], nt, preferred_element_type=jnp.float32) * INV_TEMP

        @pl.when(c + W_BUFS < full_chunks)
        def _():
            w_copy(c + W_BUFS, slot).start()

        @pl.when(c + W_BUFS == full_chunks)
        def _():
            tail_copy.start()
        return carry
    lax.fori_loop(0, full_chunks, logits, 0)
    tail_copy.wait()
    z_ref[:, full_chunks * W_ROWS:vl] = lax.dot_general(
        hs[...], wbuf[tail_slot, 0:w_tail, :], nt, preferred_element_type=jnp.float32) * INV_TEMP

    def row_stats(t, carry):
        rows = pl.ds(pl.multiple_of(t * ROWS, ROWS), ROWS)
        ending = z_ref[rows, part_of(tiles - 1)]
        m = z_ref[rows, part_of(0)]
        for j in range(1, tiles - 1):
            m = jnp.maximum(m, z_ref[rows, part_of(j)])
        m = jnp.maximum(jnp.max(m, axis=1, keepdims=True), jnp.max(ending, axis=1, keepdims=True))
        m = jnp.broadcast_to(m, (ROWS, LANES))
        ending = jnp.exp(ending - m[:, 0:last])
        z_ref[rows, part_of(tiles - 1)] = ending
        s = jnp.zeros((ROWS, LANES), jnp.float32)
        for j in range(tiles - 1):
            e = jnp.exp(z_ref[rows, part_of(j)] - m)
            z_ref[rows, part_of(j)] = e
            s = s + e
        s = jnp.sum(s, axis=1, keepdims=True) + jnp.sum(ending, axis=1, keepdims=True)
        colmax[rows, :] = m
        colsum[rows, :] = jnp.broadcast_to(s, (ROWS, LANES))
        return carry
    lax.fori_loop(0, rows_all // ROWS, row_stats, 0)
    chip = my_a * 2 + lax.div(my_b, 2)
    chips = n // 2

    def swap(i, ref):
        return pltpu.make_async_remote_copy(
            src_ref=ref.at[core], dst_ref=ref.at[core], send_sem=swap_s.at[i], recv_sem=swap_r.at[i],
            device_id={"tpa": my_a, "tpb": my_b + 1 - 2 * core}, device_id_type=MESH)

    def swap_arrival(i, ref):
        return pltpu.make_async_remote_copy(
            src_ref=ref.at[1 - core], dst_ref=ref.at[1 - core], send_sem=swap_s.at[i], recv_sem=swap_r.at[i],
            device_id={"tpa": my_a, "tpb": my_b}, device_id_type=MESH)

    def chip_copy(i, ref, h, slot):
        a, b = peer(2 * h)
        return pltpu.make_async_remote_copy(
            src_ref=ref.at[chip], dst_ref=ref.at[slot], send_sem=chip_s.at[i, h], recv_sem=chip_r.at[i, slot],
            device_id={"tpa": a, "tpb": b}, device_id_type=MESH)

    def chip_send(i, ref):
        for h in range(chips - 1, 0, -1):
            chip_copy(i, ref, h, chip).start()

    def chip_arrivals(i, ref):
        for h in range(1, chips):
            a, b = peer(2 * h)
            chip_copy(i, ref, h, a * 2 + lax.div(b, 2)).wait_recv()

    def combine(pairs):
        top = pairs[0][0]
        for m, _ in pairs[1:]:
            top = jnp.maximum(top, m)
        total = jnp.zeros_like(top)
        for m, s in pairs:
            total = total + s * jnp.exp(m - top)
        return top, total

    spare = colmax.shape[0] - rows_all
    colmax[rows_all:, :] = jnp.zeros((spare, LANES), jnp.float32)
    colsum[rows_all:, :] = jnp.ones((spare, LANES), jnp.float32)

    blocks = colmax.shape[0] // LANES

    def as_rows(ref):
        return jnp.concatenate([ref[i * LANES:(i + 1) * LANES, :].T[0:1, :] for i in range(blocks)], axis=0)
    my_max = as_rows(colmax)
    stat_core[core, 0] = my_max
    stat_core[core, 1] = as_rows(colsum)
    swap(0, stat_core).start()
    swap_arrival(0, stat_core).wait_recv()
    top, total = combine([(stat_core[c, 0], stat_core[c, 1]) for c in range(2)])
    half = blocks // 2
    mine = core == 0
    stat_chip[chip, 0] = jnp.where(mine, top[0:half], top[half:])
    stat_chip[chip, 1] = jnp.where(mine, total[0:half], total[half:])
    chip_send(0, stat_chip)
    first(phases - 1)
    send_phase(phases - 1)

    chip_arrivals(0, stat_chip)
    top, total = combine([(stat_chip[c, 0], stat_chip[c, 1]) for c in range(chips)])
    stat_half[core, 0] = top
    stat_half[core, 1] = total
    swap(1, stat_half).start()
    swap_arrival(1, stat_half).wait_recv()
    top = jnp.concatenate([stat_half[0, 0], stat_half[1, 0]], axis=0)
    total = jnp.concatenate([stat_half[0, 1], stat_half[1, 1]], axis=0)
    factor = jnp.exp(stat_core[core, 0] - top) / total
    for i in range(blocks):
        scale[i * LANES:(i + 1) * LANES, :] = jnp.broadcast_to(factor[i:i + 1, :], (LANES, LANES)).T

    for t in range(draft_rows // ROWS, rows_all // ROWS):
        rows = slice(t * ROWS, (t + 1) * ROWS)
        for j in range(tiles):
            value = z_ref[rows, part_of(j)]
            z_ref[rows, part_of(j)] = value * scale[rows, 0:value.shape[1]]

    x_copy.wait()
    lane_f = lane.astype(jnp.float32)
    num_draft = x_v.shape[1]

    def excess(g, s):
        rows = pl.ds(pl.multiple_of(g * (n * ROWS) + s * ROWS, ROWS), ROWS)
        tokens = jnp.broadcast_to(x_v[pl.ds(s, 1), :].astype(jnp.float32), (ROWS, num_draft))
        position = lax.broadcasted_iota(jnp.int32, (ROWS, num_draft), 0) + g * ROWS
        here = lax.broadcasted_iota(jnp.int32, (ROWS, num_draft), 1) == position
        token = jnp.sum(jnp.where(here, tokens, 0.0), axis=1, keepdims=True) - (me * vl).astype(jnp.float32)
        token = jnp.broadcast_to(jnp.where(token < vl, token, -1.0), (ROWS, LANES))
        sc = scale[rows, :]
        z_sum = p_pick = q_pick = jnp.zeros((ROWS, LANES), jnp.float32)
        for j in range(tiles - 1):
            q = qbuf[g, s, :, tile_of(j)]
            p = z_ref[rows, part_of(j)] * sc
            d = jnp.maximum(p - q, 0.0)
            z_ref[rows, part_of(j)] = d
            z_sum = z_sum + d
            hit = lane_f == token - float(j * LANES)
            p_pick = jnp.where(hit, p, p_pick)
            q_pick = jnp.where(hit, q, q_pick)
        j = tiles - 1
        if g < phases - 1:
            q = qbuf[g, s, :, tile_of(j)]
        else:
            q = jnp.where(lane < free, pltpu.roll(qbuf[0, s, :, tile_of(j)], free, 1),
                          pltpu.roll(qbuf[1, s, :, tile_of(j)], (free - last) % LANES, 1))
        q = q[:, 0:last]
        p = z_ref[rows, part_of(j)] * sc[:, 0:last]
        d = jnp.maximum(p - q, 0.0)
        z_ref[rows, part_of(j)] = d
        hit = (lane_f == token - float(j * LANES))[:, 0:last]
        sums = [jnp.sum(whole, axis=1, keepdims=True) + jnp.sum(ending, axis=1, keepdims=True)
                for whole, ending in ((z_sum, d), (p_pick, jnp.where(hit, p, 0.0)), (q_pick, jnp.where(hit, q, 0.0)))]
        part[rows, :] = jnp.where(lane == 0, sums[0], jnp.where(lane == 1, sums[1], sums[2]))

    def z_copy(r, s):
        a, b = peer(r)
        return pltpu.make_async_remote_copy(
            src_ref=zmsg.at[me], dst_ref=zmsg.at[s], send_sem=zs_sem.at[r], recv_sem=zr_sem.at[s],
            device_id={"tpa": a, "tpb": b}, device_id_type=MESH)

    def row_sums(g):
        block = slice(g * n * ROWS, (g + 1) * n * ROWS)
        return part[block, :].T[0:3, :]

    for g in range(phases):
        def one(i, c, g=g):
            r = arrival_order(g, i)
            a, b = peer(r)
            s = a * 4 + b

            @pl.when(r > 0)
            def _():
                q_copy(g, r, s).wait_recv()
            excess(g, s)
            return c
        lax.fori_loop(0, n, one, 0)
        if g == phases - 2:
            for h in range(2):
                sum_core[core, h] = row_sums(h)
            swap(2, sum_core).start()
            swap_arrival(2, sum_core).wait_recv()
            sum_chip[chip] = jnp.where(mine, sum_core[0, 0] + sum_core[1, 0], sum_core[0, 1] + sum_core[1, 1])
            chip_send(1, sum_chip)
    zmsg[me] = row_sums(phases - 1)
    for r in range(n - 1, 0, -1):
        z_copy(r, me).start()

    def drain(r, c):
        for g in range(phases):
            q_copy(g, r, me).wait_send()
        z_copy(r, me).wait_send()
        return c

    def divide(g):
        inverse = jnp.broadcast_to(1.0 / (tot_ref[g, 0:1, :] * SCALE), (n * ROWS, LANES)).T
        scale[0:n * ROWS, :] = inverse

        def one(s, c):
            rows = pl.ds(pl.multiple_of(g * (n * ROWS) + s * ROWS, ROWS), ROWS)
            inv = scale[pl.ds(pl.multiple_of(s * ROWS, ROWS), ROWS), :]
            for j in range(tiles):
                value = z_ref[rows, part_of(j)] * SCALE
                z_ref[rows, part_of(j)] = value * inv[:, 0:value.shape[1]]
            return c
        lax.fori_loop(0, n, one, 0)

    chip_arrivals(1, sum_chip)
    total = sum_chip[0]
    for c in range(1, chips):
        total = total + sum_chip[c]
    sum_half[core] = total
    swap(3, sum_half).start()
    swap_arrival(3, sum_half).wait_recv()
    for g in range(phases - 1):
        tot_ref[g] = sum_half[g]
        divide(g)
    lax.fori_loop(1, n, drain, 0)
    for i, ref in enumerate((stat_core, stat_half, sum_core, sum_half)):
        swap(i, ref).wait_send()
    for i, ref in enumerate((stat_chip, sum_chip)):
        for h in range(1, chips):
            chip_copy(i, ref, h, chip).wait_send()
    for r in range(1, n):
        a, b = peer(r)
        z_copy(r, a * 4 + b).wait_recv()
    total = zmsg[0]
    for s in range(1, n):
        total = total + zmsg[s]
    tot_ref[phases - 1] = total


def finish_kernel(n, phases, vl, tot_ref, z_ref, res_ref, bonus_ref, accept_ref, expected_ref, inverse, staged, accepted, expected, sem, bonus_sem, small_sem):
    width = n * ROWS
    num_draft = phases * ROWS
    last = phases - 1

    def ready_copy(g, b):
        return pltpu.make_async_copy(z_ref.at[pl.ds(pl.multiple_of(g * width + b * ROWS, ROWS), ROWS), :],
                                     res_ref.at[b, g * ROWS:(g + 1) * ROWS, :], sem.at[g, b])

    def staged_copy(b):
        return pltpu.make_async_copy(staged.at[b], res_ref.at[b, last * ROWS:, :], sem.at[last, b])

    bonus_copy = pltpu.make_async_copy(z_ref.at[phases * width:phases * width + n, :], bonus_ref, bonus_sem)

    def start(b, c):
        for g in range(last):
            ready_copy(g, b).start(priority=g % 2)
        return c
    lax.fori_loop(0, n, start, 0)
    bonus_copy.start()
    inverse[...] = jnp.broadcast_to(1.0 / (tot_ref[last, 0:1, :] * SCALE), (width, LANES)).T

    def one(b, c):
        inv = inverse[pl.ds(pl.multiple_of(b * ROWS, ROWS), ROWS), :]
        rows = pl.ds(pl.multiple_of(last * width + b * ROWS, ROWS), ROWS)
        for j in range(pl.cdiv(vl, LANES)):
            w = min(LANES, vl - j * LANES)
            staged[b, :, j * LANES:j * LANES + w] = (z_ref[rows, j * LANES:j * LANES + w] * SCALE) * inv[:, 0:w]
        staged_copy(b).start()
        return c
    lax.fori_loop(0, n, one, 0)

    seq_of = lax.broadcasted_iota(jnp.int32, (n, width), 1) // ROWS == lax.broadcasted_iota(jnp.int32, (n, width), 0)
    pos_of = lax.broadcasted_iota(jnp.int32, (ROWS, width), 1) % ROWS == lax.broadcasted_iota(jnp.int32, (ROWS, width), 0)
    to_seq = (lax.broadcasted_iota(jnp.int32, (width, n), 0) // ROWS
              == lax.broadcasted_iota(jnp.int32, (width, n), 1)).astype(jnp.float32)
    by_seq = jnp.zeros((n, num_draft), jnp.float32)
    by_pos = []
    for g in range(phases):
        a = jnp.minimum(1.0, tot_ref[g, 1:2, :] / tot_ref[g, 2:3, :])
        to_pos = (lax.broadcasted_iota(jnp.int32, (width, num_draft), 0) % ROWS + g * ROWS
                  == lax.broadcasted_iota(jnp.int32, (width, num_draft), 1)).astype(jnp.float32)
        by_seq = by_seq + jnp.dot(jnp.where(seq_of, jnp.broadcast_to(a, (n, width)), 0.0), to_pos,
                                  precision=lax.Precision.HIGHEST, preferred_element_type=jnp.float32)
        by_pos.append(jnp.dot(jnp.where(pos_of, jnp.broadcast_to(a, (ROWS, width)), 0.0), to_seq,
                              precision=lax.Precision.HIGHEST, preferred_element_type=jnp.float32))
    accepted[...] = by_seq
    accept_copy = pltpu.make_async_copy(accepted, accept_ref, small_sem.at[0])
    accept_copy.start()
    product = by_pos[0][0:1, :]
    total = product
    for k in range(1, num_draft):
        product = product * by_pos[k // ROWS][k % ROWS:k % ROWS + 1, :]
        total = total + product
    expected[...] = total
    expected_copy = pltpu.make_async_copy(expected, expected_ref, small_sem.at[1])
    expected_copy.start()

    def finished(b, c):
        for g in range(last):
            ready_copy(g, b).wait()
        staged_copy(b).wait()
        return c
    lax.fori_loop(0, n, finished, 0)
    bonus_copy.wait()
    accept_copy.wait()
    expected_copy.wait()


def solution(mesh):
    n = mesh.shape["tpa"] * mesh.shape["tpb"]

    def local_step(hidden, w_head, q_draft, x_draft):
        seqs, positions, depth = hidden.shape
        vl = w_head.shape[1]
        num_draft = x_draft.shape[1]
        phases = num_draft // ROWS
        vp = pl.cdiv(vl, LANES) * LANES
        rows = seqs * positions
        stat_rows = pl.cdiv(rows, LANES) * LANES
        f32 = jnp.float32
        any_spec = pl.BlockSpec(memory_space=pl.ANY)
        vmem_spec = pl.BlockSpec(memory_space=pltpu.VMEM)
        z, tot = pl.pallas_call(
            functools.partial(exchange_kernel, n, phases, vl),
            name="exchange",
            out_shape=(pltpu.VMEM((rows, vl), f32), pltpu.VMEM((phases, 3, LANES), f32)),
            in_specs=[any_spec] * 4,
            out_specs=(vmem_spec, vmem_spec),
            scratch_shapes=[
                pltpu.VMEM((rows, depth), jnp.bfloat16),
                pltpu.VMEM((rows, depth), jnp.bfloat16),
                pltpu.VMEM((W_BUFS, W_ROWS, depth), jnp.bfloat16),
                pltpu.VMEM((phases, n, ROWS, vp + LANES), f32),
                pltpu.VMEM((phases, n, ROWS, vp), f32),
                pltpu.VMEM((seqs, num_draft), jnp.int32),
                pltpu.VMEM((stat_rows, LANES), f32),
                pltpu.VMEM((stat_rows, LANES), f32),
                pltpu.VMEM((stat_rows, LANES), f32),
                pltpu.VMEM((phases * n * ROWS, LANES), f32),
                pltpu.VMEM((2, 2, stat_rows // LANES, LANES), f32),
                pltpu.VMEM((n // 2, 2, stat_rows // LANES // 2, LANES), f32),
                pltpu.VMEM((2, 2, stat_rows // LANES // 2, LANES), f32),
                pltpu.VMEM((2, 2, 3, LANES), f32),
                pltpu.VMEM((n // 2, 3, LANES), f32),
                pltpu.VMEM((2, 3, LANES), f32),
                pltpu.VMEM((n, 3, LANES), f32),
                pltpu.SemaphoreType.DMA((2,)),
                pltpu.SemaphoreType.DMA((W_BUFS,)),
                pltpu.SemaphoreType.DMA((phases, n)),
                pltpu.SemaphoreType.DMA((phases, n)),
                pltpu.SemaphoreType.DMA((phases, n)),
                pltpu.SemaphoreType.DMA((4,)),
                pltpu.SemaphoreType.DMA((4,)),
                pltpu.SemaphoreType.DMA((2, n // 2)),
                pltpu.SemaphoreType.DMA((2, n // 2)),
                pltpu.SemaphoreType.DMA((n,)),
                pltpu.SemaphoreType.DMA((n,)),
            ],
            compiler_params=pltpu.CompilerParams(collective_id=0, has_side_effects=True, vmem_limit_bytes=48 * 2**20),
        )(hidden.transpose(1, 0, 2).reshape(rows, depth), w_head.T, q_draft.reshape(num_draft, q_draft.shape[2]), x_draft)
        residual, bonus, accept, expected = pl.pallas_call(
            functools.partial(finish_kernel, n, phases, vl),
            name="finish",
            out_shape=(jax.ShapeDtypeStruct((seqs, num_draft, vl), f32), jax.ShapeDtypeStruct((seqs, vl), f32),
                       jax.ShapeDtypeStruct((seqs, num_draft), f32), jax.ShapeDtypeStruct((1, seqs), f32)),
            in_specs=[vmem_spec, vmem_spec],
            out_specs=(any_spec,) * 4,
            scratch_shapes=[pltpu.VMEM((n * ROWS, LANES), f32), pltpu.VMEM((seqs, ROWS, vl), f32),
                            pltpu.VMEM((seqs, num_draft), f32), pltpu.VMEM((1, seqs), f32),
                            pltpu.SemaphoreType.DMA((phases, seqs)), pltpu.SemaphoreType.DMA, pltpu.SemaphoreType.DMA((2,))],
            compiler_params=pltpu.CompilerParams(vmem_limit_bytes=32 * 2**20),
        )(tot, z)
        return accept, expected.reshape(seqs), residual, bonus

    return jax.shard_map(
        local_step, mesh=mesh,
        in_specs=(P("dp", None, None), P(None, VOCAB_AXES), P(("dp",) + VOCAB_AXES, None, None), P("dp", None)),
        out_specs=(P("dp", None), P("dp"), P("dp", None, VOCAB_AXES), P("dp", VOCAB_AXES)),
        check_vma=False)
```

```python
import functools

import jax
import jax.numpy as jnp
from jax import lax
from jax.experimental import pallas as pl
from jax.experimental.pallas import tpu as pltpu
from jax.sharding import PartitionSpec as P

INV_TEMP = 1.25
VOCAB_AXES = ("tpa", "tpb")
MESH = pl.DeviceIdType.MESH
LANES = 128
ROWS = 8
W_ROWS = 256
W_BUFS = 4
PIECES = 4
AHEAD = 4
SCALE = 2.0 ** 64


def xor4(a, r):
    low = lax.rem(lax.rem(a, 2) + lax.rem(r, 2), 2)
    high = lax.rem(lax.div(a, 2) + lax.div(r, 2), 2)
    return low + 2 * high


def exchange_kernel(n, phases, vl, hid_ref, w_ref, q_ref, x_ref, z_ref, tot_ref,
                    hid_v, hs, wbuf, sbuf, qbuf, x_v, colmax, colsum, scale, part, stat_core, stat_chip, stat_half, sum_core, sum_chip, sum_half, zmsg,
                    in_sem, w_sem, ld_sem, qs_sem, qr_sem, swap_s, swap_r, chip_s, chip_r, zs_sem, zr_sem):
    vp = qbuf.shape[3]
    tiles = vp // LANES
    last = vl - (tiles - 1) * LANES
    rows_all = z_ref.shape[0]
    draft_rows = phases * n * ROWS
    my_a, my_b = lax.axis_index("tpa"), lax.axis_index("tpb")
    me = my_a * 4 + my_b
    lane = lax.broadcasted_iota(jnp.int32, (ROWS, LANES), 1)

    def flip(a, r):
        return (a, a + 1 - 2 * lax.rem(a, 2), lax.rem(a + 2, 4), 3 - a)[r]

    def peer(r):
        if isinstance(r, int):
            return flip(my_a, r // 4), flip(my_b, r % 4)
        return xor4(my_a, lax.div(r, 4)), xor4(my_b, lax.rem(r, 4))

    def window(k):
        col = lax.div(k * vl, LANES) * LANES
        return pl.multiple_of(col, LANES), k * vl - col

    def sized(k, body):
        _, o = window(k)
        wide = o + vl > vp
        pl.when(wide)(lambda: body(vp + LANES))
        pl.when(jnp.logical_not(wide))(lambda: body(vp))

    core = lax.rem(my_b, 2)
    inner = lax.rem(lax.div(my_a + 1, 2), 2)

    def nth(g, i):
        r = lax.rem((n // 2 + 1) * (i + core) + n // 2, n)
        if g == phases - 1:
            far = lax.div(r, n // 2)
            r = (1 - far) * r + far * (n // 2 + lax.rem(r + (1 - inner) * (n // 4), n // 2))
        return r

    def arrival_order(g, i):
        far = lax.div(i, n // 2)
        return i if g < phases - 1 else (1 - far) * i + far * (n // 2 + lax.rem(i + n // 4, n // 2))

    def width_of(g):
        return vp if g < phases - 1 else vp - LANES

    def load(g, k, width):
        col, _ = window(k)
        return pltpu.make_async_copy(q_ref.at[g * ROWS:(g + 1) * ROWS, pl.ds(col, width)], sbuf.at[g, k, :, pl.ds(0, width)], ld_sem.at[g, k])

    def q_copy(g, r, s):
        a, b = peer(r)
        return pltpu.make_async_remote_copy(
            src_ref=sbuf.at[g, a * 4 + b, :, pl.ds(0, width_of(g))], dst_ref=qbuf.at[g, s, :, pl.ds(0, width_of(g))],
            send_sem=qs_sem.at[g, r], recv_sem=qr_sem.at[g, s],
            device_id={"tpa": a, "tpb": b}, device_id_type=MESH)

    def q_piece(g, r, h):
        a, b = peer(r)
        cut = [tiles * i // PIECES * LANES for i in range(PIECES)] + [width_of(g)]
        at = pl.ds(cut[h], cut[h + 1] - cut[h])
        return pltpu.make_async_remote_copy(
            src_ref=sbuf.at[g, a * 4 + b, :, at], dst_ref=qbuf.at[g, me, :, at],
            send_sem=qs_sem.at[g, r], recv_sem=qr_sem.at[g, me],
            device_id={"tpa": a, "tpb": b}, device_id_type=MESH)

    def tile_of(j):
        return slice(j * LANES, (j + 1) * LANES)

    def part_of(j):
        return slice(j * LANES, min((j + 1) * LANES, vl))

    free = LANES - last

    def prepare(g, k):
        _, o = window(k)
        shift = lax.rem(LANES - o, LANES)

        def last_tile(h):
            return jnp.where(lane < LANES - o, pltpu.roll(sbuf[h, k, :, tile_of(tiles - 1)], shift, 1),
                             pltpu.roll(sbuf[h, k, :, tile_of(tiles)], shift, 1))
        ending = last_tile(g)
        if g < phases - 1:
            guest = pltpu.roll(last_tile(phases - 1), last if g == 0 else LANES - (free - last) % LANES, 1)
            ending = jnp.where(lane < last, ending, guest)
        this = pltpu.roll(sbuf[g, k, :, tile_of(0)], shift, 1)
        for j in range(tiles - 1):
            following = pltpu.roll(sbuf[g, k, :, tile_of(j + 1)], shift, 1)
            sbuf[g, k, :, tile_of(j)] = jnp.where(lane < LANES - o, this, following)
            this = following
        sbuf[g, k, :, tile_of(tiles - 1)] = ending

    def ready(g, i):
        if g < phases - 1:
            @pl.when(i + AHEAD < n)
            def _():
                start_load(g, i + AHEAD)
        r = nth(g, i)
        a, b = peer(r)
        k = a * 4 + b
        if g == 0:
            sized(k, lambda width: load(0, k, width).wait())
            sized(k, lambda width: load(phases - 1, k, width).wait())
        elif g < phases - 1:
            sized(k, lambda width: load(g, k, width).wait())
        prepare(g, k)

        @pl.when(r == 0)
        def _():
            for j in range(tiles):
                qbuf[g, me, :, tile_of(j)] = sbuf[g, me, :, tile_of(j)]

    def first(g):
        lax.fori_loop(0, 2, lambda i, c: (ready(g, i), c)[1], 0)

    def send_phase(g):
        for h in range(PIECES):
            def one(i, c, h=h):
                r = nth(g, i)

                @pl.when(r > 0)
                def _():
                    q_piece(g, r, h).start()

                if h == 0:
                    @pl.when(i + 2 < n)
                    def _():
                        ready(g, i + 2)
                return c
            lax.fori_loop(0, n, one, 0)

    def w_copy(c, slot):
        return pltpu.make_async_copy(w_ref.at[pl.ds(pl.multiple_of(c * W_ROWS, W_ROWS), W_ROWS), :], wbuf.at[slot], w_sem.at[slot])

    full_chunks = vl // W_ROWS
    w_tail = vl - full_chunks * W_ROWS
    tail_slot = full_chunks % W_BUFS
    tail_copy = pltpu.make_async_copy(
        w_ref.at[pl.ds(full_chunks * W_ROWS, w_tail), :], wbuf.at[tail_slot, pl.ds(0, w_tail), :], w_sem.at[tail_slot])

    hid_copy = pltpu.make_async_copy(hid_ref, hid_v, in_sem.at[0])
    x_copy = pltpu.make_async_copy(x_ref, x_v, in_sem.at[1])
    barrier = pltpu.get_barrier_semaphore()

    for r in range(n - 1, 0, -1):
        a, b = peer(r)
        pl.semaphore_signal(barrier, inc=1, device_id={"tpa": a, "tpb": b}, device_id_type=MESH)

    def start_load(g, i):
        a, b = peer(nth(g, i))
        k = a * 4 + b
        for h in (0, phases - 1) if g == 0 else (g,):
            sized(k, lambda width, h=h: load(h, k, width).start())

    for i in range(AHEAD):
        start_load(0, i)
    x_copy.start()
    first(0)
    pl.semaphore_wait(barrier, n - 1)

    send_phase(0)
    for g in range(1, phases - 1):
        for i in range(AHEAD):
            start_load(g, i)
    hid_copy.start()
    for c in range(W_BUFS):
        w_copy(c, c).start()
    for g in range(1, phases - 1):
        first(g)
        send_phase(g)

    hid_copy.wait()
    row = lax.broadcasted_iota(jnp.int32, (rows_all, rows_all), 0)
    col = lax.broadcasted_iota(jnp.int32, (rows_all, rows_all), 1)
    source = jnp.where(row < draft_rows, ((row // (n * ROWS)) * ROWS + row % ROWS) * n + (row // ROWS) % n, row)
    permute = jnp.where(col == source, 1.0, 0.0).astype(jnp.bfloat16)
    depth = hid_v.shape[1]

    def permute_columns(c, carry):
        at = pl.ds(pl.multiple_of(c * 256, 256), 256)
        hs[:, at] = jnp.dot(permute, hid_v[:, at], preferred_element_type=jnp.float32).astype(jnp.bfloat16)
        return carry
    lax.fori_loop(0, depth // 256, permute_columns, 0)

    nt = (((1,), (1,)), ((), ()))

    def logits(c, carry):
        slot = lax.rem(c, W_BUFS)
        w_copy(c, slot).wait()
        z_ref[:, pl.ds(pl.multiple_of(c * W_ROWS, W_ROWS), W_ROWS)] = lax.dot_general(
            hs[...], wbuf[slot], nt, preferred_element_type=jnp.float32) * INV_TEMP

        @pl.when(c + W_BUFS < full_chunks)
        def _():
            w_copy(c + W_BUFS, slot).start()

        @pl.when(c + W_BUFS == full_chunks)
        def _():
            tail_copy.start()
        return carry
    lax.fori_loop(0, full_chunks, logits, 0)
    tail_copy.wait()
    z_ref[:, full_chunks * W_ROWS:vl] = lax.dot_general(
        hs[...], wbuf[tail_slot, 0:w_tail, :], nt, preferred_element_type=jnp.float32) * INV_TEMP

    def row_stats(t, carry):
        rows = pl.ds(pl.multiple_of(t * ROWS, ROWS), ROWS)
        ending = z_ref[rows, part_of(tiles - 1)]
        m = z_ref[rows, part_of(0)]
        for j in range(1, tiles - 1):
            m = jnp.maximum(m, z_ref[rows, part_of(j)])
        m = jnp.maximum(jnp.max(m, axis=1, keepdims=True), jnp.max(ending, axis=1, keepdims=True))
        m = jnp.broadcast_to(m, (ROWS, LANES))
        ending = jnp.exp(ending - m[:, 0:last])
        z_ref[rows, part_of(tiles - 1)] = ending
        s = jnp.zeros((ROWS, LANES), jnp.float32)
        for j in range(tiles - 1):
            e = jnp.exp(z_ref[rows, part_of(j)] - m)
            z_ref[rows, part_of(j)] = e
            s = s + e
        s = jnp.sum(s, axis=1, keepdims=True) + jnp.sum(ending, axis=1, keepdims=True)
        colmax[rows, :] = m
        colsum[rows, :] = jnp.broadcast_to(s, (ROWS, LANES))
        return carry
    lax.fori_loop(0, rows_all // ROWS, row_stats, 0)
    chip = my_a * 2 + lax.div(my_b, 2)
    chips = n // 2

    def swap(i, ref):
        return pltpu.make_async_remote_copy(
            src_ref=ref.at[core], dst_ref=ref.at[core], send_sem=swap_s.at[i], recv_sem=swap_r.at[i],
            device_id={"tpa": my_a, "tpb": my_b + 1 - 2 * core}, device_id_type=MESH)

    def swap_arrival(i, ref):
        return pltpu.make_async_remote_copy(
            src_ref=ref.at[1 - core], dst_ref=ref.at[1 - core], send_sem=swap_s.at[i], recv_sem=swap_r.at[i],
            device_id={"tpa": my_a, "tpb": my_b}, device_id_type=MESH)

    def chip_copy(i, ref, h, slot):
        a, b = peer(2 * h)
        return pltpu.make_async_remote_copy(
            src_ref=ref.at[chip], dst_ref=ref.at[slot], send_sem=chip_s.at[i, h], recv_sem=chip_r.at[i, slot],
            device_id={"tpa": a, "tpb": b}, device_id_type=MESH)

    def chip_send(i, ref):
        for h in range(chips - 1, 0, -1):
            chip_copy(i, ref, h, chip).start()

    def chip_arrivals(i, ref):
        for h in range(1, chips):
            a, b = peer(2 * h)
            chip_copy(i, ref, h, a * 2 + lax.div(b, 2)).wait_recv()

    def combine(pairs):
        top = pairs[0][0]
        for m, _ in pairs[1:]:
            top = jnp.maximum(top, m)
        total = jnp.zeros_like(top)
        for m, s in pairs:
            total = total + s * jnp.exp(m - top)
        return top, total

    spare = colmax.shape[0] - rows_all
    colmax[rows_all:, :] = jnp.zeros((spare, LANES), jnp.float32)
    colsum[rows_all:, :] = jnp.ones((spare, LANES), jnp.float32)

    blocks = colmax.shape[0] // LANES

    def as_rows(ref):
        return jnp.concatenate([ref[i * LANES:(i + 1) * LANES, :].T[0:1, :] for i in range(blocks)], axis=0)
    my_max = as_rows(colmax)
    stat_core[core, 0] = my_max
    stat_core[core, 1] = as_rows(colsum)
    swap(0, stat_core).start()
    swap_arrival(0, stat_core).wait_recv()
    top, total = combine([(stat_core[c, 0], stat_core[c, 1]) for c in range(2)])
    half = blocks // 2
    mine = core == 0
    stat_chip[chip, 0] = jnp.where(mine, top[0:half], top[half:])
    stat_chip[chip, 1] = jnp.where(mine, total[0:half], total[half:])
    chip_send(0, stat_chip)
    first(phases - 1)
    send_phase(phases - 1)

    chip_arrivals(0, stat_chip)
    top, total = combine([(stat_chip[c, 0], stat_chip[c, 1]) for c in range(chips)])
    stat_half[core, 0] = top
    stat_half[core, 1] = total
    swap(1, stat_half).start()
    swap_arrival(1, stat_half).wait_recv()
    top = jnp.concatenate([stat_half[0, 0], stat_half[1, 0]], axis=0)
    total = jnp.concatenate([stat_half[0, 1], stat_half[1, 1]], axis=0)
    factor = jnp.exp(stat_core[core, 0] - top) / total
    for i in range(blocks):
        scale[i * LANES:(i + 1) * LANES, :] = jnp.broadcast_to(factor[i:i + 1, :], (LANES, LANES)).T

    for t in range(draft_rows // ROWS, rows_all // ROWS):
        rows = slice(t * ROWS, (t + 1) * ROWS)
        for j in range(tiles):
            value = z_ref[rows, part_of(j)]
            z_ref[rows, part_of(j)] = value * scale[rows, 0:value.shape[1]]

    x_copy.wait()
    lane_f = lane.astype(jnp.float32)
    num_draft = x_v.shape[1]

    def excess(g, s):
        rows = pl.ds(pl.multiple_of(g * (n * ROWS) + s * ROWS, ROWS), ROWS)
        tokens = jnp.broadcast_to(x_v[pl.ds(s, 1), :].astype(jnp.float32), (ROWS, num_draft))
        position = lax.broadcasted_iota(jnp.int32, (ROWS, num_draft), 0) + g * ROWS
        here = lax.broadcasted_iota(jnp.int32, (ROWS, num_draft), 1) == position
        token = jnp.sum(jnp.where(here, tokens, 0.0), axis=1, keepdims=True) - (me * vl).astype(jnp.float32)
        token = jnp.broadcast_to(jnp.where(token < vl, token, -1.0), (ROWS, LANES))
        sc = scale[rows, :]
        z_sum = p_pick = q_pick = jnp.zeros((ROWS, LANES), jnp.float32)
        for j in range(tiles - 1):
            q = qbuf[g, s, :, tile_of(j)]
            p = z_ref[rows, part_of(j)] * sc
            d = jnp.maximum(p - q, 0.0)
            z_ref[rows, part_of(j)] = d
            z_sum = z_sum + d
            hit = lane_f == token - float(j * LANES)
            p_pick = jnp.where(hit, p, p_pick)
            q_pick = jnp.where(hit, q, q_pick)
        j = tiles - 1
        if g < phases - 1:
            q = qbuf[g, s, :, tile_of(j)]
        else:
            q = jnp.where(lane < free, pltpu.roll(qbuf[0, s, :, tile_of(j)], free, 1),
                          pltpu.roll(qbuf[1, s, :, tile_of(j)], (free - last) % LANES, 1))
        q = q[:, 0:last]
        p = z_ref[rows, part_of(j)] * sc[:, 0:last]
        d = jnp.maximum(p - q, 0.0)
        z_ref[rows, part_of(j)] = d
        hit = (lane_f == token - float(j * LANES))[:, 0:last]
        sums = [jnp.sum(whole, axis=1, keepdims=True) + jnp.sum(ending, axis=1, keepdims=True)
                for whole, ending in ((z_sum, d), (p_pick, jnp.where(hit, p, 0.0)), (q_pick, jnp.where(hit, q, 0.0)))]
        part[rows, :] = jnp.where(lane == 0, sums[0], jnp.where(lane == 1, sums[1], sums[2]))

    def z_copy(r, s):
        a, b = peer(r)
        return pltpu.make_async_remote_copy(
            src_ref=zmsg.at[me], dst_ref=zmsg.at[s], send_sem=zs_sem.at[r], recv_sem=zr_sem.at[s],
            device_id={"tpa": a, "tpb": b}, device_id_type=MESH)

    def row_sums(g):
        block = slice(g * n * ROWS, (g + 1) * n * ROWS)
        return part[block, :].T[0:3, :]

    for g in range(phases):
        def one(i, c, g=g):
            r = arrival_order(g, i)
            a, b = peer(r)
            s = a * 4 + b

            @pl.when(r > 0)
            def _():
                q_copy(g, r, s).wait_recv()
            excess(g, s)
            return c
        lax.fori_loop(0, n, one, 0)
        if g == phases - 2:
            for h in range(2):
                sum_core[core, h] = row_sums(h)
            swap(2, sum_core).start()
            swap_arrival(2, sum_core).wait_recv()
            sum_chip[chip] = jnp.where(mine, sum_core[0, 0] + sum_core[1, 0], sum_core[0, 1] + sum_core[1, 1])
            chip_send(1, sum_chip)
    zmsg[me] = row_sums(phases - 1)
    for r in range(n - 1, 0, -1):
        z_copy(r, me).start()

    def drain(r, c):
        for g in range(phases):
            q_copy(g, r, me).wait_send()
        z_copy(r, me).wait_send()
        return c

    def divide(g):
        inverse = jnp.broadcast_to(1.0 / (tot_ref[g, 0:1, :] * SCALE), (n * ROWS, LANES)).T
        scale[0:n * ROWS, :] = inverse

        def one(s, c):
            rows = pl.ds(pl.multiple_of(g * (n * ROWS) + s * ROWS, ROWS), ROWS)
            inv = scale[pl.ds(pl.multiple_of(s * ROWS, ROWS), ROWS), :]
            for j in range(tiles):
                value = z_ref[rows, part_of(j)] * SCALE
                z_ref[rows, part_of(j)] = value * inv[:, 0:value.shape[1]]
            return c
        lax.fori_loop(0, n, one, 0)

    chip_arrivals(1, sum_chip)
    total = sum_chip[0]
    for c in range(1, chips):
        total = total + sum_chip[c]
    sum_half[core] = total
    swap(3, sum_half).start()
    swap_arrival(3, sum_half).wait_recv()
    for g in range(phases - 1):
        tot_ref[g] = sum_half[g]
        divide(g)
    lax.fori_loop(1, n, drain, 0)
    for i, ref in enumerate((stat_core, stat_half, sum_core, sum_half)):
        swap(i, ref).wait_send()
    for i, ref in enumerate((stat_chip, sum_chip)):
        for h in range(1, chips):
            chip_copy(i, ref, h, chip).wait_send()
    for r in range(1, n):
        a, b = peer(r)
        z_copy(r, a * 4 + b).wait_recv()
    total = zmsg[0]
    for s in range(1, n):
        total = total + zmsg[s]
    tot_ref[phases - 1] = total


def finish_kernel(n, phases, vl, tot_ref, z_ref, res_ref, bonus_ref, accept_ref, expected_ref, inverse, staged, accepted, expected, sem, bonus_sem, small_sem):
    width = n * ROWS
    num_draft = phases * ROWS
    last = phases - 1

    def ready_copy(g, b):
        return pltpu.make_async_copy(z_ref.at[pl.ds(pl.multiple_of(g * width + b * ROWS, ROWS), ROWS), :],
                                     res_ref.at[b, g * ROWS:(g + 1) * ROWS, :], sem.at[g, b])

    def staged_copy(b):
        return pltpu.make_async_copy(staged.at[b], res_ref.at[b, last * ROWS:, :], sem.at[last, b])

    bonus_copy = pltpu.make_async_copy(z_ref.at[phases * width:phases * width + n, :], bonus_ref, bonus_sem)

    def start(b, c):
        for g in range(last):
            ready_copy(g, b).start(priority=g % 2)
        return c
    lax.fori_loop(0, n, start, 0)
    bonus_copy.start()
    inverse[...] = jnp.broadcast_to(1.0 / (tot_ref[last, 0:1, :] * SCALE), (width, LANES)).T

    def one(b, c):
        inv = inverse[pl.ds(pl.multiple_of(b * ROWS, ROWS), ROWS), :]
        rows = pl.ds(pl.multiple_of(last * width + b * ROWS, ROWS), ROWS)
        for j in range(pl.cdiv(vl, LANES)):
            w = min(LANES, vl - j * LANES)
            staged[b, :, j * LANES:j * LANES + w] = (z_ref[rows, j * LANES:j * LANES + w] * SCALE) * inv[:, 0:w]
        staged_copy(b).start()
        return c
    lax.fori_loop(0, n, one, 0)

    seq_of = lax.broadcasted_iota(jnp.int32, (n, width), 1) // ROWS == lax.broadcasted_iota(jnp.int32, (n, width), 0)
    pos_of = lax.broadcasted_iota(jnp.int32, (ROWS, width), 1) % ROWS == lax.broadcasted_iota(jnp.int32, (ROWS, width), 0)
    to_seq = (lax.broadcasted_iota(jnp.int32, (width, n), 0) // ROWS
              == lax.broadcasted_iota(jnp.int32, (width, n), 1)).astype(jnp.float32)
    by_seq = jnp.zeros((n, num_draft), jnp.float32)
    by_pos = []
    for g in range(phases):
        a = jnp.minimum(1.0, tot_ref[g, 1:2, :] / tot_ref[g, 2:3, :])
        to_pos = (lax.broadcasted_iota(jnp.int32, (width, num_draft), 0) % ROWS + g * ROWS
                  == lax.broadcasted_iota(jnp.int32, (width, num_draft), 1)).astype(jnp.float32)
        by_seq = by_seq + jnp.dot(jnp.where(seq_of, jnp.broadcast_to(a, (n, width)), 0.0), to_pos,
                                  precision=lax.Precision.HIGHEST, preferred_element_type=jnp.float32)
        by_pos.append(jnp.dot(jnp.where(pos_of, jnp.broadcast_to(a, (ROWS, width)), 0.0), to_seq,
                              precision=lax.Precision.HIGHEST, preferred_element_type=jnp.float32))
    accepted[...] = by_seq
    accept_copy = pltpu.make_async_copy(accepted, accept_ref, small_sem.at[0])
    accept_copy.start()
    product = by_pos[0][0:1, :]
    total = product
    for k in range(1, num_draft):
        product = product * by_pos[k // ROWS][k % ROWS:k % ROWS + 1, :]
        total = total + product
    expected[...] = total
    expected_copy = pltpu.make_async_copy(expected, expected_ref, small_sem.at[1])
    expected_copy.start()

    def finished(b, c):
        for g in range(last):
            ready_copy(g, b).wait()
        staged_copy(b).wait()
        return c
    lax.fori_loop(0, n, finished, 0)
    bonus_copy.wait()
    accept_copy.wait()
    expected_copy.wait()


def solution(mesh):
    n = mesh.shape["tpa"] * mesh.shape["tpb"]

    def local_step(hidden, w_head, q_draft, x_draft):
        seqs, positions, depth = hidden.shape
        vl = w_head.shape[1]
        num_draft = x_draft.shape[1]
        phases = num_draft // ROWS
        vp = pl.cdiv(vl, LANES) * LANES
        rows = seqs * positions
        stat_rows = pl.cdiv(rows, LANES) * LANES
        f32 = jnp.float32
        any_spec = pl.BlockSpec(memory_space=pl.ANY)
        vmem_spec = pl.BlockSpec(memory_space=pltpu.VMEM)
        z, tot = pl.pallas_call(
            functools.partial(exchange_kernel, n, phases, vl),
            name="exchange",
            out_shape=(pltpu.VMEM((rows, vl), f32), pltpu.VMEM((phases, 3, LANES), f32)),
            in_specs=[any_spec] * 4,
            out_specs=(vmem_spec, vmem_spec),
            scratch_shapes=[
                pltpu.VMEM((rows, depth), jnp.bfloat16),
                pltpu.VMEM((rows, depth), jnp.bfloat16),
                pltpu.VMEM((W_BUFS, W_ROWS, depth), jnp.bfloat16),
                pltpu.VMEM((phases, n, ROWS, vp + LANES), f32),
                pltpu.VMEM((phases, n, ROWS, vp), f32),
                pltpu.VMEM((seqs, num_draft), jnp.int32),
                pltpu.VMEM((stat_rows, LANES), f32),
                pltpu.VMEM((stat_rows, LANES), f32),
                pltpu.VMEM((stat_rows, LANES), f32),
                pltpu.VMEM((phases * n * ROWS, LANES), f32),
                pltpu.VMEM((2, 2, stat_rows // LANES, LANES), f32),
                pltpu.VMEM((n // 2, 2, stat_rows // LANES // 2, LANES), f32),
                pltpu.VMEM((2, 2, stat_rows // LANES // 2, LANES), f32),
                pltpu.VMEM((2, 2, 3, LANES), f32),
                pltpu.VMEM((n // 2, 3, LANES), f32),
                pltpu.VMEM((2, 3, LANES), f32),
                pltpu.VMEM((n, 3, LANES), f32),
                pltpu.SemaphoreType.DMA((2,)),
                pltpu.SemaphoreType.DMA((W_BUFS,)),
                pltpu.SemaphoreType.DMA((phases, n)),
                pltpu.SemaphoreType.DMA((phases, n)),
                pltpu.SemaphoreType.DMA((phases, n)),
                pltpu.SemaphoreType.DMA((4,)),
                pltpu.SemaphoreType.DMA((4,)),
                pltpu.SemaphoreType.DMA((2, n // 2)),
                pltpu.SemaphoreType.DMA((2, n // 2)),
                pltpu.SemaphoreType.DMA((n,)),
                pltpu.SemaphoreType.DMA((n,)),
            ],
            compiler_params=pltpu.CompilerParams(collective_id=0, has_side_effects=True, vmem_limit_bytes=48 * 2**20),
        )(hidden.transpose(1, 0, 2).reshape(rows, depth), w_head.T, q_draft.reshape(num_draft, q_draft.shape[2]), x_draft)
        residual, bonus, accept, expected = pl.pallas_call(
            functools.partial(finish_kernel, n, phases, vl),
            name="finish",
            out_shape=(jax.ShapeDtypeStruct((seqs, num_draft, vl), f32), jax.ShapeDtypeStruct((seqs, vl), f32),
                       jax.ShapeDtypeStruct((seqs, num_draft), f32), jax.ShapeDtypeStruct((1, seqs), f32)),
            in_specs=[vmem_spec, vmem_spec],
            out_specs=(any_spec,) * 4,
            scratch_shapes=[pltpu.VMEM((n * ROWS, LANES), f32), pltpu.VMEM((seqs, ROWS, vl), f32),
                            pltpu.VMEM((seqs, num_draft), f32), pltpu.VMEM((1, seqs), f32),
                            pltpu.SemaphoreType.DMA((phases, seqs)), pltpu.SemaphoreType.DMA, pltpu.SemaphoreType.DMA((2,))],
            compiler_params=pltpu.CompilerParams(vmem_limit_bytes=32 * 2**20),
        )(tot, z)
        return accept, expected.reshape(seqs), residual, bonus

    return jax.shard_map(
        local_step, mesh=mesh,
        in_specs=(P("dp", None, None), P(None, VOCAB_AXES), P(("dp",) + VOCAB_AXES, None, None), P("dp", None)),
        out_specs=(P("dp", None), P("dp"), P("dp", None, VOCAB_AXES), P("dp", VOCAB_AXES)),
        check_vma=False)
```
